32 devices in a mesh: section: 2 (over core), dp: 2 (over y), tensor: 8 (over z, x).
Axes of the slice: x: 2, y: 2, z: 4, core: 2. Of those that a mesh axis runs over, the one named last changes fastest.
Arguments:
- residual_parts: bfloat16 [2, 768, 16384], P('section', 'dp', 'tensor'), may hold values from -120 to 120
- attn_out: bfloat16 [2, 768, 16384], P('section', 'dp', 'tensor'), may hold values from -6 to 6
- ffn_input: bfloat16 [2, 768, 53248], P('section', 'dp', 'tensor'), may hold values from -6 to 6
- norm_gain: float32 [2, 16384], P('section', 'tensor'), may hold values from 0.25 to 1.75
- mixing: bfloat16 [2, 52, 52], P('section'), may hold values from -0.875 to 0.875
- blocks: int32 [2, 2], P('section'), may hold values from 0 to 25, as said below
Outputs:
- hess_in: float32 [2, 16384, 1024], P('section', 'tensor', 'dp')
- hess_o: float32 [2, 16384, 1024], P('section', 'tensor', 'dp')
- hess_down: float32 [2, 2048, 2048], P('section', 'tensor', 'dp')
The draws below stay inside these ranges and needn't reach their ends.
Inputs may be any that keep to these rules, and one draw needn't show every extreme that they name: `blocks`: entry [s, 0] is below 16; entry [s, 1] is below 26. In every draw one layer has entry [s, 0] = 0 and entry [s, 1] = 25.
All inputs are finite; a program needn't handle non-finite values.
Results may differ from the reference program's by a relative error of at most 0.0038.
Values may be sent and summed in bfloat16 or wider, within the bound.
A program may use at most 128 MiB of HBM per device.

```python
import math
import jax
import jax.numpy as jnp
from jax import lax

D = 16384
FF = 53248
KB = 52
HBLK = 1024
BLK = 2048
MB_TOK = 192
KA = 1024
TOKENS = 768
N_SECTION = 2


def draw_residual_parts(key, part):
    key_base, key_rows, key_cols, key_delta = jax.random.split(jax.random.fold_in(key, 11), 4)
    base = jax.random.normal(key_base, (TOKENS, D), jnp.float32)
    row_scale = jnp.exp(jax.random.uniform(key_rows, (TOKENS,), jnp.float32, 0.0, math.log(10.0)))
    rising = jnp.exp(math.log(3.0) * jnp.arange(D, dtype=jnp.float32) / D)
    col_scale = rising * jnp.exp(jax.random.uniform(key_cols, (D,), jnp.float32, 0.0, math.log(10.0))) / 3.0
    stream = base * row_scale[:, None] * col_scale[None, :]
    update = 2.0 * jax.random.normal(key_delta, (TOKENS, D), jnp.float32) * row_scale[:, None]
    parts = jnp.stack([stream, update] + [update] * (N_SECTION - 2))
    return jnp.clip(parts, -120.0, 120.0).astype(jnp.bfloat16)


def draw_blocks(key, part):
    key_in, key_down, key_pick = jax.random.split(jax.random.fold_in(key, 23), 3)
    first = jax.random.randint(key_in, (N_SECTION,), 0, D // HBLK, jnp.int32)
    second = jax.random.randint(key_down, (N_SECTION,), 0, FF // BLK, jnp.int32)
    picked = jax.random.randint(key_pick, (), 0, N_SECTION, jnp.int32)
    is_picked = jnp.arange(N_SECTION, dtype=jnp.int32) == picked
    first = jnp.where(is_picked, 0, first).astype(jnp.int32)
    second = jnp.where(is_picked, FF // BLK - 1, second).astype(jnp.int32)
    return jnp.stack([first, second], axis=1)


def levels(stream_key, dims, pieces, least, high):
    loudness = 1.0
    for dim, blocks in pieces:
        steps = jax.random.uniform(jax.random.fold_in(jax.random.fold_in(stream_key, 6), dim), (blocks,), jnp.float32, least / len(pieces), high / len(pieces))
        loudness = loudness * jnp.repeat(jnp.exp(steps), dims[dim] // blocks).reshape((-1,) + (1,) * (len(dims) - 1 - dim))
    return loudness


def normal_values(stream_key, shape, spread, limit, cuts=(), kind=jnp.bfloat16):
    drawn = spread * jax.random.normal(stream_key, shape, jnp.float32)
    if cuts:
        drawn = drawn * levels(stream_key, shape, cuts, -0.22, 0.18)
    return jnp.clip(drawn, -limit, limit).astype(kind)


def setup_inputs(seed: int = 0) -> dict:
    key_list = jax.random.split(jax.random.key(seed), 7)
    residual_parts = draw_residual_parts(jax.random.fold_in(key_list[6], 71), 0)
    attn_out = normal_values(key_list[1], (N_SECTION, TOKENS, D), 1.0, 6.0, ((0, 2), (1, 2), (2, 8)))
    ffn_input = normal_values(key_list[2], (N_SECTION, TOKENS, FF), 1.0, 6.0, ((0, 2), (1, 2), (2, 8)))
    norm_gain = jnp.clip(1.0 + 0.15 * jax.random.normal(key_list[3], (N_SECTION, D), jnp.float32), 0.25, 1.75)
    mixing = normal_values(key_list[4], (N_SECTION, KB, KB), KB ** -0.5, 0.875, ((0, 2),))
    blocks = draw_blocks(jax.random.fold_in(key_list[6], 71), 0)
    return {"residual_parts": residual_parts, "attn_out": attn_out, "ffn_input": ffn_input, "norm_gain": norm_gain, "mixing": mixing, "blocks": blocks}


EPS = 1e-05

def bit_parity(values):
    total = jnp.zeros_like(values)
    for position in range(16):
        total = total + values // (1 << position) % 2
    return total % 2

def sylvester(order):
    index = jnp.arange(order, dtype=jnp.int32)
    parity = bit_parity(jnp.bitwise_and(index[:, None], index[None, :]))
    return (1 - 2 * parity).astype(jnp.float32)

def gram(left, right):
    return jnp.dot(left.T, right, preferred_element_type=jnp.float32)

def down_block(hidden, mixing_one, start):
    width_a = BLK // KB + 2
    first_a = jnp.minimum(start // KB, KA - width_a).astype(jnp.int32)
    chosen = lax.dynamic_slice_in_dim(sylvester(KA), first_a, width_a, 1)
    inner = (start - first_a * KB).astype(jnp.int32)
    factor = mixing_one.astype(jnp.float32)

    def one_block(token_rows):
        cube = token_rows.astype(jnp.float32).reshape(MB_TOK, KA, KB)
        mixed = jnp.einsum('rak,kc->rac', cube, factor, precision=lax.Precision.HIGHEST)
        turned = jnp.einsum('rac,ae->rec', mixed, chosen, precision=lax.Precision.HIGHEST)
        turned = turned / math.sqrt(KA)
        flat = turned.reshape(MB_TOK, width_a * KB)
        return lax.dynamic_slice_in_dim(flat, inner, BLK, 1).astype(jnp.bfloat16)
    grouped = hidden.reshape(TOKENS // MB_TOK, MB_TOK, FF)
    return lax.map(one_block, grouped).reshape(TOKENS, BLK)

def reference(residual_parts, attn_out, ffn_input, norm_gain, mixing, blocks):
    scale = 2.0 / TOKENS
    list_in, list_o, list_down = ([], [], [])
    for layer in range(N_SECTION):
        layer_in = residual_parts[layer].astype(jnp.float32)
        if layer > 0:
            layer_in = residual_parts[layer - 1].astype(jnp.float32) + layer_in
        mean_sq = lax.optimization_barrier(jnp.mean(layer_in * layer_in, axis=1))
        normed = (layer_in * lax.rsqrt(mean_sq + EPS)[:, None] * norm_gain[layer][None, :]).astype(jnp.bfloat16)
        first = (blocks[layer, 0] * HBLK).astype(jnp.int32)
        norm_cols = lax.dynamic_slice_in_dim(normed, first, HBLK, 1)
        list_in.append(scale * gram(normed, norm_cols))
        attention = attn_out[layer]
        attn_cols = lax.dynamic_slice_in_dim(attention, first, HBLK, 1)
        list_o.append(scale * gram(attention, attn_cols))
        start = (blocks[layer, 1] * BLK).astype(jnp.int32)
        down_cols = down_block(ffn_input[layer], mixing[layer], start)
        list_down.append(scale * gram(down_cols, down_cols))
    return (jnp.stack(list_in), jnp.stack(list_o), jnp.stack(list_down))
```

```python
import functools
import math

import jax
import jax.numpy as jnp
from jax import lax
from jax.experimental import pallas as pl
from jax.experimental.pallas import tpu as pltpu
from jax.sharding import PartitionSpec as P

D = 16384
KB = 52
HBLK = 1024
BLK = 2048
GROUP = 32


EPS = 1e-05

MESH = pl.DeviceIdType.MESH


def passed_along(x, axis, by):
    devices = lax.axis_size(axis)
    pairs = [(i, i + by) for i in range(devices) if 0 <= i + by < devices]
    return lax.ppermute(x, axis, pairs)


def shifted(x, axis, by):
    devices = lax.axis_size(axis)
    return lax.ppermute(x, axis, [(i, (i + by) % devices) for i in range(devices)])


def gathered(x, axis):
    return [x] + [shifted(x, axis, by) for by in range(1, lax.axis_size(axis))]


def reduce_kernel(n, extras, *refs):
    x_ref, refs = refs[0], refs[1:]
    e_ref, refs = (refs[0], refs[1:]) if extras else (None, refs)
    out_ref, refs = refs[0], refs[1:]
    eout_ref, refs = (refs[0], refs[1:]) if extras else (None, refs)
    recv, mine, send_a, recv_a, send_b, recv_b = refs[:6]
    me = lax.axis_index("tensor")

    barrier = pltpu.get_barrier_semaphore()
    for k in range(1, n):
        pl.semaphore_signal(
            barrier, inc=1, device_id={"tensor": lax.rem(me + k, n)}, device_id_type=MESH
        )
    pl.semaphore_wait(barrier, n - 1)

    def remote(src, dst, send, receive, k):
        return pltpu.make_async_remote_copy(
            src_ref=src,
            dst_ref=dst,
            send_sem=send.at[k],
            recv_sem=receive.at[k],
            device_id={"tensor": lax.rem(me + k, n)},
            device_id_type=MESH,
        )

    order = sorted(range(1, n), key=lambda k: -min(k, n - k))
    extra = []
    if extras:
        erecv, send_e, recv_e = refs[6:]
        extra = [remote(e_ref, erecv.at[k], send_e, recv_e, k) for k in order]
    first = [remote(x_ref.at[lax.rem(me + k, n)], recv.at[k], send_a, recv_a, k) for k in order]
    for copy in extra + first:
        copy.start()
    if extras:
        for copy in extra:
            copy.wait()
        eout_ref[...] = e_ref[...] + functools.reduce(
            lambda a, k: a + erecv[k], range(2, n), erecv[1]
        )
    for copy in first:
        copy.wait()
    total = x_ref[me].astype(jnp.float32)
    for k in range(1, n):
        total = total + recv[k].astype(jnp.float32)
    mine[...] = total.astype(mine.dtype)
    out_ref[me] = total.astype(mine.dtype)
    partner = me + 1 - 2 * lax.rem(me, 2)
    half = n // 2

    def placed(src, slot, index, target):
        return pltpu.make_async_remote_copy(
            src_ref=src,
            dst_ref=out_ref.at[slot],
            send_sem=send_b.at[index],
            recv_sem=recv_b.at[index],
            device_id={"tensor": target},
            device_id_type=MESH,
        )

    ring = sorted(range(1, half), key=lambda k: -min(k, half - k))
    along = {k: placed(mine, me, k, lax.rem(me + 2 * k, n)) for k in ring}
    across = [placed(mine, me, 0, partner)]
    for copy in list(along.values()) + across:
        copy.start()
    for k in sorted(range(1, half), key=lambda k: min(k, half - k)):
        along[k].wait_recv()
        source = lax.rem(me + n - 2 * k, n)
        copy = placed(out_ref.at[source], source, half - 1 + k, partner)
        copy.start()
        across.append(copy)
    for copy in along.values():
        copy.wait_send()
    for copy in across:
        copy.wait()


def tensor_sum(x, extra, ident):
    n = lax.axis_size("tensor")
    rows, columns = x.shape
    x = x.reshape(n, rows // n, columns)
    vmem = pl.BlockSpec(memory_space=pltpu.VMEM)
    operands = [x] + ([extra] if extra is not None else [])
    shapes = [jax.ShapeDtypeStruct(x.shape, jnp.bfloat16)]
    scratch = [
        pltpu.VMEM(x.shape, x.dtype),
        pltpu.VMEM(x.shape[1:], jnp.bfloat16),
    ] + [pltpu.SemaphoreType.DMA((n,))] * 4
    if extra is not None:
        shapes.append(jax.ShapeDtypeStruct(extra.shape, extra.dtype))
        scratch += [pltpu.VMEM((n,) + extra.shape, extra.dtype)]
        scratch += [pltpu.SemaphoreType.DMA((n,))] * 2
    out = pl.pallas_call(
        functools.partial(reduce_kernel, n, extra is not None),
        out_shape=shapes,
        in_specs=[vmem] * len(operands),
        out_specs=[vmem] * len(shapes),
        scratch_shapes=scratch,
        compiler_params=pltpu.CompilerParams(
            collective_id=ident, has_side_effects=True, vmem_limit_bytes=32 << 20
        ),
        cost_estimate=pl.CostEstimate(flops=0, bytes_accessed=100 << 20, transcendentals=0),
    )(*operands)
    return [out[0].reshape(rows, columns)] + list(out[1:])


def chosen(index, values):
    picked = jnp.int32(values[0])
    for place, value in enumerate(values[1:], 1):
        picked = jnp.where(index == place, jnp.int32(value), picked)
    return picked


def line_order(count):
    def edge(c):
        return min(c, count - 1 - c)

    return [
        sorted(range(count), key=lambda c: (-abs(c - z), edge(c))) for z in range(count)
    ]


def exchange_kernel(n, groups, *refs):
    attn_h, res_h, ffn_h, base, signs, gain, flags = refs[:7]
    attn_o, norm_o, slab_o, rot_o, own_o = refs[7:12]
    (
        attn_v, res_v, ffn_v, attn_s, attn_y, res_y, rc, xs, xr, zs, left_b, right_b,
        sq_col, sq_s, sq_r, tot_s, tot_r, inv, sl_k, sl_s, sl_x, sl_p, fl_s, fl_r, piece,
        local_sem, send_sem, recv_sem,
    ) = refs[12:]
    rows, features = attn_v.shape
    deep = ffn_v.shape[1] // groups
    share = xs.shape[2]
    half = features // 2
    width = slab_o.shape[3]
    line = n // 2
    near = line // 2
    f32, bf16 = jnp.float32, jnp.bfloat16

    s = lax.axis_index("section")
    d = lax.axis_index("dp")
    t = lax.axis_index("tensor")
    z = t // 2
    x = t - 2 * z
    x_peer = {"tensor": t + 1 - 2 * x}
    y_peer = {"dp": 1 - d}
    c_peer = {"section": 1 - s}

    taken = [0]

    def sems(count):
        first = taken[0]
        taken[0] += count
        return first

    def remote(source, target, send, receive, device):
        return pltpu.make_async_remote_copy(
            src_ref=source,
            dst_ref=target,
            send_sem=send_sem.at[send],
            recv_sem=recv_sem.at[receive],
            device_id=device,
            device_id_type=MESH,
        )

    loads = [
        pltpu.make_async_copy(a, b, local_sem.at[i])
        for i, (a, b) in enumerate([(attn_h, attn_v), (res_h, res_v), (ffn_h, ffn_v)])
    ]
    for copy in loads:
        copy.start()

    barrier = pltpu.get_barrier_semaphore()
    others = [{"tensor": lax.rem(t + k, n)} for k in range(1, n)] + [y_peer, c_peer]
    for device in others:
        pl.semaphore_signal(barrier, inc=1, device_id=device, device_id_type=MESH)
    pl.semaphore_wait(barrier, n + 1)

    swap = flags[0] > 0
    owned = flags[1] > 0
    last = []

    loads[0].wait()
    low, high = attn_v[:, :half], attn_v[:, half:]
    attn_s[0] = jnp.where(swap, high, low)
    attn_s[1] = jnp.where(swap, low, high)
    k = sems(2)
    attn_copy = [remote(attn_s.at[i], attn_y.at[i], k + i, k + i, y_peer) for i in range(2)]
    attn_copy[0].start()

    loads[1].wait()
    k = sems(2)
    lift = [remote(res_v, rc.at[0], k, k, c_peer), remote(res_y, rc.at[1], k + 1, k + 1, c_peer)]

    @pl.when(s == 0)
    def _():
        lift[0].start()
        rc[...] = jnp.zeros_like(rc)

    @pl.when(z == 0)
    def _():
        for m in range(2):
            fl_r[m, 0] = jnp.zeros((rows, width), bf16)

    @pl.when(z == line - 1)
    def _():
        for m in range(2):
            fl_r[m, 1] = jnp.zeros((rows, width), bf16)

    order = line_order(line)

    def destination(i):
        flat = [order[a][b] for a in range(line) for b in range(line)]
        return chosen(z * line + i, flat)

    def rotate(j):
        total = None
        for g in range(groups):
            part = jnp.dot(
                ffn_v[:, g * deep : (g + 1) * deep],
                base[:, pl.ds(pl.multiple_of(j * share, share), share)],
                preferred_element_type=f32,
            )
            part = part * signs[j, g : g + 1, :]
            total = part if total is None else total + part
        return total

    loads[2].wait()
    x_sem = sems(line)

    def to_x(i):
        return remote(xs.at[i], xr.at[i], x_sem + i, x_sem + i, x_peer)

    xs[0] = rotate(2 * destination(0) + 1 - x)

    @pl.when(s > 0)
    def _():
        lift[0].wait_recv()

    strip = 64

    def squares(b, carry):
        at = pl.ds(pl.multiple_of(b * strip, strip), strip)
        acc = jnp.zeros((strip, 128), f32)
        for c in range(features // 128):
            lanes = slice(c * 128, (c + 1) * 128)
            v = res_v[at, lanes].astype(f32) + rc[0, at, lanes].astype(f32)
            acc = acc + v * v
        sq_col[at, :] = jnp.broadcast_to(jnp.sum(acc, axis=1, keepdims=True), (strip, 128))
        return carry

    lax.fori_loop(0, rows // strip, squares, 0)
    sq_s[...] = jnp.transpose(sq_col[...])[:8, :]
    k = sems(n)
    stats = [
        remote(sq_s, sq_r.at[i], k + i, k + i, {"tensor": lax.rem(t + i, n)}) for i in range(1, n)
    ]
    for copy in stats:
        copy.start()
    to_x(0).start()

    def outward(i, carry):
        xs[i] = rotate(2 * destination(i) + 1 - x)
        to_x(i).start()
        return carry

    lax.fori_loop(1, line, outward, 0)

    for copy in stats:
        copy.wait_recv()
    last.extend(copy.wait_send for copy in stats)
    total = sq_s[...]
    for i in range(1, n):
        total = total + sq_r[i]
    tot_s[...] = total
    k = sems(1)
    tot_copy = remote(tot_s, tot_r, k, k, y_peer)
    tot_copy.start()
    k = sems(1)
    res_copy = remote(res_v, res_y, k, k, y_peer)
    res_copy.start()

    def inverse(slot, sums):
        spread = jnp.broadcast_to(sums[:1, :], (128, rows))
        inv[slot] = lax.rsqrt(jnp.transpose(spread) / (n * features) + EPS)

    inverse(0, total)

    def normalize(slot, part):
        def step(b, carry):
            at = pl.ds(pl.multiple_of(b * strip, strip), strip)
            by = inv[slot, at, :]
            for c in range(features // 128):
                lanes = slice(c * 128, (c + 1) * 128)
                v = part[at, lanes].astype(f32) + rc[slot, at, lanes].astype(f32)
                norm_o[slot, at, lanes] = (v * by * gain[:, lanes]).astype(bf16)
            return carry

        lax.fori_loop(0, rows // strip, step, 0)

    slab_x = sems(2)

    def slab_copy(m):
        return remote(sl_s.at[m], sl_x.at[m], slab_x + m, slab_x + m, x_peer)

    def slab_start(m, first, second):
        first = jnp.where(owned, first, jnp.zeros_like(first))
        second = jnp.where(owned, second, jnp.zeros_like(second))
        sl_k[m] = jnp.where(x == 0, first, second)
        sl_s[m] = jnp.where(x == 0, second, first)
        slab_copy(m).start()

    mine = pl.ds(pl.multiple_of(d * width, width), width)
    pieces = 2
    tall = rows // pieces
    flood_sem = sems(2 * 2 * pieces)

    def flood_copy(m, way, q):
        at = pl.ds(q * tall, tall)
        k = flood_sem + (m * 2 + way) * pieces + q
        return remote(
            fl_s.at[m, way, at], fl_r.at[m, way, at], k, k, {"tensor": t + 2 - 4 * way}
        )

    def flood_way(phase):
        before = jnp.where(z < near, 0, 1)
        return before if phase == 0 else 1 - before

    def flood(m, phase):
        way = flood_way(phase)
        first = jnp.where(way == 0, z == 0, z == line - 1)
        final = jnp.where(way == 0, z == line - 1, z == 0)
        for q in range(pieces):
            at = pl.ds(q * tall, tall)

            @pl.when(jnp.logical_not(first))
            def _():
                flood_copy(m, way, q).wait_recv()

            @pl.when(jnp.logical_not(final))
            def _():
                fl_s[m, way, at] = sl_p[m, at] + fl_r[m, way, at]
                flood_copy(m, way, q).start()

    def flood_finish(m, phase):
        way = flood_way(phase)
        final = jnp.where(way == 0, z == line - 1, z == 0)

        @pl.when(jnp.logical_not(final))
        def _():
            for q in range(pieces):
                flood_copy(m, way, q).wait_send()

    slab_back = sems(2 * pieces)

    def back_copy(m, q):
        at = pl.ds(q * tall, tall)
        k = slab_back + m * pieces + q
        return remote(slab_o.at[m, x, at], slab_o.at[m, x, at], k, k, x_peer)

    def back_wait(m, q):
        at = pl.ds(q * tall, tall)
        k = slab_back + m * pieces + q
        remote(slab_o.at[m, x, at], slab_o.at[m, 1 - x, at], k, k, x_peer).wait_recv()

    def slab_pair(m):
        slab_copy(m).wait_recv()
        sl_p[m] = sl_k[m] + sl_x[m]

    def slab_end(m):
        for q in range(pieces):
            at = pl.ds(q * tall, tall)
            slab_o[m, x, at] = sl_p[m, at] + fl_r[m, 0, at] + fl_r[m, 1, at]
            back_copy(m, q).start()

    z_send = sems(line)
    left_sem = sems(line)
    right_sem = sems(line)

    def to_right(i, to):
        return remote(zs.at[i], left_b.at[to], z_send + i, left_sem + to, {"tensor": t + 2})

    def to_left(i, to):
        return remote(zs.at[i], right_b.at[to], z_send + i, right_sem + to, {"tensor": t - 2})

    def inward(i, carry):
        to = destination(i)
        zs[i] = rotate(2 * to + x)
        to_x(i).wait_recv()
        zs[i] = zs[i] + xr[i]

        @pl.when((to >= z) & (z > 0))
        def _():
            to_right(i, to).wait_recv()
            zs[i] = zs[i] + left_b[to]

        @pl.when((to <= z) & (z < line - 1))
        def _():
            to_left(i, to).wait_recv()
            zs[i] = zs[i] + right_b[to]

        @pl.when(to > z)
        def _():
            to_right(i, to).start()

        @pl.when(to < z)
        def _():
            to_left(i, to).start()

        return carry

    lax.fori_loop(0, near, inward, 0)
    attn_copy[0].wait_recv()
    slab_start(0, attn_s[0, :, mine], attn_y[0, :, mine])
    lax.fori_loop(near, line, inward, 0)

    own_o[0] = zs[line - 1].astype(bf16)
    piece[...] = own_o[0]
    k = sems(1)
    piece_copy = remote(piece, own_o.at[1], k, k, y_peer)
    piece_copy.start()
    attn_copy[1].start()

    u = jnp.where(d == 0, z, line - 1 - z)
    onward = {"tensor": t + 2 - 4 * d}
    inner = {"tensor": t - 2 + 4 * d}
    gather_z = sems(near * 2)
    gather_out = sems(near * 2)
    gather_in = sems(near * 2)
    gather_x = sems(near * 2)

    def slot(ref, source, column, b):
        place = jnp.where(d == 0, source, near - 1 - source) * 2 + column
        return ref.at[b, :, pl.ds(pl.multiple_of(place * share, share), share)]

    def gather_copy(source, b, kind):
        k = source * 2 + b
        into = slot(rot_o, source, x, b)
        if kind == "own_out":
            return remote(piece if b == 0 else own_o.at[1], into, gather_out + k, gather_z + k, onward)
        if kind == "own_in":
            return remote(piece if b == 0 else own_o.at[1], into, gather_in + k, gather_z + k, inner)
        if kind == "out":
            return remote(into, into, gather_out + k, gather_z + k, onward)
        if kind == "in":
            return remote(into, into, gather_in + k, gather_z + k, inner)
        return remote(into, into, gather_x + k, gather_x + k, x_peer)

    def gather_own(b):
        for source in range(near):

            @pl.when(u == source)
            def _():
                gather_copy(source, b, "own_out").start()
                if source > 0:
                    gather_copy(source, b, "own_in").start()
                place = jnp.where(d == 0, source, near - 1 - source) * 2 + x
                rot_o[b, :, pl.ds(pl.multiple_of(place * share, share), share)] = own_o[b]

    def gather_rest(b):
        for source in reversed(range(near)):

            @pl.when(u != source)
            def _():
                gather_copy(source, b, "out").wait_recv()

            @pl.when((u > source) & (u < line - 1))
            def _():
                gather_copy(source, b, "out").start()

            @pl.when((u < source) & (u > 0))
            def _():
                gather_copy(source, b, "in").start()

            gather_copy(source, b, "x").start()

    def gather_finish(b):
        for source in range(near):

            @pl.when((u >= source) & (u < line - 1))
            def _():
                gather_copy(source, b, "out").wait_send()

            @pl.when((u <= source) & (u > 0) & (source > 0))
            def _():
                gather_copy(source, b, "in").wait_send()

            k = source * 2 + b
            remote(
                slot(rot_o, source, x, b), slot(rot_o, source, 1 - x, b),
                gather_x + k, gather_x + k, x_peer,
            ).wait()

    gather_own(0)
    slab_pair(0)
    flood(0, 0)
    normalize(0, res_v)
    gather_rest(0)
    flood(0, 1)
    slab_end(0)

    res_copy.wait_recv()

    @pl.when(s == 0)
    def _():
        lift[1].start()

    piece_copy.wait_recv()
    gather_own(1)
    tot_copy.wait_recv()
    inverse(1, tot_r[...])

    @pl.when(s > 0)
    def _():
        lift[1].wait_recv()

    normalize(1, res_y)
    upper = pl.ds(pl.multiple_of(half + d * width, width), width)
    slab_start(
        1,
        jnp.where(swap, norm_o[0, :, upper], norm_o[0, :, mine]),
        jnp.where(swap, norm_o[1, :, upper], norm_o[1, :, mine]),
    )
    gather_rest(1)
    slab_pair(1)
    flood(1, 0)
    flood(1, 1)
    slab_end(1)

    attn_o[0] = attn_v[...]
    attn_copy[1].wait_recv()
    low, high = attn_y[0], attn_y[1]
    attn_o[1, :, :half] = jnp.where(swap, high, low)
    attn_o[1, :, half:] = jnp.where(swap, low, high)

    for m in range(2):
        for q in range(pieces):
            back_wait(m, q)
            back_copy(m, q).wait_send()
        slab_copy(m).wait_send()
        for phase in range(2):
            flood_finish(m, phase)
    for b in range(2):
        gather_finish(b)
    for copy in attn_copy + [tot_copy, res_copy, piece_copy]:
        copy.wait_send()

    @pl.when(s == 0)
    def _():
        lift[0].wait_send()
        lift[1].wait_send()

    def finish(i, carry):
        to_x(i).wait_send()
        to = destination(i)

        @pl.when(to != z)
        def _():
            to_right(i, to).wait_send()

        return carry

    lax.fori_loop(0, line, finish, 0)
    for wait in last:
        wait()


SEMAPHORES = 96


def exchanged(attn, res, ffn, base, signs, gain, flags, groups):
    n = lax.axis_size("tensor")
    rows, features = attn.shape
    half, share, width = features // 2, BLK // n, HBLK // 2
    line = n // 2
    f32, bf16 = jnp.float32, jnp.bfloat16
    vmem = pl.BlockSpec(memory_space=pltpu.VMEM)
    anywhere = pl.BlockSpec(memory_space=pl.ANY)
    return pl.pallas_call(
        functools.partial(exchange_kernel, n, groups),
        out_shape=[
            jax.ShapeDtypeStruct((2, rows, features), bf16),
            jax.ShapeDtypeStruct((2, rows, features), bf16),
            jax.ShapeDtypeStruct((2, 2, rows, width), bf16),
            jax.ShapeDtypeStruct((2, rows, BLK // 2), bf16),
            jax.ShapeDtypeStruct((2, rows, share), bf16),
        ],
        in_specs=[anywhere] * 3 + [vmem] * 3 + [pl.BlockSpec(memory_space=pltpu.SMEM)],
        out_specs=[vmem] * 5,
        scratch_shapes=[
            pltpu.VMEM((rows, features), bf16),
            pltpu.VMEM((rows, features), bf16),
            pltpu.VMEM(ffn.shape, bf16),
            pltpu.VMEM((2, rows, half), bf16),
            pltpu.VMEM((2, rows, half), bf16),
            pltpu.VMEM((rows, features), bf16),
            pltpu.VMEM((2, rows, features), bf16),
            pltpu.VMEM((line, rows, share), f32),
            pltpu.VMEM((line, rows, share), f32),
            pltpu.VMEM((line, rows, share), f32),
            pltpu.VMEM((line, rows, share), f32),
            pltpu.VMEM((line, rows, share), f32),
            pltpu.VMEM((rows, 128), f32),
            pltpu.VMEM((8, rows), f32),
            pltpu.VMEM((n, 8, rows), f32),
            pltpu.VMEM((8, rows), f32),
            pltpu.VMEM((8, rows), f32),
            pltpu.VMEM((2, rows, 128), f32),
            pltpu.VMEM((2, rows, width), bf16),
            pltpu.VMEM((2, rows, width), bf16),
            pltpu.VMEM((2, rows, width), bf16),
            pltpu.VMEM((2, rows, width), bf16),
            pltpu.VMEM((2, 2, rows, width), bf16),
            pltpu.VMEM((2, 2, rows, width), bf16),
            pltpu.VMEM((rows, share), bf16),
            pltpu.SemaphoreType.DMA((3,)),
            pltpu.SemaphoreType.DMA((SEMAPHORES,)),
            pltpu.SemaphoreType.DMA((SEMAPHORES,)),
        ],
        compiler_params=pltpu.CompilerParams(
            collective_id=2, has_side_effects=True, vmem_limit_bytes=60 << 20
        ),
    )(attn, res, ffn, base, signs, gain, flags)


def parity_sign(values):
    return (1 - 2 * (lax.population_count(values) & 1)).astype(jnp.float32)


def gram(left, right):
    return lax.dot_general(
        left, right, (((0,), (0,)), ((), ())), preferred_element_type=jnp.float32
    )


def general(residual_parts, attn_out, ffn_input, norm_gain, mixing, blocks):
    local_d = residual_parts.shape[2]
    local_f = ffn_input.shape[2]
    token_rows = residual_parts.shape[1]
    dp_count = lax.axis_size("dp")
    dp_member = lax.axis_index("dp")
    tensor_count = lax.axis_size("tensor")
    member = lax.axis_index("tensor")
    own_part = residual_parts[0]
    parts = gathered(own_part, "dp")
    attention = jnp.concatenate(gathered(attn_out[0], "dp"), axis=0)
    earlier = [passed_along(part, "section", 1) for part in parts]
    layers = [
        e.astype(jnp.float32) + p.astype(jnp.float32) for e, p in zip(earlier, parts)
    ]
    squares = jnp.sum(layers[0] * layers[0], axis=1).reshape(token_rows // 128, 128)

    a_local = local_f // KB
    order_a = a_local * tensor_count
    deep = GROUP * KB
    column = blocks[0, 1] * BLK + jnp.arange(BLK, dtype=jnp.int32)
    a_col, c_col = column // KB, column % KB
    pick = (jnp.arange(KB, dtype=jnp.int32)[:, None] == c_col[None, :]).astype(jnp.bfloat16)
    spread = jnp.dot(
        jnp.tile(mixing[0], (GROUP, 1)), pick, preferred_element_type=jnp.float32
    )
    row_a = jnp.arange(deep, dtype=jnp.int32) // KB
    base = (spread * parity_sign(row_a[:, None] & a_col[None, :])).astype(jnp.bfloat16)
    term = None
    for g in range(a_local // GROUP):
        sign = parity_sign((member * a_local + g * GROUP) & a_col) / math.sqrt(order_a)
        piece = jnp.dot(
            ffn_input[0, :, g * deep : (g + 1) * deep], base, preferred_element_type=jnp.float32
        )
        piece = piece * sign[None, :]
        term = piece if term is None else term + piece

    rotated, square_own = tensor_sum(term, squares, 0)

    square_total = gathered(square_own, "dp")
    rotated, square_total = lax.optimization_barrier((rotated, square_total))
    square_total = [s.reshape(token_rows) for s in square_total]
    share = BLK // tensor_count
    own_cols = lax.dynamic_slice_in_dim(rotated, member * share, share, 1)
    part_down = gram(own_cols, rotated)
    half = BLK // dp_count
    if dp_count == 2:
        kept = lax.dynamic_slice_in_dim(part_down, dp_member * half, half, 1)
        sent = lax.dynamic_slice_in_dim(part_down, (1 - dp_member) * half, half, 1)
        sum_down = kept + shifted(sent, "dp", 1)
    else:
        sum_down = lax.psum_scatter(part_down, "dp", scatter_dimension=1, tiled=True)

    normed = jnp.concatenate(
        [
            (x * lax.rsqrt(s / D + EPS)[:, None] * norm_gain[0][None, :]).astype(jnp.bfloat16)
            for x, s in zip(layers, square_total)
        ],
        axis=0,
    )
    first_col = blocks[0, 0] * HBLK
    width = HBLK // dp_count
    offset = first_col % local_d + dp_member * width
    owned = first_col // local_d == member
    slab = jnp.concatenate(
        [
            lax.dynamic_slice_in_dim(normed, offset, width, 1),
            lax.dynamic_slice_in_dim(attention, offset, width, 1),
        ],
        axis=0,
    )
    slab = jnp.where(owned, slab, 0).astype(jnp.bfloat16)
    (got,) = tensor_sum(slab, None, 1)
    tokens = token_rows * dp_count
    scale = 2.0 / tokens
    hess_in = (scale * gram(normed, got[:tokens]))[None]
    hess_o = (scale * gram(attention, got[tokens:]))[None]
    hess_down = (scale * sum_down)[None]
    return (hess_in, hess_o, hess_down)


def paired(residual_parts, attn_out, ffn_input, norm_gain, mixing, blocks):
    local_d = residual_parts.shape[2]
    local_f = ffn_input.shape[2]
    token_rows = residual_parts.shape[1]
    n = lax.axis_size("tensor")
    member = lax.axis_index("tensor")
    share = BLK // n
    a_local = local_f // KB
    groups = a_local // GROUP
    deep = GROUP * KB
    column = blocks[0, 1] * BLK + jnp.arange(BLK, dtype=jnp.int32)
    a_col, c_col = column // KB, column % KB
    pick = (jnp.arange(KB, dtype=jnp.int32)[:, None] == c_col[None, :]).astype(jnp.bfloat16)
    spread = jnp.dot(
        jnp.tile(mixing[0], (GROUP, 1)), pick, preferred_element_type=jnp.float32
    )
    row_a = jnp.arange(deep, dtype=jnp.int32) // KB
    base = (spread * parity_sign(row_a[:, None] & a_col[None, :])).astype(jnp.bfloat16)
    first_a = member * a_local + GROUP * jnp.arange(groups, dtype=jnp.int32)
    signs = parity_sign(first_a[:, None] & a_col[None, :]) / math.sqrt(a_local * n)
    signs = signs.reshape(groups, n, share).transpose(1, 0, 2)
    first_col = blocks[0, 0] * HBLK
    swap = (first_col % local_d) // HBLK
    owned = (first_col // local_d == member).astype(jnp.int32)
    flags = jnp.stack([swap, owned]).astype(jnp.int32)
    attention, normed, slab, rotated, own = exchanged(
        attn_out[0], residual_parts[0], ffn_input[0], base, signs, norm_gain, flags, groups
    )
    tokens = token_rows * 2
    scale = 2.0 / tokens
    attention, normed = attention.reshape(tokens, local_d), normed.reshape(tokens, local_d)
    slab = slab.reshape(2, tokens, HBLK // 2)
    hess_down = (scale * gram(own.reshape(tokens, share), rotated.reshape(tokens, BLK // 2)))[None]
    hess_in = (scale * gram(normed, slab[1]))[None]
    hess_o = (scale * gram(attention, slab[0]))[None]
    return (hess_in, hess_o, hess_down)


def local(*arguments):
    n = lax.axis_size("tensor")
    by_pairs = lax.axis_size("dp") == 2 and lax.axis_size("section") == 2 and n % 4 == 0
    if by_pairs and arguments[0].shape[2] == 2 * HBLK:
        return paired(*arguments)
    return general(*arguments)


def solution(mesh):
    return jax.shard_map(
        local,
        mesh=mesh,
        in_specs=(
            P("section", "dp", "tensor"),
            P("section", "dp", "tensor"),
            P("section", "dp", "tensor"),
            P("section", "tensor"),
            P("section", None, None),
            P("section", None),
        ),
        out_specs=(
            P("section", "tensor", "dp"),
            P("section", "tensor", "dp"),
            P("section", "tensor", "dp"),
        ),
        check_vma=False,
    )
```

```python
import functools
import math

import jax
import jax.numpy as jnp
from jax import lax
from jax.experimental import pallas as pl
from jax.experimental.pallas import tpu as pltpu
from jax.sharding import PartitionSpec as P

D = 16384
KB = 52
HBLK = 1024
BLK = 2048
GROUP = 32


EPS = 1e-05

MESH = pl.DeviceIdType.MESH


def passed_along(x, axis, by):
    devices = lax.axis_size(axis)
    pairs = [(i, i + by) for i in range(devices) if 0 <= i + by < devices]
    return lax.ppermute(x, axis, pairs)


def shifted(x, axis, by):
    devices = lax.axis_size(axis)
    return lax.ppermute(x, axis, [(i, (i + by) % devices) for i in range(devices)])


def gathered(x, axis):
    return [x] + [shifted(x, axis, by) for by in range(1, lax.axis_size(axis))]


def reduce_kernel(n, extras, *refs):
    x_ref, refs = refs[0], refs[1:]
    e_ref, refs = (refs[0], refs[1:]) if extras else (None, refs)
    out_ref, refs = refs[0], refs[1:]
    eout_ref, refs = (refs[0], refs[1:]) if extras else (None, refs)
    recv, mine, send_a, recv_a, send_b, recv_b = refs[:6]
    me = lax.axis_index("tensor")

    barrier = pltpu.get_barrier_semaphore()
    for k in range(1, n):
        pl.semaphore_signal(
            barrier, inc=1, device_id={"tensor": lax.rem(me + k, n)}, device_id_type=MESH
        )
    pl.semaphore_wait(barrier, n - 1)

    def remote(src, dst, send, receive, k):
        return pltpu.make_async_remote_copy(
            src_ref=src,
            dst_ref=dst,
            send_sem=send.at[k],
            recv_sem=receive.at[k],
            device_id={"tensor": lax.rem(me + k, n)},
            device_id_type=MESH,
        )

    order = sorted(range(1, n), key=lambda k: -min(k, n - k))
    extra = []
    if extras:
        erecv, send_e, recv_e = refs[6:]
        extra = [remote(e_ref, erecv.at[k], send_e, recv_e, k) for k in order]
    first = [remote(x_ref.at[lax.rem(me + k, n)], recv.at[k], send_a, recv_a, k) for k in order]
    for copy in extra + first:
        copy.start()
    if extras:
        for copy in extra:
            copy.wait()
        eout_ref[...] = e_ref[...] + functools.reduce(
            lambda a, k: a + erecv[k], range(2, n), erecv[1]
        )
    for copy in first:
        copy.wait()
    total = x_ref[me].astype(jnp.float32)
    for k in range(1, n):
        total = total + recv[k].astype(jnp.float32)
    mine[...] = total.astype(mine.dtype)
    out_ref[me] = total.astype(mine.dtype)
    partner = me + 1 - 2 * lax.rem(me, 2)
    half = n // 2

    def placed(src, slot, index, target):
        return pltpu.make_async_remote_copy(
            src_ref=src,
            dst_ref=out_ref.at[slot],
            send_sem=send_b.at[index],
            recv_sem=recv_b.at[index],
            device_id={"tensor": target},
            device_id_type=MESH,
        )

    ring = sorted(range(1, half), key=lambda k: -min(k, half - k))
    along = {k: placed(mine, me, k, lax.rem(me + 2 * k, n)) for k in ring}
    across = [placed(mine, me, 0, partner)]
    for copy in list(along.values()) + across:
        copy.start()
    for k in sorted(range(1, half), key=lambda k: min(k, half - k)):
        along[k].wait_recv()
        source = lax.rem(me + n - 2 * k, n)
        copy = placed(out_ref.at[source], source, half - 1 + k, partner)
        copy.start()
        across.append(copy)
    for copy in along.values():
        copy.wait_send()
    for copy in across:
        copy.wait()


def tensor_sum(x, extra, ident):
    n = lax.axis_size("tensor")
    rows, columns = x.shape
    x = x.reshape(n, rows // n, columns)
    vmem = pl.BlockSpec(memory_space=pltpu.VMEM)
    operands = [x] + ([extra] if extra is not None else [])
    shapes = [jax.ShapeDtypeStruct(x.shape, jnp.bfloat16)]
    scratch = [
        pltpu.VMEM(x.shape, x.dtype),
        pltpu.VMEM(x.shape[1:], jnp.bfloat16),
    ] + [pltpu.SemaphoreType.DMA((n,))] * 4
    if extra is not None:
        shapes.append(jax.ShapeDtypeStruct(extra.shape, extra.dtype))
        scratch += [pltpu.VMEM((n,) + extra.shape, extra.dtype)]
        scratch += [pltpu.SemaphoreType.DMA((n,))] * 2
    out = pl.pallas_call(
        functools.partial(reduce_kernel, n, extra is not None),
        out_shape=shapes,
        in_specs=[vmem] * len(operands),
        out_specs=[vmem] * len(shapes),
        scratch_shapes=scratch,
        compiler_params=pltpu.CompilerParams(
            collective_id=ident, has_side_effects=True, vmem_limit_bytes=32 << 20
        ),
        cost_estimate=pl.CostEstimate(flops=0, bytes_accessed=100 << 20, transcendentals=0),
    )(*operands)
    return [out[0].reshape(rows, columns)] + list(out[1:])


UNITS = ("ao", "no", "ap", "np")
HALVED = ("ao", "no", "ap", "np",)
SHARED = (
    9, 5, 10, 13, 6, 7, 11, 14, 12, 15, 16, 8,
)
ORDERS = (
    (
        33, 9, 17, 0, 5, 37, 41, 10, 18, 13, 6, 21, 7, 34, 11, 14, 19, 22, 12, 38, 15, 42, 20,
        16, 23, 1, 35, 49, 3, 39, 43, 8, 24, 4, 25, 29, 2, 36, 27, 31, 26, 30, 40, 44, 28, 32,
        50, 51, 52,
    ),
    (
        33, 9, 17, 0, 5, 37, 10, 18, 13, 6, 41, 7, 11, 34, 45, 14, 19, 12, 38, 21, 15, 20, 16,
        23, 1, 35, 22, 42, 49, 3, 24, 4, 39, 27, 31, 8, 36, 46, 2, 43, 50, 28, 25, 29, 47, 40,
        26, 30, 44, 32, 48, 51, 52,
    ),
    (
        33, 9, 17, 0, 5, 37, 10, 18, 13, 6, 45, 7, 11, 34, 41, 14, 19, 12, 38, 21, 15, 20, 16,
        23, 1, 35, 22, 46, 49, 3, 24, 4, 39, 8, 36, 42, 2, 50, 47, 27, 31, 40, 43, 51, 48, 28,
        32, 25, 29, 26, 30, 44, 52,
    ),
    (
        33, 9, 17, 0, 5, 37, 45, 10, 18, 13, 6, 21, 7, 34, 11, 14, 19, 22, 12, 38, 15, 46, 20,
        16, 23, 1, 35, 49, 3, 39, 47, 8, 24, 4, 36, 2, 50, 40, 48, 27, 31, 51, 28, 32, 25, 29,
        26, 30, 52,
    ),
)


def step_names(line, near):
    numbers = [str(i) for i in range(line)]
    pairs = [str(a) + str(b) for a in range(near) for b in range(2)]
    names = ["res", "A2", "B", "lift2s", "pc", "stat", "statr", "normo", "normp"]
    names += [k + i for k in ("X", "O", "xs", "I") for i in numbers]
    names += [k + p for k in ("G", "GX") for p in pairs]
    names += [k + unit for k in ("S", "P", "fo", "fi", "e") for unit in UNITS]
    return names + [k + unit + i for k in ("r", "v") for unit in UNITS for i in numbers]


def chosen(index, values):
    picked = jnp.int32(values[0])
    for place, value in enumerate(values[1:], 1):
        picked = jnp.where(index == place, jnp.int32(value), picked)
    return picked


def line_order(count):
    def edge(c):
        return min(c, count - 1 - c)

    return [
        sorted(range(count), key=lambda c: (-abs(c - z), edge(c))) for z in range(count)
    ]


def segments(order, shared):
    parts, rest = [], list(order)
    for heavy in shared:
        at = rest.index(heavy)
        parts.append(rest[:at])
        rest = rest[at + 1 :]
    return parts + [rest]


def exchange_kernel(n, groups, *refs):
    attn_h, res_h, ffn_h, base, signs, gain, flags = refs[:7]
    attn_o, norm_o, slab_o, rot_o, own_o = refs[7:12]
    (
        attn_v, res_v, ffn_v, attn_s, attn_y, res_y, rc, xs, xr, zs, onto, into,
        sq_col, sq_s, sq_r, tot_s, tot_r, inv, sl_k, sl_s, sl_x, sl_p, fl_s, fl_r,
        qt_f, qt_s, qt_o, qt_i, qt_x, local_sem, send_sem, recv_sem,
    ) = refs[12:]
    rows, features = attn_v.shape
    deep = ffn_v.shape[1] // groups
    share = xs.shape[2]
    half = features // 2
    width = slab_o.shape[3]
    line = n // 2
    near = line // 2
    f32, bf16 = jnp.float32, jnp.bfloat16

    s = lax.axis_index("section")
    d = lax.axis_index("dp")
    t = lax.axis_index("tensor")
    z = t // 2
    x = t - 2 * z
    u = jnp.where(d == 0, z, line - 1 - z)
    toward = 2 - 4 * d
    outward = {"tensor": t + toward}
    inner = {"tensor": t - toward}
    x_peer = {"tensor": t + 1 - 2 * x}
    y_peer = {"dp": 1 - d}
    c_peer = {"section": 1 - s}
    order = line_order(line)
    names = {}

    def sem(name):
        return names.setdefault(name, len(names))

    def remote(source, target, send, receive, device):
        return pltpu.make_async_remote_copy(
            src_ref=source,
            dst_ref=target,
            send_sem=send_sem.at[sem(send)],
            recv_sem=recv_sem.at[sem(receive)],
            device_id=device,
            device_id_type=MESH,
        )

    sent = {}

    def post(uc, make):
        make().start()
        sent.setdefault(uc, []).append(make)

    def combine(target, parts, count, kind=None, strip=48):
        def step(b, carry):
            at = pl.ds(pl.multiple_of(b * strip, strip), strip)
            total = parts[0][at, :]
            for part in parts[1:]:
                total = total + part[at, :]
            target[at, :] = total if kind is None else total.astype(kind)
            return carry

        lax.fori_loop(0, count // strip, step, 0)

    loads = [
        pltpu.make_async_copy(a, b, local_sem.at[i])
        for i, (a, b) in enumerate([(attn_h, attn_v), (res_h, res_v), (ffn_h, ffn_v)])
    ]
    for copy in loads:
        copy.start()

    barrier = pltpu.get_barrier_semaphore()
    others = [{"tensor": lax.rem(t + k, n)} for k in range(1, n)] + [y_peer, c_peer]
    for device in others:
        pl.semaphore_signal(barrier, inc=1, device_id=device, device_id_type=MESH)
    pl.semaphore_wait(barrier, n + 1)

    swap = flags[0] > 0
    owned = flags[1] > 0

    def q0():
        return remote(attn_s.at[1 - d], attn_y.at[1 - d], "q0", "q0", y_peer)

    def a2():
        return remote(attn_s.at[d], attn_y.at[d], "A2", "A2", y_peer)

    def b2():
        return remote(attn_s.at[2:4], attn_y.at[2:4], "B", "B", y_peer)

    def res():
        return remote(res_v, res_y, "res", "res", y_peer)

    def tot():
        return remote(tot_s, tot_r, "tot", "tot", y_peer)

    def pc():
        return remote(own_o.at[0], own_o.at[1], "pc", "pc", y_peer)

    def lift(slot, source):
        return remote(source, rc.at[slot], "lift" + str(slot), "lift" + str(slot), c_peer)

    loads[0].wait()
    for k in range(4):
        here = slice(k * width, (k + 1) * width)
        there = slice((k + 2) % 4 * width, ((k + 2) % 4 + 1) * width)
        attn_s[k] = jnp.where(swap, attn_v[:, there], attn_v[:, here])
    post(None, q0)
    loads[1].wait()

    @pl.when(s == 0)
    def _():
        lift(0, res_v).start()
        rc[...] = jnp.zeros_like(rc)

    def destination(i):
        flat = [order[a][i] for a in range(line)]
        to = chosen(u, flat)
        return jnp.where(d == 0, to, line - 1 - to)

    def rotate(target, j):
        def step(g, carry):
            at = pl.ds(pl.multiple_of(g * deep, 128), deep)
            part = jnp.dot(
                ffn_v[:, at],
                base[:, pl.ds(pl.multiple_of(j * share, share), share)],
                preferred_element_type=f32,
            )
            part = part * signs[j, pl.ds(g, 1), :]

            @pl.when(g == 0)
            def _():
                target[...] = part

            @pl.when(g > 0)
            def _():
                target[...] = target[...] + part

            return carry

        lax.fori_loop(0, groups, step, 0)

    strip = 64

    def stat():
        @pl.when(s > 0)
        def _():
            lift(0, res_v).wait_recv()

        def squares(b, carry):
            at = pl.ds(pl.multiple_of(b * strip, strip), strip)
            acc = jnp.zeros((strip, 128), f32)
            for c in range(features // 128):
                lanes = slice(c * 128, (c + 1) * 128)
                v = res_v[at, lanes].astype(f32) + rc[0, at, lanes].astype(f32)
                acc = acc + v * v
            sq_col[at, :] = jnp.broadcast_to(jnp.sum(acc, axis=1, keepdims=True), (strip, 128))
            return carry

        lax.fori_loop(0, rows // strip, squares, 0)
        sq_s[...] = jnp.transpose(sq_col[...])[:8, :]
        for i in range(1, n):
            post(None, functools.partial(stat_copy, i))

    def stat_copy(i):
        name = "stat" + str(i)
        return remote(sq_s, sq_r.at[i], name, name, {"tensor": lax.rem(t + i, n)})

    def inverse(slot, sums):
        spread = jnp.broadcast_to(sums[:1, :], (128, rows))
        inv[slot] = lax.rsqrt(jnp.transpose(spread) / (n * features) + EPS)

    def stats_in():
        total = sq_s[...]
        for i in range(1, n):
            stat_copy(i).wait_recv()
            total = total + sq_r[i]
        tot_s[...] = total
        post(None, tot)
        inverse(0, total)

    def normalize(slot, part):
        def step(b, carry):
            at = pl.ds(pl.multiple_of(b * strip, strip), strip)
            by = inv[slot, at, :]
            for c in range(features // 128):
                lanes = slice(c * 128, (c + 1) * 128)
                v = part[at, lanes].astype(f32) + rc[slot, at, lanes].astype(f32)
                norm_o[slot, at, lanes] = (v * by * gain[:, lanes]).astype(bf16)
            return carry

        lax.fori_loop(0, rows // strip, step, 0)

    def normalize_peer():
        tot().wait_recv()
        inverse(1, tot_r[...])

        @pl.when(s > 0)
        def _():
            res().wait_recv()
            lift(1, res_y).wait_recv()

        normalize(1, res_y)

    def heavy(name):
        if name[0] in "XO":
            i = int(name[1:])
            column = 1 - x if name[0] == "X" else x
            rotate((xs if name[0] == "X" else zs).at[i], 2 * destination(i) + column)
        elif name == "stat":
            stat()
        elif name == "statr":
            stats_in()
        elif name == "normo":
            normalize(0, res_v)
        else:
            normalize_peer()

    mine = pl.ds(pl.multiple_of(d * width, width), width)
    upper = pl.ds(pl.multiple_of(half + d * width, width), width)

    def slab_source(name):
        slot = 0 if name[1] == "o" else 1
        if name[0] == "a":
            value = attn_s[d] if slot == 0 else attn_y[d]
        else:
            value = jnp.where(swap, norm_o[slot, :, upper], norm_o[slot, :, mine])
        return jnp.where(owned, value, jnp.zeros_like(value))

    tall = rows // 2
    low = rows // line

    def light(uc, name):
        def slab(unit):
            return slab_o.at[0 if unit[0] == "a" else 1, 0 if unit[1] == "o" else 1]

        def half_of(unit, column):
            return slab(unit).at[pl.ds(pl.multiple_of(column * tall, tall), tall)]

        def quarter_of(unit, to):
            return slab(unit).at[to * low : (to + 1) * low]

        def place(source, column, b):
            spot = jnp.where(d == 0, source, near - 1 - source) * 2 + column
            return rot_o.at[b, :, pl.ds(pl.multiple_of(spot * share, share), share)]

        def gather(source, b, way, device):
            name = "g" + str(source) + str(b)
            where = place(source, x, b)
            return remote(own_o.at[b] if uc == source else where, where, name + way, name, device)

        if name == "res":
            post(uc, res)
        elif name == "A2":
            post(uc, a2)
        elif name == "B":
            post(uc, b2)
        elif name == "lift2s":

            @pl.when(s == 0)
            def _():
                res().wait_recv()
                lift(1, res_y).start()

        elif name == "pc":
            post(uc, pc)
        elif name[:2] == "xs":
            i = int(name[2:])
            post(uc, lambda: remote(xs.at[i], xr.at[i], "x" + str(i), "x" + str(i), x_peer))
        elif name[0] == "I":
            i = int(name[1:])
            to = order[uc][i]
            remote(xs.at[i], xr.at[i], "x" + str(i), "x" + str(i), x_peer).wait_recv()
            parts = [zs.at[i], xr.at[i]]
            if to >= uc and uc > 0:
                remote(zs.at[i], onto.at[to], "zs" + str(i), "L" + str(to), outward).wait_recv()
                parts.append(onto.at[to])
            if to <= uc and uc < line - 1:
                remote(zs.at[i], into.at[to], "zs" + str(i), "R" + str(to), inner).wait_recv()
                parts.append(into.at[to])
            if to == uc:
                combine(own_o.at[0], parts, rows, bf16)
            else:
                combine(zs.at[i], parts, rows)
            if to > uc:
                post(uc, lambda: remote(zs.at[i], onto.at[to], "zs" + str(i), "L" + str(to), outward))
            if to < uc:
                post(uc, lambda: remote(zs.at[i], into.at[to], "zs" + str(i), "R" + str(to), inner))
        elif name[:2] == "GX":
            source, b = int(name[2]), int(name[3])
            where, key = place(source, x, b), "gx" + name[2:]
            post(uc, lambda: remote(place(source, x, b), place(source, x, b), key, key, x_peer))
        elif name[0] == "G":
            source, b = int(name[1]), int(name[2])
            if uc == source:
                if b == 1:
                    pc().wait_recv()
            else:
                gather(source, b, "o", outward).wait_recv()
            if uc >= source and uc < line - 1:
                post(uc, lambda: gather(source, b, "o", outward))
            if uc <= source and uc > 0:
                post(uc, lambda: gather(source, b, "i", inner))
            if uc == source:
                combine(place(source, x, b), [own_o.at[b]], rows)
        else:
            slabs(uc, name, half_of, quarter_of)

    def slabs(uc, name, half_of, quarter_of):
        unit = next(k for k in UNITS if k in name)
        kind, rest = name.split(unit)
        k = UNITS.index(unit)

        def cross():
            return remote(sl_s.at[k], sl_x.at[k], "S" + unit, "S" + unit, x_peer)

        def flood(way):
            key = "fo" if way == 0 else "fi"
            device = outward if way == 0 else inner
            return remote(fl_s.at[k, way], fl_r.at[k, way], key + unit, key + unit, device)

        def back():
            return remote(half_of(unit, x), half_of(unit, x), "b" + unit, "b" + unit, x_peer)

        def reduce(to):
            key = "r" + unit + str(to)
            if to > uc:
                return remote(qt_s.at[k, to], qt_o.at[k, to], key, key + "o", outward)
            if to < uc:
                return remote(qt_s.at[k, to], qt_i.at[k, to], key, key + "i", inner)
            return remote(qt_s.at[k, to], qt_x.at[k], key, "rx" + unit, x_peer)

        def wave(source, way, device):
            key = "w" + unit + str(source)
            return remote(quarter_of(unit, source), quarter_of(unit, source), key + way, key, device)

        if unit in HALVED:
            if kind == "S":
                if unit == "ap":
                    q0().wait_recv()
                value = slab_source(unit)
                first, second = value[:tall], value[tall:]
                sl_k[k] = jnp.where(x == 0, first, second)
                sl_s[k] = jnp.where(x == 0, second, first)
                post(uc, cross)
            elif kind == "P":
                cross().wait_recv()
                combine(sl_p.at[k], [sl_k.at[k], sl_x.at[k]], tall)
            elif kind == "fo":
                parts = [sl_p.at[k]]
                if uc > 0:
                    flood(0).wait_recv()
                    parts.append(fl_r.at[k, 0])
                combine(fl_s.at[k, 0], parts, tall)
                post(uc, lambda: flood(0))
            elif kind == "fi":
                parts = [sl_p.at[k]]
                if uc < line - 1:
                    flood(1).wait_recv()
                    parts.append(fl_r.at[k, 1])
                combine(fl_s.at[k, 1], parts, tall)
                post(uc, lambda: flood(1))
            else:
                parts = [sl_p.at[k]]
                if uc > 0:
                    parts.append(fl_r.at[k, 0])
                    if uc == line - 1:
                        flood(0).wait_recv()
                if uc < line - 1:
                    parts.append(fl_r.at[k, 1])
                    if uc == 0:
                        flood(1).wait_recv()
                combine(half_of(unit, x), parts, tall)
                post(uc, back)
            return
        if kind == "S":
            if unit == "ap":
                q0().wait_recv()
            qt_f[k] = slab_source(unit)
        elif kind == "r":
            to = int(rest)
            parts = [qt_f.at[k, to * low : (to + 1) * low]]
            if to >= uc and uc > 0:
                remote(qt_s.at[k, to], qt_o.at[k, to], "r" + unit + rest, "r" + unit + rest + "o", outward).wait_recv()
                parts.append(qt_o.at[k, to])
            if to <= uc and uc < line - 1:
                remote(qt_s.at[k, to], qt_i.at[k, to], "r" + unit + rest, "r" + unit + rest + "i", inner).wait_recv()
                parts.append(qt_i.at[k, to])
            combine(qt_s.at[k, to], parts, low)
            post(uc, lambda: reduce(to))
        else:
            source = int(rest)
            if source == uc:
                reduce(uc).wait_recv()
                combine(quarter_of(unit, uc), [qt_s.at[k, uc], qt_x.at[k]], low)
            else:
                wave(source, "o", outward).wait_recv()
            if source <= uc and uc < line - 1:
                post(uc, lambda: wave(source, "o", outward))
            if source >= uc and uc > 0:
                post(uc, lambda: wave(source, "i", inner))

    steps = step_names(line, near)
    shared = [steps[i] for i in SHARED]
    parts = [segments([steps[i] for i in o], shared) for o in ORDERS]
    started = [False]
    for k, name in enumerate(shared + [None]):
        for uc in range(line):
            if parts[uc][k]:

                @pl.when(u == uc)
                def _():
                    for each in parts[uc][k]:
                        light(uc, each)

        if name is None:
            break
        if name[0] in "XO" and not started[0]:
            started[0] = True
            loads[2].wait()
        heavy(name)

    @pl.when(u >= near)
    def _():
        pc().wait_recv()

    combine(attn_o.at[0], [attn_v], rows)
    a2().wait_recv()
    b2().wait_recv()
    for k in range(4):
        here = slice(k * width, (k + 1) * width)
        attn_o[1, :, here] = jnp.where(swap, attn_y[(k + 2) % 4], attn_y[k])

    for unit in HALVED:
        k = UNITS.index(unit)
        m, b = 0 if unit[0] == "a" else 1, 0 if unit[1] == "o" else 1
        where = slab_o.at[m, b, pl.ds(pl.multiple_of((1 - x) * tall, tall), tall)]
        remote(where, where, "b" + unit, "b" + unit, x_peer).wait_recv()
    for source in range(near):
        for b in range(2):
            spot = jnp.where(d == 0, source, near - 1 - source) * 2 + 1 - x
            where = rot_o.at[b, :, pl.ds(pl.multiple_of(spot * share, share), share)]
            key = "gx" + str(source) + str(b)
            remote(where, where, key, key, x_peer).wait_recv()

    for make in sent[None]:
        make().wait_send()
    for uc in range(line):

        @pl.when(u == uc)
        def _():
            for make in sent[uc]:
                make().wait_send()

    @pl.when(s == 0)
    def _():
        lift(0, res_v).wait_send()
        lift(1, res_y).wait_send()


SEMAPHORES = 160


def exchanged(attn, res, ffn, base, signs, gain, flags, groups):
    n = lax.axis_size("tensor")
    rows, features = attn.shape
    share, width = BLK // n, HBLK // 2
    line = n // 2
    halved, units = len(UNITS), len(UNITS)
    f32, bf16 = jnp.float32, jnp.bfloat16
    vmem = pl.BlockSpec(memory_space=pltpu.VMEM)
    anywhere = pl.BlockSpec(memory_space=pl.ANY)
    return pl.pallas_call(
        functools.partial(exchange_kernel, n, groups),
        out_shape=[
            jax.ShapeDtypeStruct((2, rows, features), bf16),
            jax.ShapeDtypeStruct((2, rows, features), bf16),
            jax.ShapeDtypeStruct((2, 2, rows, width), bf16),
            jax.ShapeDtypeStruct((2, rows, BLK // 2), bf16),
            jax.ShapeDtypeStruct((2, rows, share), bf16),
        ],
        in_specs=[anywhere] * 3 + [vmem] * 3 + [pl.BlockSpec(memory_space=pltpu.SMEM)],
        out_specs=[vmem] * 5,
        scratch_shapes=[
            pltpu.VMEM((rows, features), bf16),
            pltpu.VMEM((rows, features), bf16),
            pltpu.VMEM(ffn.shape, bf16),
            pltpu.VMEM((4, rows, width), bf16),
            pltpu.VMEM((4, rows, width), bf16),
            pltpu.VMEM((rows, features), bf16),
            pltpu.VMEM((2, rows, features), bf16),
            pltpu.VMEM((line, rows, share), f32),
            pltpu.VMEM((line, rows, share), f32),
            pltpu.VMEM((line, rows, share), f32),
            pltpu.VMEM((line, rows, share), f32),
            pltpu.VMEM((line, rows, share), f32),
            pltpu.VMEM((rows, 128), f32),
            pltpu.VMEM((8, rows), f32),
            pltpu.VMEM((n, 8, rows), f32),
            pltpu.VMEM((8, rows), f32),
            pltpu.VMEM((8, rows), f32),
            pltpu.VMEM((2, rows, 128), f32),
            pltpu.VMEM((halved, rows // 2, width), bf16),
            pltpu.VMEM((halved, rows // 2, width), bf16),
            pltpu.VMEM((halved, rows // 2, width), bf16),
            pltpu.VMEM((halved, rows // 2, width), bf16),
            pltpu.VMEM((halved, 2, rows // 2, width), bf16),
            pltpu.VMEM((halved, 2, rows // 2, width), bf16),
            pltpu.VMEM((units, rows, width), bf16),
            pltpu.VMEM((units, line, rows // line, width), bf16),
            pltpu.VMEM((units, line, rows // line, width), bf16),
            pltpu.VMEM((units, line, rows // line, width), bf16),
            pltpu.VMEM((units, rows // line, width), bf16),
            pltpu.SemaphoreType.DMA((3,)),
            pltpu.SemaphoreType.DMA((SEMAPHORES,)),
            pltpu.SemaphoreType.DMA((SEMAPHORES,)),
        ],
        compiler_params=pltpu.CompilerParams(
            collective_id=2, has_side_effects=True, vmem_limit_bytes=60 << 20
        ),
    )(attn, res, ffn, base, signs, gain, flags)


def parity_sign(values):
    return (1 - 2 * (lax.population_count(values) & 1)).astype(jnp.float32)


def gram(left, right):
    return lax.dot_general(
        left, right, (((0,), (0,)), ((), ())), preferred_element_type=jnp.float32
    )


def general(residual_parts, attn_out, ffn_input, norm_gain, mixing, blocks):
    local_d = residual_parts.shape[2]
    local_f = ffn_input.shape[2]
    token_rows = residual_parts.shape[1]
    dp_count = lax.axis_size("dp")
    dp_member = lax.axis_index("dp")
    tensor_count = lax.axis_size("tensor")
    member = lax.axis_index("tensor")
    own_part = residual_parts[0]
    parts = gathered(own_part, "dp")
    attention = jnp.concatenate(gathered(attn_out[0], "dp"), axis=0)
    earlier = [passed_along(part, "section", 1) for part in parts]
    layers = [
        e.astype(jnp.float32) + p.astype(jnp.float32) for e, p in zip(earlier, parts)
    ]
    squares = jnp.sum(layers[0] * layers[0], axis=1).reshape(token_rows // 128, 128)

    a_local = local_f // KB
    order_a = a_local * tensor_count
    deep = GROUP * KB
    column = blocks[0, 1] * BLK + jnp.arange(BLK, dtype=jnp.int32)
    a_col, c_col = column // KB, column % KB
    pick = (jnp.arange(KB, dtype=jnp.int32)[:, None] == c_col[None, :]).astype(jnp.bfloat16)
    spread = jnp.dot(
        jnp.tile(mixing[0], (GROUP, 1)), pick, preferred_element_type=jnp.float32
    )
    row_a = jnp.arange(deep, dtype=jnp.int32) // KB
    base = (spread * parity_sign(row_a[:, None] & a_col[None, :])).astype(jnp.bfloat16)
    term = None
    for g in range(a_local // GROUP):
        sign = parity_sign((member * a_local + g * GROUP) & a_col) / math.sqrt(order_a)
        piece = jnp.dot(
            ffn_input[0, :, g * deep : (g + 1) * deep], base, preferred_element_type=jnp.float32
        )
        piece = piece * sign[None, :]
        term = piece if term is None else term + piece

    rotated, square_own = tensor_sum(term, squares, 0)

    square_total = gathered(square_own, "dp")
    rotated, square_total = lax.optimization_barrier((rotated, square_total))
    square_total = [s.reshape(token_rows) for s in square_total]
    share = BLK // tensor_count
    own_cols = lax.dynamic_slice_in_dim(rotated, member * share, share, 1)
    part_down = gram(own_cols, rotated)
    half = BLK // dp_count
    if dp_count == 2:
        kept = lax.dynamic_slice_in_dim(part_down, dp_member * half, half, 1)
        sent = lax.dynamic_slice_in_dim(part_down, (1 - dp_member) * half, half, 1)
        sum_down = kept + shifted(sent, "dp", 1)
    else:
        sum_down = lax.psum_scatter(part_down, "dp", scatter_dimension=1, tiled=True)

    normed = jnp.concatenate(
        [
            (x * lax.rsqrt(s / D + EPS)[:, None] * norm_gain[0][None, :]).astype(jnp.bfloat16)
            for x, s in zip(layers, square_total)
        ],
        axis=0,
    )
    first_col = blocks[0, 0] * HBLK
    width = HBLK // dp_count
    offset = first_col % local_d + dp_member * width
    owned = first_col // local_d == member
    slab = jnp.concatenate(
        [
            lax.dynamic_slice_in_dim(normed, offset, width, 1),
            lax.dynamic_slice_in_dim(attention, offset, width, 1),
        ],
        axis=0,
    )
    slab = jnp.where(owned, slab, 0).astype(jnp.bfloat16)
    (got,) = tensor_sum(slab, None, 1)
    tokens = token_rows * dp_count
    scale = 2.0 / tokens
    hess_in = (scale * gram(normed, got[:tokens]))[None]
    hess_o = (scale * gram(attention, got[tokens:]))[None]
    hess_down = (scale * sum_down)[None]
    return (hess_in, hess_o, hess_down)


def paired(residual_parts, attn_out, ffn_input, norm_gain, mixing, blocks):
    local_d = residual_parts.shape[2]
    local_f = ffn_input.shape[2]
    token_rows = residual_parts.shape[1]
    n = lax.axis_size("tensor")
    member = lax.axis_index("tensor")
    share = BLK // n
    a_local = local_f // KB
    groups = a_local // GROUP
    deep = GROUP * KB
    column = blocks[0, 1] * BLK + jnp.arange(BLK, dtype=jnp.int32)
    a_col, c_col = column // KB, column % KB
    pick = (jnp.arange(KB, dtype=jnp.int32)[:, None] == c_col[None, :]).astype(jnp.bfloat16)
    spread = jnp.dot(
        jnp.tile(mixing[0], (GROUP, 1)), pick, preferred_element_type=jnp.float32
    )
    row_a = jnp.arange(deep, dtype=jnp.int32) // KB
    base = (spread * parity_sign(row_a[:, None] & a_col[None, :])).astype(jnp.bfloat16)
    first_a = member * a_local + GROUP * jnp.arange(groups, dtype=jnp.int32)
    signs = parity_sign(first_a[:, None] & a_col[None, :]) / math.sqrt(a_local * n)
    signs = signs.reshape(groups, n, share).transpose(1, 0, 2)
    first_col = blocks[0, 0] * HBLK
    swap = (first_col % local_d) // HBLK
    owned = (first_col // local_d == member).astype(jnp.int32)
    flags = jnp.stack([swap, owned]).astype(jnp.int32)
    attention, normed, slab, rotated, own = exchanged(
        attn_out[0], residual_parts[0], ffn_input[0], base, signs, norm_gain, flags, groups
    )
    tokens = token_rows * 2
    scale = 2.0 / tokens
    attention, normed = attention.reshape(tokens, local_d), normed.reshape(tokens, local_d)
    slab = slab.reshape(2, tokens, HBLK // 2)
    hess_down = (scale * gram(own.reshape(tokens, share), rotated.reshape(tokens, BLK // 2)))[None]
    hess_in = (scale * gram(normed, slab[1]))[None]
    hess_o = (scale * gram(attention, slab[0]))[None]
    return (hess_in, hess_o, hess_down)


def local(*arguments):
    n = lax.axis_size("tensor")
    by_pairs = lax.axis_size("dp") == 2 and lax.axis_size("section") == 2 and n == 2 * len(ORDERS)
    if by_pairs and arguments[0].shape[2] == 2 * HBLK:
        return paired(*arguments)
    return general(*arguments)


def solution(mesh):
    return jax.shard_map(
        local,
        mesh=mesh,
        in_specs=(
            P("section", "dp", "tensor"),
            P("section", "dp", "tensor"),
            P("section", "dp", "tensor"),
            P("section", "tensor"),
            P("section", None, None),
            P("section", None),
        ),
        out_specs=(
            P("section", "tensor", "dp"),
            P("section", "tensor", "dp"),
            P("section", "tensor", "dp"),
        ),
        check_vma=False,
    )
```

```python
import functools
import math

import jax
import jax.numpy as jnp
from jax import lax
from jax.experimental import pallas as pl
from jax.experimental.pallas import tpu as pltpu
from jax.sharding import PartitionSpec as P

D = 16384
KB = 52
HBLK = 1024
BLK = 2048
GROUP = 32


EPS = 1e-05

MESH = pl.DeviceIdType.MESH


def passed_along(x, axis, by):
    devices = lax.axis_size(axis)
    pairs = [(i, i + by) for i in range(devices) if 0 <= i + by < devices]
    return lax.ppermute(x, axis, pairs)


def shifted(x, axis, by):
    devices = lax.axis_size(axis)
    return lax.ppermute(x, axis, [(i, (i + by) % devices) for i in range(devices)])


def gathered(x, axis):
    return [x] + [shifted(x, axis, by) for by in range(1, lax.axis_size(axis))]


def reduce_kernel(n, extras, *refs):
    x_ref, refs = refs[0], refs[1:]
    e_ref, refs = (refs[0], refs[1:]) if extras else (None, refs)
    out_ref, refs = refs[0], refs[1:]
    eout_ref, refs = (refs[0], refs[1:]) if extras else (None, refs)
    recv, mine, send_a, recv_a, send_b, recv_b = refs[:6]
    me = lax.axis_index("tensor")

    barrier = pltpu.get_barrier_semaphore()
    for k in range(1, n):
        pl.semaphore_signal(
            barrier, inc=1, device_id={"tensor": lax.rem(me + k, n)}, device_id_type=MESH
        )
    pl.semaphore_wait(barrier, n - 1)

    def remote(src, dst, send, receive, k):
        return pltpu.make_async_remote_copy(
            src_ref=src,
            dst_ref=dst,
            send_sem=send.at[k],
            recv_sem=receive.at[k],
            device_id={"tensor": lax.rem(me + k, n)},
            device_id_type=MESH,
        )

    order = sorted(range(1, n), key=lambda k: -min(k, n - k))
    extra = []
    if extras:
        erecv, send_e, recv_e = refs[6:]
        extra = [remote(e_ref, erecv.at[k], send_e, recv_e, k) for k in order]
    first = [remote(x_ref.at[lax.rem(me + k, n)], recv.at[k], send_a, recv_a, k) for k in order]
    for copy in extra + first:
        copy.start()
    if extras:
        for copy in extra:
            copy.wait()
        eout_ref[...] = e_ref[...] + functools.reduce(
            lambda a, k: a + erecv[k], range(2, n), erecv[1]
        )
    for copy in first:
        copy.wait()
    total = x_ref[me].astype(jnp.float32)
    for k in range(1, n):
        total = total + recv[k].astype(jnp.float32)
    mine[...] = total.astype(mine.dtype)
    out_ref[me] = total.astype(mine.dtype)
    partner = me + 1 - 2 * lax.rem(me, 2)
    half = n // 2

    def placed(src, slot, index, target):
        return pltpu.make_async_remote_copy(
            src_ref=src,
            dst_ref=out_ref.at[slot],
            send_sem=send_b.at[index],
            recv_sem=recv_b.at[index],
            device_id={"tensor": target},
            device_id_type=MESH,
        )

    ring = sorted(range(1, half), key=lambda k: -min(k, half - k))
    along = {k: placed(mine, me, k, lax.rem(me + 2 * k, n)) for k in ring}
    across = [placed(mine, me, 0, partner)]
    for copy in list(along.values()) + across:
        copy.start()
    for k in sorted(range(1, half), key=lambda k: min(k, half - k)):
        along[k].wait_recv()
        source = lax.rem(me + n - 2 * k, n)
        copy = placed(out_ref.at[source], source, half - 1 + k, partner)
        copy.start()
        across.append(copy)
    for copy in along.values():
        copy.wait_send()
    for copy in across:
        copy.wait()


def tensor_sum(x, extra, ident):
    n = lax.axis_size("tensor")
    rows, columns = x.shape
    x = x.reshape(n, rows // n, columns)
    vmem = pl.BlockSpec(memory_space=pltpu.VMEM)
    operands = [x] + ([extra] if extra is not None else [])
    shapes = [jax.ShapeDtypeStruct(x.shape, jnp.bfloat16)]
    scratch = [
        pltpu.VMEM(x.shape, x.dtype),
        pltpu.VMEM(x.shape[1:], jnp.bfloat16),
    ] + [pltpu.SemaphoreType.DMA((n,))] * 4
    if extra is not None:
        shapes.append(jax.ShapeDtypeStruct(extra.shape, extra.dtype))
        scratch += [pltpu.VMEM((n,) + extra.shape, extra.dtype)]
        scratch += [pltpu.SemaphoreType.DMA((n,))] * 2
    out = pl.pallas_call(
        functools.partial(reduce_kernel, n, extra is not None),
        out_shape=shapes,
        in_specs=[vmem] * len(operands),
        out_specs=[vmem] * len(shapes),
        scratch_shapes=scratch,
        compiler_params=pltpu.CompilerParams(
            collective_id=ident, has_side_effects=True, vmem_limit_bytes=32 << 20
        ),
        cost_estimate=pl.CostEstimate(flops=0, bytes_accessed=100 << 20, transcendentals=0),
    )(*operands)
    return [out[0].reshape(rows, columns)] + list(out[1:])


UNITS = ("ao", "no", "ap", "np")
HALVED = ("ao", "no", "ap", "np",)
SHARED = (
    9, 5, 10, 13, 6, 7, 11, 14, 12, 15, 16, 8,
)
ORDERS = (
    (
        33, 9, 17, 0, 5, 37, 41, 10, 18, 13, 6, 21, 7, 34, 11, 14, 19, 22, 12, 38, 15, 42, 20,
        16, 23, 1, 35, 49, 3, 39, 43, 8, 24, 4, 25, 29, 2, 36, 27, 31, 26, 30, 40, 44, 28, 32,
        50, 51, 52,
    ),
    (
        33, 9, 17, 0, 5, 37, 10, 18, 13, 6, 41, 7, 11, 34, 45, 14, 19, 12, 38, 21, 15, 20, 16,
        23, 1, 35, 22, 42, 49, 3, 24, 4, 39, 27, 31, 8, 36, 46, 2, 43, 50, 28, 25, 29, 47, 40,
        26, 30, 44, 32, 48, 51, 52,
    ),
    (
        33, 9, 17, 0, 5, 37, 10, 18, 13, 6, 45, 7, 11, 34, 41, 14, 19, 12, 38, 21, 15, 20, 16,
        23, 1, 35, 22, 46, 49, 3, 24, 4, 39, 8, 36, 42, 2, 50, 47, 27, 31, 40, 43, 51, 48, 28,
        32, 25, 29, 26, 30, 44, 52,
    ),
    (
        33, 9, 17, 0, 5, 37, 45, 10, 18, 13, 6, 21, 7, 34, 11, 14, 19, 22, 12, 38, 15, 46, 20,
        16, 23, 1, 35, 49, 3, 39, 47, 8, 24, 4, 36, 2, 50, 40, 48, 27, 31, 51, 28, 32, 25, 29,
        26, 30, 52,
    ),
)


def step_names(line, near):
    numbers = [str(i) for i in range(line)]
    pairs = [str(a) + str(b) for a in range(near) for b in range(2)]
    names = ["res", "A2", "B", "lift2s", "pc", "stat", "statr", "normo", "normp"]
    names += [k + i for k in ("X", "O", "xs", "I") for i in numbers]
    names += [k + p for k in ("G", "GX") for p in pairs]
    names += [k + unit for k in ("S", "P", "fo", "fi", "e") for unit in UNITS]
    return names + [k + unit + i for k in ("r", "v") for unit in UNITS for i in numbers]


def chosen(index, values):
    picked = jnp.int32(values[0])
    for place, value in enumerate(values[1:], 1):
        picked = jnp.where(index == place, jnp.int32(value), picked)
    return picked


def line_order(count):
    def edge(c):
        return min(c, count - 1 - c)

    return [
        sorted(range(count), key=lambda c: (-abs(c - z), edge(c))) for z in range(count)
    ]


def segments(order, shared):
    parts, rest = [], list(order)
    for heavy in shared:
        at = rest.index(heavy)
        parts.append(rest[:at])
        rest = rest[at + 1 :]
    return parts + [rest]


def exchange_kernel(n, groups, *refs):
    attn_h, res_h, ffn_h, gain, mixing, blocks = refs[:6]
    attn_o, norm_o, slab_a, slab_n, rot_o, own_o = refs[6:12]
    (
        attn_v, res_v, ffn_v, attn_s, attn_y, res_y, rc, xs, xr, zs, onto, into,
        sq_col, sq_s, sq_r, tot_s, tot_r, inv, sl_k, sl_s, sl_x, sl_p, fl_s, fl_r,
        qt_f, qt_s, qt_o, qt_i, qt_x, mix, pattern, flips, scaled, base,
        local_sem, send_sem, recv_sem,
    ) = refs[12:]
    rows, features = attn_v.shape
    deep = ffn_v.shape[1] // groups
    share = xs.shape[2]
    half = features // 2
    width = slab_a.shape[2]
    slab_o = (slab_a, slab_n)
    line = n // 2
    near = line // 2
    f32, bf16 = jnp.float32, jnp.bfloat16

    s = lax.axis_index("section")
    d = lax.axis_index("dp")
    t = lax.axis_index("tensor")
    z = t // 2
    x = t - 2 * z
    u = jnp.where(d == 0, z, line - 1 - z)
    toward = 2 - 4 * d
    outward = {"tensor": t + toward}
    inner = {"tensor": t - toward}
    x_peer = {"tensor": t + 1 - 2 * x}
    y_peer = {"dp": 1 - d}
    c_peer = {"section": 1 - s}
    order = line_order(line)
    names = {}

    def sem(name):
        return names.setdefault(name, len(names))

    def remote(source, target, send, receive, device):
        return pltpu.make_async_remote_copy(
            src_ref=source,
            dst_ref=target,
            send_sem=send_sem.at[sem(send)],
            recv_sem=recv_sem.at[sem(receive)],
            device_id=device,
            device_id_type=MESH,
        )

    sent = {}

    def post(uc, make):
        make().start()
        sent.setdefault(uc, []).append(make)

    def combine(target, parts, count, kind=None, strip=48):
        def step(b, carry):
            at = pl.ds(pl.multiple_of(b * strip, strip), strip)
            total = parts[0][at, :]
            for part in parts[1:]:
                total = total + part[at, :]
            target[at, :] = total if kind is None else total.astype(kind)
            return carry

        lax.fori_loop(0, count // strip, step, 0)

    loads = [
        pltpu.make_async_copy(a, b, local_sem.at[i])
        for i, (a, b) in enumerate([(attn_h, attn_v), (res_h, res_v), (ffn_h, ffn_v)])
    ]
    for copy in loads:
        copy.start()

    barrier = pltpu.get_barrier_semaphore()
    others = [{"tensor": lax.rem(t + k, n)} for k in range(1, n)] + [y_peer, c_peer]
    for device in others:
        pl.semaphore_signal(barrier, inc=1, device_id=device, device_id_type=MESH)
    pl.semaphore_wait(barrier, n + 1)

    per = features // HBLK
    swap = lax.rem(blocks[0, 0], per) > 0
    owned = lax.div(blocks[0, 0], per) == t

    def q0():
        return remote(attn_s.at[1 - d], attn_y.at[1 - d], "q0", "q0", y_peer)

    def a2():
        return remote(attn_s.at[d], attn_y.at[d], "A2", "A2", y_peer)

    def b2():
        return remote(attn_s.at[2:4], attn_y.at[2:4], "B", "B", y_peer)

    def res():
        return remote(res_v, res_y, "res", "res", y_peer)

    def tot():
        return remote(tot_s, tot_r, "tot", "tot", y_peer)

    def pc():
        return remote(own_o.at[0], own_o.at[1], "pc", "pc", y_peer)

    def lift(slot, source):
        return remote(source, rc.at[slot], "lift" + str(slot), "lift" + str(slot), c_peer)

    loads[0].wait()
    for k in range(4):
        here = slice(k * width, (k + 1) * width)
        there = slice((k + 2) % 4 * width, ((k + 2) % 4 + 1) * width)
        attn_s[k] = jnp.where(swap, attn_v[:, there], attn_v[:, here])
    post(None, q0)
    loads[1].wait()

    @pl.when(s == 0)
    def _():
        lift(0, res_v).start()
        rc[...] = jnp.zeros_like(rc)

    def destination(i):
        flat = [order[a][i] for a in range(line)]
        to = chosen(u, flat)
        return jnp.where(d == 0, to, line - 1 - to)

    def setup():
        mix[...] = jnp.zeros_like(mix)
        mix[:KB, :KB] = mixing[0]
        row = lax.broadcasted_iota(jnp.int32, pattern.shape, 0)
        lane = lax.broadcasted_iota(jnp.int32, pattern.shape, 1)
        inside = jnp.bitwise_and(lane, ROOM - 1)
        hit = (row == (lane // ROOM) * KB + inside) & (inside < KB)
        pattern[...] = jnp.where(hit, 1.0, 0.0).astype(bf16)

    def odd(values):
        for shift in (8, 4, 2, 1):
            values = jnp.bitwise_xor(values, jnp.right_shift(values, shift))
        return (1 - 2 * jnp.bitwise_and(values, 1)).astype(f32)

    def rotate(target, j):
        lane = lax.broadcasted_iota(jnp.int32, (8, share), 1)
        column = blocks[0, 1] * BLK + j * share + lane
        a_col = ((column.astype(f32) + 0.5) / KB).astype(jnp.int32)
        c_col = column - a_col * KB
        depth = mix.shape[1]
        row = lax.broadcasted_iota(jnp.int32, (depth, share), 0)
        pick = jnp.where(row == c_col[:1, :], 1.0, 0.0).astype(bf16)
        mixed = jnp.dot(mix[...], pick, preferred_element_type=f32)
        for start in range(0, GROUP, 8):
            rank = start + lax.broadcasted_iota(jnp.int32, (8, share), 0)
            flips[start : start + 8, :] = odd(jnp.bitwise_and(rank, a_col))
        quad = pattern.shape[0] // KB

        def build(q, carry):
            for i in range(quad):
                flip = flips[pl.ds(q * quad + i, 1), :]
                scaled[i * ROOM : (i + 1) * ROOM, :] = (mixed * flip).astype(bf16)
            at = pl.ds(pl.multiple_of(q * quad * KB, 16), quad * KB)
            base[at, :] = jnp.dot(
                pattern[...], scaled[...], preferred_element_type=f32
            ).astype(bf16)
            return carry

        lax.fori_loop(0, GROUP // quad, build, 0)
        a_local = groups * GROUP

        def step(g, carry):
            at = pl.ds(pl.multiple_of(g * deep, 128), deep)
            part = jnp.dot(ffn_v[:, at], base[...], preferred_element_type=f32)
            sign = odd(jnp.bitwise_and(t * a_local + g * GROUP, a_col)) / math.sqrt(a_local * n)
            part = part * sign[:1, :]

            @pl.when(g == 0)
            def _():
                target[...] = part

            @pl.when(g > 0)
            def _():
                target[...] = target[...] + part

            return carry

        lax.fori_loop(0, groups, step, 0)

    strip = 64

    def stat():
        @pl.when(s > 0)
        def _():
            lift(0, res_v).wait_recv()

        def squares(b, carry):
            at = pl.ds(pl.multiple_of(b * strip, strip), strip)
            acc = jnp.zeros((strip, 128), f32)
            for c in range(features // 128):
                lanes = slice(c * 128, (c + 1) * 128)
                v = res_v[at, lanes].astype(f32) + rc[0, at, lanes].astype(f32)
                acc = acc + v * v
            sq_col[at, :] = jnp.broadcast_to(jnp.sum(acc, axis=1, keepdims=True), (strip, 128))
            return carry

        lax.fori_loop(0, rows // strip, squares, 0)
        sq_s[...] = jnp.transpose(sq_col[...])[:8, :]
        for i in range(1, n):
            post(None, functools.partial(stat_copy, i))

    def stat_copy(i):
        name = "stat" + str(i)
        return remote(sq_s, sq_r.at[i], name, name, {"tensor": lax.rem(t + i, n)})

    def inverse(slot, sums):
        spread = jnp.broadcast_to(sums[:1, :], (128, rows))
        inv[slot] = lax.rsqrt(jnp.transpose(spread) / (n * features) + EPS)

    def stats_in():
        total = sq_s[...]
        for i in range(1, n):
            stat_copy(i).wait_recv()
            total = total + sq_r[i]
        tot_s[...] = total
        post(None, tot)
        inverse(0, total)

    def normalize(slot, part):
        def step(b, carry):
            at = pl.ds(pl.multiple_of(b * strip, strip), strip)
            by = inv[slot, at, :]
            for c in range(features // 128):
                lanes = slice(c * 128, (c + 1) * 128)
                v = part[at, lanes].astype(f32) + rc[slot, at, lanes].astype(f32)
                norm_o[slot, at, lanes] = (v * by * gain[:, lanes]).astype(bf16)
            return carry

        lax.fori_loop(0, rows // strip, step, 0)

    def normalize_peer():
        tot().wait_recv()
        inverse(1, tot_r[...])

        @pl.when(s > 0)
        def _():
            res().wait_recv()
            lift(1, res_y).wait_recv()

        normalize(1, res_y)

    def heavy(name):
        if name[0] in "XO":
            i = int(name[1:])
            column = 1 - x if name[0] == "X" else x
            rotate((xs if name[0] == "X" else zs).at[i], 2 * destination(i) + column)
        elif name == "stat":
            stat()
        elif name == "statr":
            stats_in()
        elif name == "normo":
            normalize(0, res_v)
        else:
            normalize_peer()

    mine = pl.ds(pl.multiple_of(d * width, width), width)
    upper = pl.ds(pl.multiple_of(half + d * width, width), width)

    def slab_source(name):
        slot = 0 if name[1] == "o" else 1
        if name[0] == "a":
            value = attn_s[d] if slot == 0 else attn_y[d]
        else:
            value = jnp.where(swap, norm_o[slot, :, upper], norm_o[slot, :, mine])
        return jnp.where(owned, value, jnp.zeros_like(value))

    tall = rows // 2
    low = rows // line

    def light(uc, name):
        def slab(unit):
            return slab_o[0 if unit[0] == "a" else 1].at[0 if unit[1] == "o" else 1]

        def half_of(unit, column):
            return slab(unit).at[pl.ds(pl.multiple_of(column * tall, tall), tall)]

        def quarter_of(unit, to):
            return slab(unit).at[to * low : (to + 1) * low]

        def place(source, column, b):
            spot = jnp.where(d == 0, source, near - 1 - source) * 2 + column
            return rot_o.at[b, :, pl.ds(pl.multiple_of(spot * share, share), share)]

        def gather(source, b, way, device):
            name = "g" + str(source) + str(b)
            where = place(source, x, b)
            return remote(own_o.at[b] if uc == source else where, where, name + way, name, device)

        if name == "res":
            post(uc, res)
        elif name == "A2":
            post(uc, a2)
        elif name == "B":
            post(uc, b2)
        elif name == "lift2s":

            @pl.when(s == 0)
            def _():
                res().wait_recv()
                lift(1, res_y).start()

        elif name == "pc":
            post(uc, pc)
        elif name[:2] == "xs":
            i = int(name[2:])
            post(uc, lambda: remote(xs.at[i], xr.at[i], "x" + str(i), "x" + str(i), x_peer))
        elif name[0] == "I":
            i = int(name[1:])
            to = order[uc][i]
            remote(xs.at[i], xr.at[i], "x" + str(i), "x" + str(i), x_peer).wait_recv()
            parts = [zs.at[i], xr.at[i]]
            if to >= uc and uc > 0:
                remote(zs.at[i], onto.at[to], "zs" + str(i), "L" + str(to), outward).wait_recv()
                parts.append(onto.at[to])
            if to <= uc and uc < line - 1:
                remote(zs.at[i], into.at[to], "zs" + str(i), "R" + str(to), inner).wait_recv()
                parts.append(into.at[to])
            if to == uc:
                combine(own_o.at[0], parts, rows, bf16)
            else:
                combine(zs.at[i], parts, rows)
            if to > uc:
                post(uc, lambda: remote(zs.at[i], onto.at[to], "zs" + str(i), "L" + str(to), outward))
            if to < uc:
                post(uc, lambda: remote(zs.at[i], into.at[to], "zs" + str(i), "R" + str(to), inner))
        elif name[:2] == "GX":
            source, b = int(name[2]), int(name[3])
            where, key = place(source, x, b), "gx" + name[2:]
            post(uc, lambda: remote(place(source, x, b), place(source, x, b), key, key, x_peer))
        elif name[0] == "G":
            source, b = int(name[1]), int(name[2])
            if uc == source:
                if b == 1:
                    pc().wait_recv()
            else:
                gather(source, b, "o", outward).wait_recv()
            if uc >= source and uc < line - 1:
                post(uc, lambda: gather(source, b, "o", outward))
            if uc <= source and uc > 0:
                post(uc, lambda: gather(source, b, "i", inner))
            if uc == source:
                combine(place(source, x, b), [own_o.at[b]], rows)
        else:
            slabs(uc, name, half_of, quarter_of)

    def slabs(uc, name, half_of, quarter_of):
        unit = next(k for k in UNITS if k in name)
        kind, rest = name.split(unit)
        k = UNITS.index(unit)

        def cross():
            return remote(sl_s.at[k], sl_x.at[k], "S" + unit, "S" + unit, x_peer)

        def flood(way):
            key = "fo" if way == 0 else "fi"
            device = outward if way == 0 else inner
            return remote(fl_s.at[k, way], fl_r.at[k, way], key + unit, key + unit, device)

        def back():
            return remote(half_of(unit, x), half_of(unit, x), "b" + unit, "b" + unit, x_peer)

        def reduce(to):
            key = "r" + unit + str(to)
            if to > uc:
                return remote(qt_s.at[k, to], qt_o.at[k, to], key, key + "o", outward)
            if to < uc:
                return remote(qt_s.at[k, to], qt_i.at[k, to], key, key + "i", inner)
            return remote(qt_s.at[k, to], qt_x.at[k], key, "rx" + unit, x_peer)

        def wave(source, way, device):
            key = "w" + unit + str(source)
            return remote(quarter_of(unit, source), quarter_of(unit, source), key + way, key, device)

        if unit in HALVED:
            if kind == "S":
                if unit == "ap":
                    q0().wait_recv()
                value = slab_source(unit)
                first, second = value[:tall], value[tall:]
                sl_k[k] = jnp.where(x == 0, first, second)
                sl_s[k] = jnp.where(x == 0, second, first)
                post(uc, cross)
            elif kind == "P":
                cross().wait_recv()
                combine(sl_p.at[k], [sl_k.at[k], sl_x.at[k]], tall)
            elif kind == "fo":
                parts = [sl_p.at[k]]
                if uc > 0:
                    flood(0).wait_recv()
                    parts.append(fl_r.at[k, 0])
                combine(fl_s.at[k, 0], parts, tall)
                post(uc, lambda: flood(0))
            elif kind == "fi":
                parts = [sl_p.at[k]]
                if uc < line - 1:
                    flood(1).wait_recv()
                    parts.append(fl_r.at[k, 1])
                combine(fl_s.at[k, 1], parts, tall)
                post(uc, lambda: flood(1))
            else:
                parts = [sl_p.at[k]]
                if uc > 0:
                    parts.append(fl_r.at[k, 0])
                    if uc == line - 1:
                        flood(0).wait_recv()
                if uc < line - 1:
                    parts.append(fl_r.at[k, 1])
                    if uc == 0:
                        flood(1).wait_recv()
                combine(half_of(unit, x), parts, tall)
                post(uc, back)
            return
        if kind == "S":
            if unit == "ap":
                q0().wait_recv()
            qt_f[k] = slab_source(unit)
        elif kind == "r":
            to = int(rest)
            parts = [qt_f.at[k, to * low : (to + 1) * low]]
            if to >= uc and uc > 0:
                remote(qt_s.at[k, to], qt_o.at[k, to], "r" + unit + rest, "r" + unit + rest + "o", outward).wait_recv()
                parts.append(qt_o.at[k, to])
            if to <= uc and uc < line - 1:
                remote(qt_s.at[k, to], qt_i.at[k, to], "r" + unit + rest, "r" + unit + rest + "i", inner).wait_recv()
                parts.append(qt_i.at[k, to])
            combine(qt_s.at[k, to], parts, low)
            post(uc, lambda: reduce(to))
        else:
            source = int(rest)
            if source == uc:
                reduce(uc).wait_recv()
                combine(quarter_of(unit, uc), [qt_s.at[k, uc], qt_x.at[k]], low)
            else:
                wave(source, "o", outward).wait_recv()
            if source <= uc and uc < line - 1:
                post(uc, lambda: wave(source, "o", outward))
            if source >= uc and uc > 0:
                post(uc, lambda: wave(source, "i", inner))

    steps = step_names(line, near)
    shared = [steps[i] for i in SHARED]
    parts = [segments([steps[i] for i in o], shared) for o in ORDERS]
    started = [False]
    for k, name in enumerate(shared + [None]):
        for uc in range(line):
            if parts[uc][k]:

                @pl.when(u == uc)
                def _():
                    for each in parts[uc][k]:
                        light(uc, each)

        if name is None:
            break
        if name[0] in "XO" and not started[0]:
            started[0] = True
            setup()
            loads[2].wait()
        heavy(name)

    @pl.when(u >= near)
    def _():
        pc().wait_recv()

    combine(attn_o.at[0], [attn_v], rows)
    a2().wait_recv()
    b2().wait_recv()
    for k in range(4):
        here = slice(k * width, (k + 1) * width)
        attn_o[1, :, here] = jnp.where(swap, attn_y[(k + 2) % 4], attn_y[k])

    for unit in HALVED:
        k = UNITS.index(unit)
        m, b = 0 if unit[0] == "a" else 1, 0 if unit[1] == "o" else 1
        where = slab_o[m].at[b, pl.ds(pl.multiple_of((1 - x) * tall, tall), tall)]
        remote(where, where, "b" + unit, "b" + unit, x_peer).wait_recv()
    for source in range(near):
        for b in range(2):
            spot = jnp.where(d == 0, source, near - 1 - source) * 2 + 1 - x
            where = rot_o.at[b, :, pl.ds(pl.multiple_of(spot * share, share), share)]
            key = "gx" + str(source) + str(b)
            remote(where, where, key, key, x_peer).wait_recv()

    for make in sent[None]:
        make().wait_send()
    for uc in range(line):

        @pl.when(u == uc)
        def _():
            for make in sent[uc]:
                make().wait_send()

    @pl.when(s == 0)
    def _():
        lift(0, res_v).wait_send()
        lift(1, res_y).wait_send()


SEMAPHORES = 160
ROOM = 64


def exchanged(attn, res, ffn, gain, mixing, blocks):
    n = lax.axis_size("tensor")
    rows, features = attn.shape
    share, width = BLK // n, HBLK // 2
    line = n // 2
    groups = ffn.shape[1] // (GROUP * KB)
    halved = len(UNITS)
    units = 1 if len(HALVED) == len(UNITS) else len(UNITS)
    f32, bf16 = jnp.float32, jnp.bfloat16
    vmem = pl.BlockSpec(memory_space=pltpu.VMEM)
    anywhere = pl.BlockSpec(memory_space=pl.ANY)
    return pl.pallas_call(
        functools.partial(exchange_kernel, n, groups),
        out_shape=[
            jax.ShapeDtypeStruct((2, rows, features), bf16),
            jax.ShapeDtypeStruct((2, rows, features), bf16),
            jax.ShapeDtypeStruct((2, rows, width), bf16),
            jax.ShapeDtypeStruct((2, rows, width), bf16),
            jax.ShapeDtypeStruct((2, rows, BLK // 2), bf16),
            jax.ShapeDtypeStruct((2, rows, share), bf16),
        ],
        in_specs=[anywhere] * 3 + [vmem] * 2 + [pl.BlockSpec(memory_space=pltpu.SMEM)],
        out_specs=[vmem] * 6,
        scratch_shapes=[
            pltpu.VMEM((rows, features), bf16),
            pltpu.VMEM((rows, features), bf16),
            pltpu.VMEM(ffn.shape, bf16),
            pltpu.VMEM((4, rows, width), bf16),
            pltpu.VMEM((4, rows, width), bf16),
            pltpu.VMEM((rows, features), bf16),
            pltpu.VMEM((2, rows, features), bf16),
            pltpu.VMEM((line, rows, share), f32),
            pltpu.VMEM((line, rows, share), f32),
            pltpu.VMEM((line, rows, share), f32),
            pltpu.VMEM((line, rows, share), f32),
            pltpu.VMEM((line, rows, share), f32),
            pltpu.VMEM((rows, 128), f32),
            pltpu.VMEM((8, rows), f32),
            pltpu.VMEM((n, 8, rows), f32),
            pltpu.VMEM((8, rows), f32),
            pltpu.VMEM((8, rows), f32),
            pltpu.VMEM((2, rows, 128), f32),
            pltpu.VMEM((halved, rows // 2, width), bf16),
            pltpu.VMEM((halved, rows // 2, width), bf16),
            pltpu.VMEM((halved, rows // 2, width), bf16),
            pltpu.VMEM((halved, rows // 2, width), bf16),
            pltpu.VMEM((halved, 2, rows // 2, width), bf16),
            pltpu.VMEM((halved, 2, rows // 2, width), bf16),
            pltpu.VMEM((units, rows, width), bf16),
            pltpu.VMEM((units, line, rows // line, width), bf16),
            pltpu.VMEM((units, line, rows // line, width), bf16),
            pltpu.VMEM((units, line, rows // line, width), bf16),
            pltpu.VMEM((units, rows // line, width), bf16),
            pltpu.VMEM((ROOM, 128), bf16),
            pltpu.VMEM((4 * KB, 4 * ROOM), bf16),
            pltpu.VMEM((GROUP, share), f32),
            pltpu.VMEM((4 * ROOM, share), bf16),
            pltpu.VMEM((GROUP * KB, share), bf16),
            pltpu.SemaphoreType.DMA((3,)),
            pltpu.SemaphoreType.DMA((SEMAPHORES,)),
            pltpu.SemaphoreType.DMA((SEMAPHORES,)),
        ],
        compiler_params=pltpu.CompilerParams(
            collective_id=2, has_side_effects=True, vmem_limit_bytes=40 << 20
        ),
    )(attn, res, ffn, gain, mixing, blocks)


def parity_sign(values):
    return (1 - 2 * (lax.population_count(values) & 1)).astype(jnp.float32)


def gram(left, right):
    return lax.dot_general(
        left, right, (((0,), (0,)), ((), ())), preferred_element_type=jnp.float32
    )


def general(residual_parts, attn_out, ffn_input, norm_gain, mixing, blocks):
    local_d = residual_parts.shape[2]
    local_f = ffn_input.shape[2]
    token_rows = residual_parts.shape[1]
    dp_count = lax.axis_size("dp")
    dp_member = lax.axis_index("dp")
    tensor_count = lax.axis_size("tensor")
    member = lax.axis_index("tensor")
    own_part = residual_parts[0]
    parts = gathered(own_part, "dp")
    attention = jnp.concatenate(gathered(attn_out[0], "dp"), axis=0)
    earlier = [passed_along(part, "section", 1) for part in parts]
    layers = [
        e.astype(jnp.float32) + p.astype(jnp.float32) for e, p in zip(earlier, parts)
    ]
    squares = jnp.sum(layers[0] * layers[0], axis=1).reshape(token_rows // 128, 128)

    a_local = local_f // KB
    order_a = a_local * tensor_count
    deep = GROUP * KB
    column = blocks[0, 1] * BLK + jnp.arange(BLK, dtype=jnp.int32)
    a_col, c_col = column // KB, column % KB
    pick = (jnp.arange(KB, dtype=jnp.int32)[:, None] == c_col[None, :]).astype(jnp.bfloat16)
    spread = jnp.dot(
        jnp.tile(mixing[0], (GROUP, 1)), pick, preferred_element_type=jnp.float32
    )
    row_a = jnp.arange(deep, dtype=jnp.int32) // KB
    base = (spread * parity_sign(row_a[:, None] & a_col[None, :])).astype(jnp.bfloat16)
    term = None
    for g in range(a_local // GROUP):
        sign = parity_sign((member * a_local + g * GROUP) & a_col) / math.sqrt(order_a)
        piece = jnp.dot(
            ffn_input[0, :, g * deep : (g + 1) * deep], base, preferred_element_type=jnp.float32
        )
        piece = piece * sign[None, :]
        term = piece if term is None else term + piece

    rotated, square_own = tensor_sum(term, squares, 0)

    square_total = gathered(square_own, "dp")
    rotated, square_total = lax.optimization_barrier((rotated, square_total))
    square_total = [s.reshape(token_rows) for s in square_total]
    share = BLK // tensor_count
    own_cols = lax.dynamic_slice_in_dim(rotated, member * share, share, 1)
    part_down = gram(own_cols, rotated)
    half = BLK // dp_count
    if dp_count == 2:
        kept = lax.dynamic_slice_in_dim(part_down, dp_member * half, half, 1)
        sent = lax.dynamic_slice_in_dim(part_down, (1 - dp_member) * half, half, 1)
        sum_down = kept + shifted(sent, "dp", 1)
    else:
        sum_down = lax.psum_scatter(part_down, "dp", scatter_dimension=1, tiled=True)

    normed = jnp.concatenate(
        [
            (x * lax.rsqrt(s / D + EPS)[:, None] * norm_gain[0][None, :]).astype(jnp.bfloat16)
            for x, s in zip(layers, square_total)
        ],
        axis=0,
    )
    first_col = blocks[0, 0] * HBLK
    width = HBLK // dp_count
    offset = first_col % local_d + dp_member * width
    owned = first_col // local_d == member
    slab = jnp.concatenate(
        [
            lax.dynamic_slice_in_dim(normed, offset, width, 1),
            lax.dynamic_slice_in_dim(attention, offset, width, 1),
        ],
        axis=0,
    )
    slab = jnp.where(owned, slab, 0).astype(jnp.bfloat16)
    (got,) = tensor_sum(slab, None, 1)
    tokens = token_rows * dp_count
    scale = 2.0 / tokens
    hess_in = (scale * gram(normed, got[:tokens]))[None]
    hess_o = (scale * gram(attention, got[tokens:]))[None]
    hess_down = (scale * sum_down)[None]
    return (hess_in, hess_o, hess_down)


def paired(residual_parts, attn_out, ffn_input, norm_gain, mixing, blocks):
    local_d = residual_parts.shape[2]
    token_rows = residual_parts.shape[1]
    share = BLK // lax.axis_size("tensor")
    attention, normed, slab_a, slab_n, rotated, own = exchanged(
        attn_out[0], residual_parts[0], ffn_input[0], norm_gain, mixing, blocks
    )
    tokens = token_rows * 2
    scale = 2.0 / tokens
    attention, normed = attention.reshape(tokens, local_d), normed.reshape(tokens, local_d)
    slab_a, slab_n = slab_a.reshape(tokens, HBLK // 2), slab_n.reshape(tokens, HBLK // 2)
    hess_down = (scale * gram(own.reshape(tokens, share), rotated.reshape(tokens, BLK // 2)))[None]
    hess_in = (scale * gram(normed, slab_n))[None]
    hess_o = (scale * gram(attention, slab_a))[None]
    return (hess_in, hess_o, hess_down)


def local(*arguments):
    n = lax.axis_size("tensor")
    by_pairs = lax.axis_size("dp") == 2 and lax.axis_size("section") == 2 and n == 2 * len(ORDERS)
    if by_pairs and arguments[0].shape[2] == 2 * HBLK:
        return paired(*arguments)
    return general(*arguments)


def solution(mesh):
    return jax.shard_map(
        local,
        mesh=mesh,
        in_specs=(
            P("section", "dp", "tensor"),
            P("section", "dp", "tensor"),
            P("section", "dp", "tensor"),
            P("section", "tensor"),
            P("section", None, None),
            P("section", None),
        ),
        out_specs=(
            P("section", "tensor", "dp"),
            P("section", "tensor", "dp"),
            P("section", "tensor", "dp"),
        ),
        check_vma=False,
    )
```

```python
import functools
import math

import jax
import jax.numpy as jnp
from jax import lax
from jax.experimental import pallas as pl
from jax.experimental.pallas import tpu as pltpu
from jax.sharding import PartitionSpec as P

D = 16384
KB = 52
HBLK = 1024
BLK = 2048
GROUP = 32


EPS = 1e-05

MESH = pl.DeviceIdType.MESH


def passed_along(x, axis, by):
    devices = lax.axis_size(axis)
    pairs = [(i, i + by) for i in range(devices) if 0 <= i + by < devices]
    return lax.ppermute(x, axis, pairs)


def shifted(x, axis, by):
    devices = lax.axis_size(axis)
    return lax.ppermute(x, axis, [(i, (i + by) % devices) for i in range(devices)])


def gathered(x, axis):
    return [x] + [shifted(x, axis, by) for by in range(1, lax.axis_size(axis))]


def reduce_kernel(n, extras, *refs):
    x_ref, refs = refs[0], refs[1:]
    e_ref, refs = (refs[0], refs[1:]) if extras else (None, refs)
    out_ref, refs = refs[0], refs[1:]
    eout_ref, refs = (refs[0], refs[1:]) if extras else (None, refs)
    recv, mine, send_a, recv_a, send_b, recv_b = refs[:6]
    me = lax.axis_index("tensor")

    barrier = pltpu.get_barrier_semaphore()
    for k in range(1, n):
        pl.semaphore_signal(
            barrier, inc=1, device_id={"tensor": lax.rem(me + k, n)}, device_id_type=MESH
        )
    pl.semaphore_wait(barrier, n - 1)

    def remote(src, dst, send, receive, k):
        return pltpu.make_async_remote_copy(
            src_ref=src,
            dst_ref=dst,
            send_sem=send.at[k],
            recv_sem=receive.at[k],
            device_id={"tensor": lax.rem(me + k, n)},
            device_id_type=MESH,
        )

    order = sorted(range(1, n), key=lambda k: -min(k, n - k))
    extra = []
    if extras:
        erecv, send_e, recv_e = refs[6:]
        extra = [remote(e_ref, erecv.at[k], send_e, recv_e, k) for k in order]
    first = [remote(x_ref.at[lax.rem(me + k, n)], recv.at[k], send_a, recv_a, k) for k in order]
    for copy in extra + first:
        copy.start()
    if extras:
        for copy in extra:
            copy.wait()
        eout_ref[...] = e_ref[...] + functools.reduce(
            lambda a, k: a + erecv[k], range(2, n), erecv[1]
        )
    for copy in first:
        copy.wait()
    total = x_ref[me].astype(jnp.float32)
    for k in range(1, n):
        total = total + recv[k].astype(jnp.float32)
    mine[...] = total.astype(mine.dtype)
    out_ref[me] = total.astype(mine.dtype)
    partner = me + 1 - 2 * lax.rem(me, 2)
    half = n // 2

    def placed(src, slot, index, target):
        return pltpu.make_async_remote_copy(
            src_ref=src,
            dst_ref=out_ref.at[slot],
            send_sem=send_b.at[index],
            recv_sem=recv_b.at[index],
            device_id={"tensor": target},
            device_id_type=MESH,
        )

    ring = sorted(range(1, half), key=lambda k: -min(k, half - k))
    along = {k: placed(mine, me, k, lax.rem(me + 2 * k, n)) for k in ring}
    across = [placed(mine, me, 0, partner)]
    for copy in list(along.values()) + across:
        copy.start()
    for k in sorted(range(1, half), key=lambda k: min(k, half - k)):
        along[k].wait_recv()
        source = lax.rem(me + n - 2 * k, n)
        copy = placed(out_ref.at[source], source, half - 1 + k, partner)
        copy.start()
        across.append(copy)
    for copy in along.values():
        copy.wait_send()
    for copy in across:
        copy.wait()


def tensor_sum(x, extra, ident):
    n = lax.axis_size("tensor")
    rows, columns = x.shape
    x = x.reshape(n, rows // n, columns)
    vmem = pl.BlockSpec(memory_space=pltpu.VMEM)
    operands = [x] + ([extra] if extra is not None else [])
    shapes = [jax.ShapeDtypeStruct(x.shape, jnp.bfloat16)]
    scratch = [
        pltpu.VMEM(x.shape, x.dtype),
        pltpu.VMEM(x.shape[1:], jnp.bfloat16),
    ] + [pltpu.SemaphoreType.DMA((n,))] * 4
    if extra is not None:
        shapes.append(jax.ShapeDtypeStruct(extra.shape, extra.dtype))
        scratch += [pltpu.VMEM((n,) + extra.shape, extra.dtype)]
        scratch += [pltpu.SemaphoreType.DMA((n,))] * 2
    out = pl.pallas_call(
        functools.partial(reduce_kernel, n, extra is not None),
        out_shape=shapes,
        in_specs=[vmem] * len(operands),
        out_specs=[vmem] * len(shapes),
        scratch_shapes=scratch,
        compiler_params=pltpu.CompilerParams(
            collective_id=ident, has_side_effects=True, vmem_limit_bytes=32 << 20
        ),
        cost_estimate=pl.CostEstimate(flops=0, bytes_accessed=100 << 20, transcendentals=0),
    )(*operands)
    return [out[0].reshape(rows, columns)] + list(out[1:])


UNITS = ("ao", "no", "ap", "np")
HALVED = ("ao", "no", "ap", "np",)
CROSSED = ()
SHARED = (
    9, 5, 10, 13, 6, 7, 11, 14, 12, 15, 16, 8,
)
ORDERS = (
    (
        37, 9, 17, 0, 5, 41, 45, 10, 18, 13, 6, 21, 7, 38, 11, 14, 19, 22, 12, 42, 15, 46, 20,
        16, 23, 1, 39, 53, 3, 43, 47, 8, 24, 4, 25, 29, 2, 40, 27, 31, 26, 30, 44, 48, 28, 32,
        54, 55, 56,
    ),
    (
        37, 9, 17, 0, 5, 41, 10, 18, 13, 6, 45, 7, 11, 38, 49, 14, 19, 12, 42, 21, 15, 20, 16,
        23, 1, 39, 22, 46, 53, 3, 24, 4, 43, 27, 31, 8, 40, 50, 2, 47, 54, 28, 25, 29, 51, 44,
        26, 30, 48, 32, 52, 55, 56,
    ),
    (
        37, 9, 17, 0, 5, 41, 10, 18, 13, 6, 49, 7, 11, 38, 45, 14, 19, 12, 42, 21, 15, 20, 16,
        23, 1, 39, 22, 50, 53, 3, 24, 4, 43, 8, 40, 46, 2, 54, 51, 27, 31, 44, 47, 55, 52, 28,
        32, 25, 29, 26, 30, 48, 56,
    ),
    (
        37, 9, 17, 0, 5, 41, 49, 10, 18, 13, 6, 21, 7, 38, 11, 14, 19, 22, 12, 42, 15, 50, 20,
        16, 23, 1, 39, 53, 3, 43, 51, 8, 24, 4, 40, 2, 54, 44, 52, 27, 31, 55, 28, 32, 25, 29,
        26, 30, 56,
    ),
)


def step_names(line, near):
    numbers = [str(i) for i in range(line)]
    pairs = [str(a) + str(b) for a in range(near) for b in range(2)]
    names = ["res", "A2", "B", "lift2s", "pc", "stat", "statr", "normo", "normp"]
    names += [k + i for k in ("X", "O", "xs", "I") for i in numbers]
    names += [k + p for k in ("G", "GX", "H") for p in pairs]
    names += [k + unit for k in ("S", "P", "fo", "fi", "e") for unit in UNITS]
    return names + [k + unit + i for k in ("r", "v") for unit in UNITS for i in numbers]


def chosen(index, values):
    picked = jnp.int32(values[0])
    for place, value in enumerate(values[1:], 1):
        picked = jnp.where(index == place, jnp.int32(value), picked)
    return picked


def line_order(count):
    def edge(c):
        return min(c, count - 1 - c)

    return [
        sorted(range(count), key=lambda c: (-abs(c - z), edge(c))) for z in range(count)
    ]


def segments(order, shared):
    parts, rest = [], list(order)
    for heavy in shared:
        at = rest.index(heavy)
        parts.append(rest[:at])
        rest = rest[at + 1 :]
    return parts + [rest]


def exchange_kernel(n, groups, *refs):
    attn_h, res_h, ffn_h, gain_h, mixing_h, blocks_h = refs[:6]
    attn_o, norm_o, slab_a, slab_n, rot_o, own_o = refs[6:12]
    (
        attn_v, res_v, ffn_v, attn_s, attn_y, res_y, rc, xs, xr, zs, onto, into,
        sq_col, sq_s, sq_r, tot_s, tot_r, inv, sl_k, sl_s, sl_x, sl_p, fl_s, fl_r,
        gain, mixing, blocks, qt_f, qt_s, qt_o, qt_i, qt_x, mix, pattern, flips, scaled, base,
        local_sem, send_sem, recv_sem,
    ) = refs[12:]
    rows, features = attn_v.shape
    deep = ffn_v.shape[1] // groups
    share = xs.shape[2]
    half = features // 2
    width = slab_a.shape[2]
    slab_o = (slab_a, slab_n)
    line = n // 2
    near = line // 2
    f32, bf16 = jnp.float32, jnp.bfloat16

    s = lax.axis_index("section")
    d = lax.axis_index("dp")
    t = lax.axis_index("tensor")
    z = t // 2
    x = t - 2 * z
    u = jnp.where(d == 0, z, line - 1 - z)
    toward = 2 - 4 * d
    outward = {"tensor": t + toward}
    inner = {"tensor": t - toward}
    x_peer = {"tensor": t + 1 - 2 * x}
    y_peer = {"dp": 1 - d}
    c_peer = {"section": 1 - s}
    order = line_order(line)
    names = {}

    def sem(name):
        return names.setdefault(name, len(names))

    def remote(source, target, send, receive, device):
        return pltpu.make_async_remote_copy(
            src_ref=source,
            dst_ref=target,
            send_sem=send_sem.at[sem(send)],
            recv_sem=recv_sem.at[sem(receive)],
            device_id=device,
            device_id_type=MESH,
        )

    sent = {}

    def post(uc, make):
        make().start()
        sent.setdefault(uc, []).append(make)

    def combine(target, parts, count, kind=None, strip=48):
        def step(b, carry):
            at = pl.ds(pl.multiple_of(b * strip, strip), strip)
            total = parts[0][at, :]
            for part in parts[1:]:
                total = total + part[at, :]
            target[at, :] = total if kind is None else total.astype(kind)
            return carry

        lax.fori_loop(0, count // strip, step, 0)

    pairs = [(attn_h, attn_v), (res_h, res_v), (ffn_h, ffn_v)]
    pairs += [(gain_h, gain), (mixing_h, mixing), (blocks_h, blocks)]
    loads = [pltpu.make_async_copy(a, b, local_sem.at[i]) for i, (a, b) in enumerate(pairs)]
    for i in (5, 0, 1, 2, 3, 4):
        loads[i].start()

    barrier = pltpu.get_barrier_semaphore()
    others = [{"tensor": lax.rem(t + k, n)} for k in range(1, n)] + [y_peer, c_peer]
    for device in others:
        pl.semaphore_signal(barrier, inc=1, device_id=device, device_id_type=MESH)
    pl.semaphore_wait(barrier, n + 1)

    loads[5].wait()
    per = features // HBLK
    swap = lax.rem(blocks[0, 0], per) > 0
    owned = lax.div(blocks[0, 0], per) == t

    def q0():
        return remote(attn_s.at[1 - d], attn_y.at[1 - d], "q0", "q0", y_peer)

    def a2():
        return remote(attn_s.at[d], attn_y.at[d], "A2", "A2", y_peer)

    def b2():
        return remote(attn_s.at[2:4], attn_y.at[2:4], "B", "B", y_peer)

    def res():
        return remote(res_v, res_y, "res", "res", y_peer)

    def tot():
        return remote(tot_s, tot_r, "tot", "tot", y_peer)

    def pc():
        return remote(own_o.at[0], own_o.at[1], "pc", "pc", y_peer)

    def lift(slot, source):
        return remote(source, rc.at[slot], "lift" + str(slot), "lift" + str(slot), c_peer)

    loads[0].wait()
    for k in range(4):
        here = slice(k * width, (k + 1) * width)
        there = slice((k + 2) % 4 * width, ((k + 2) % 4 + 1) * width)
        attn_s[k] = jnp.where(swap, attn_v[:, there], attn_v[:, here])
    post(None, q0)
    loads[1].wait()

    @pl.when(s == 0)
    def _():
        lift(0, res_v).start()
        rc[...] = jnp.zeros_like(rc)

    def destination(i):
        flat = [order[a][i] for a in range(line)]
        to = chosen(u, flat)
        return jnp.where(d == 0, to, line - 1 - to)

    def setup():
        mix[...] = jnp.zeros_like(mix)
        mix[:KB, :KB] = mixing[0]
        row = lax.broadcasted_iota(jnp.int32, pattern.shape, 0)
        lane = lax.broadcasted_iota(jnp.int32, pattern.shape, 1)
        inside = jnp.bitwise_and(lane, ROOM - 1)
        hit = (row == (lane // ROOM) * KB + inside) & (inside < KB)
        pattern[...] = jnp.where(hit, 1.0, 0.0).astype(bf16)

    def odd(values):
        for shift in (8, 4, 2, 1):
            values = jnp.bitwise_xor(values, jnp.right_shift(values, shift))
        return (1 - 2 * jnp.bitwise_and(values, 1)).astype(f32)

    def rotate(target, j):
        lane = lax.broadcasted_iota(jnp.int32, (8, share), 1)
        column = blocks[0, 1] * BLK + j * share + lane
        a_col = ((column.astype(f32) + 0.5) / KB).astype(jnp.int32)
        c_col = column - a_col * KB
        depth = mix.shape[1]
        row = lax.broadcasted_iota(jnp.int32, (depth, share), 0)
        pick = jnp.where(row == c_col[:1, :], 1.0, 0.0).astype(bf16)
        mixed = jnp.dot(mix[...], pick, preferred_element_type=f32)
        for start in range(0, GROUP, 8):
            rank = start + lax.broadcasted_iota(jnp.int32, (8, share), 0)
            flips[start : start + 8, :] = odd(jnp.bitwise_and(rank, a_col))
        quad = pattern.shape[0] // KB

        def build(q, carry):
            for i in range(quad):
                flip = flips[pl.ds(q * quad + i, 1), :]
                scaled[i * ROOM : (i + 1) * ROOM, :] = (mixed * flip).astype(bf16)
            at = pl.ds(pl.multiple_of(q * quad * KB, 16), quad * KB)
            base[at, :] = jnp.dot(
                pattern[...], scaled[...], preferred_element_type=f32
            ).astype(bf16)
            return carry

        lax.fori_loop(0, GROUP // quad, build, 0)
        a_local = groups * GROUP

        def step(g, carry):
            at = pl.ds(pl.multiple_of(g * deep, 128), deep)
            part = jnp.dot(ffn_v[:, at], base[...], preferred_element_type=f32)
            sign = odd(jnp.bitwise_and(t * a_local + g * GROUP, a_col)) / math.sqrt(a_local * n)
            part = part * sign[:1, :]

            @pl.when(g == 0)
            def _():
                target[...] = part

            @pl.when(g > 0)
            def _():
                target[...] = target[...] + part

            return carry

        lax.fori_loop(0, groups, step, 0)

    strip = 64

    def stat():
        @pl.when(s > 0)
        def _():
            lift(0, res_v).wait_recv()

        def squares(b, carry):
            at = pl.ds(pl.multiple_of(b * strip, strip), strip)
            acc = jnp.zeros((strip, 128), f32)
            for c in range(features // 128):
                lanes = slice(c * 128, (c + 1) * 128)
                v = res_v[at, lanes].astype(f32) + rc[0, at, lanes].astype(f32)
                acc = acc + v * v
            sq_col[at, :] = jnp.broadcast_to(jnp.sum(acc, axis=1, keepdims=True), (strip, 128))
            return carry

        lax.fori_loop(0, rows // strip, squares, 0)
        sq_s[...] = jnp.transpose(sq_col[...])[:8, :]
        for i in range(1, n):
            post(None, functools.partial(stat_copy, i))

    def stat_copy(i):
        name = "stat" + str(i)
        return remote(sq_s, sq_r.at[i], name, name, {"tensor": lax.rem(t + i, n)})

    def inverse(slot, sums):
        spread = jnp.broadcast_to(sums[:1, :], (128, rows))
        inv[slot] = lax.rsqrt(jnp.transpose(spread) / (n * features) + EPS)

    def stats_in():
        total = sq_s[...]
        for i in range(1, n):
            stat_copy(i).wait_recv()
            total = total + sq_r[i]
        tot_s[...] = total
        post(None, tot)
        inverse(0, total)

    def normalize(slot, part):
        def step(b, carry):
            at = pl.ds(pl.multiple_of(b * strip, strip), strip)
            by = inv[slot, at, :]
            for c in range(features // 128):
                lanes = slice(c * 128, (c + 1) * 128)
                v = part[at, lanes].astype(f32) + rc[slot, at, lanes].astype(f32)
                norm_o[slot, at, lanes] = (v * by * gain[:, lanes]).astype(bf16)
            return carry

        lax.fori_loop(0, rows // strip, step, 0)

    def normalize_peer():
        tot().wait_recv()
        inverse(1, tot_r[...])

        @pl.when(s > 0)
        def _():
            res().wait_recv()
            lift(1, res_y).wait_recv()

        normalize(1, res_y)

    def heavy(name):
        if name[0] in "XO":
            i = int(name[1:])
            column = 1 - x if name[0] == "X" else x
            rotate((xs if name[0] == "X" else zs).at[i], 2 * destination(i) + column)
        elif name == "stat":
            stat()
        elif name == "statr":
            stats_in()
        elif name == "normo":
            normalize(0, res_v)
        else:
            normalize_peer()

    mine = pl.ds(pl.multiple_of(d * width, width), width)
    upper = pl.ds(pl.multiple_of(half + d * width, width), width)

    def slab_source(name):
        slot = 0 if name[1] == "o" else 1
        if name[0] == "a":
            value = attn_s[d] if slot == 0 else attn_y[d]
        else:
            value = jnp.where(swap, norm_o[slot, :, upper], norm_o[slot, :, mine])
        return jnp.where(owned, value, jnp.zeros_like(value))

    tall = rows // 2
    low = rows // line
    paired_up = set()

    def own_ready(uc, b):
        if b == 1 and uc not in paired_up:
            paired_up.add(uc)
            pc().wait_recv()

    def light(uc, name):
        def slab(unit):
            return slab_o[0 if unit[0] == "a" else 1].at[0 if unit[1] == "o" else 1]

        def half_of(unit, column):
            return slab(unit).at[pl.ds(pl.multiple_of(column * tall, tall), tall)]

        def quarter_of(unit, to):
            return slab(unit).at[to * low : (to + 1) * low]

        def place(source, column, b):
            spot = jnp.where(d == 0, source, near - 1 - source) * 2 + column
            return rot_o.at[b, :, pl.ds(pl.multiple_of(spot * share, share), share)]

        def shared_from(uc, source, b):
            return own_o.at[b] if uc == source else place(source, x, b)

        def gather(source, b, way, device):
            name = "g" + str(source) + str(b)
            where = place(source, x, b)
            return remote(shared_from(uc, source, b), where, name + way, name, device)

        if name == "res":
            post(uc, res)
        elif name == "A2":
            post(uc, a2)
        elif name == "B":
            post(uc, b2)
        elif name == "lift2s":

            @pl.when(s == 0)
            def _():
                res().wait_recv()
                lift(1, res_y).start()

        elif name == "pc":
            post(uc, pc)
        elif name[:2] == "xs":
            i = int(name[2:])
            post(uc, lambda: remote(xs.at[i], xr.at[i], "x" + str(i), "x" + str(i), x_peer))
        elif name[0] == "I":
            i = int(name[1:])
            to = order[uc][i]
            remote(xs.at[i], xr.at[i], "x" + str(i), "x" + str(i), x_peer).wait_recv()
            parts = [zs.at[i], xr.at[i]]
            if to >= uc and uc > 0:
                remote(zs.at[i], onto.at[to], "zs" + str(i), "L" + str(to), outward).wait_recv()
                parts.append(onto.at[to])
            if to <= uc and uc < line - 1:
                remote(zs.at[i], into.at[to], "zs" + str(i), "R" + str(to), inner).wait_recv()
                parts.append(into.at[to])
            if to == uc:
                combine(own_o.at[0], parts, rows, bf16)
            else:
                combine(zs.at[i], parts, rows)
            if to > uc:
                post(uc, lambda: remote(zs.at[i], onto.at[to], "zs" + str(i), "L" + str(to), outward))
            if to < uc:
                post(uc, lambda: remote(zs.at[i], into.at[to], "zs" + str(i), "R" + str(to), inner))
        elif name[:2] == "GX":
            source, b = int(name[2]), int(name[3])
            key = "gx" + name[2:]
            if b in CROSSED:
                own_ready(uc, b)
            post(uc, lambda: remote(shared_from(uc, source, b), place(source, x, b), key, key, x_peer))
        elif name[0] == "H":
            source, b = int(name[1]), int(name[2])
            where, key = place(source, 1 - x, b), "h" + name[1:]
            if uc == source:
                remote(where, where, "gx" + name[1:], "gx" + name[1:], x_peer).wait_recv()
            else:
                remote(where, where, key + "o", key, outward).wait_recv()

            def ahead(way, device):
                spot = place(source, 1 - x, b)
                return remote(spot, spot, key + way, key, device)

            if uc >= source and uc < line - 1:
                post(uc, lambda: ahead("o", outward))
            if uc <= source and uc > 0:
                post(uc, lambda: ahead("i", inner))
        elif name[0] == "G":
            source, b = int(name[1]), int(name[2])
            if uc == source:
                own_ready(uc, b)
            else:
                gather(source, b, "o", outward).wait_recv()
            if uc >= source and uc < line - 1:
                post(uc, lambda: gather(source, b, "o", outward))
            if uc <= source and uc > 0:
                post(uc, lambda: gather(source, b, "i", inner))
            if uc == source:
                combine(place(source, x, b), [own_o.at[b]], rows)
        else:
            slabs(uc, name, half_of, quarter_of)

    def slabs(uc, name, half_of, quarter_of):
        unit = next(k for k in UNITS if k in name)
        kind, rest = name.split(unit)
        k = UNITS.index(unit)

        def cross():
            return remote(sl_s.at[k], sl_x.at[k], "S" + unit, "S" + unit, x_peer)

        def flood(way):
            key = "fo" if way == 0 else "fi"
            device = outward if way == 0 else inner
            return remote(fl_s.at[k, way], fl_r.at[k, way], key + unit, key + unit, device)

        def back():
            return remote(half_of(unit, x), half_of(unit, x), "b" + unit, "b" + unit, x_peer)

        def reduce(to):
            key = "r" + unit + str(to)
            if to > uc:
                return remote(qt_s.at[k, to], qt_o.at[k, to], key, key + "o", outward)
            if to < uc:
                return remote(qt_s.at[k, to], qt_i.at[k, to], key, key + "i", inner)
            return remote(qt_s.at[k, to], qt_x.at[k], key, "rx" + unit, x_peer)

        def wave(source, way, device):
            key = "w" + unit + str(source)
            return remote(quarter_of(unit, source), quarter_of(unit, source), key + way, key, device)

        if unit in HALVED:
            if kind == "S":
                if unit == "ap":
                    q0().wait_recv()
                value = slab_source(unit)
                first, second = value[:tall], value[tall:]
                sl_k[k] = jnp.where(x == 0, first, second)
                sl_s[k] = jnp.where(x == 0, second, first)
                post(uc, cross)
            elif kind == "P":
                cross().wait_recv()
                combine(sl_p.at[k], [sl_k.at[k], sl_x.at[k]], tall)
            elif kind == "fo":
                parts = [sl_p.at[k]]
                if uc > 0:
                    flood(0).wait_recv()
                    parts.append(fl_r.at[k, 0])
                combine(fl_s.at[k, 0], parts, tall)
                post(uc, lambda: flood(0))
            elif kind == "fi":
                parts = [sl_p.at[k]]
                if uc < line - 1:
                    flood(1).wait_recv()
                    parts.append(fl_r.at[k, 1])
                combine(fl_s.at[k, 1], parts, tall)
                post(uc, lambda: flood(1))
            else:
                parts = [sl_p.at[k]]
                if uc > 0:
                    parts.append(fl_r.at[k, 0])
                    if uc == line - 1:
                        flood(0).wait_recv()
                if uc < line - 1:
                    parts.append(fl_r.at[k, 1])
                    if uc == 0:
                        flood(1).wait_recv()
                combine(half_of(unit, x), parts, tall)
                post(uc, back)
            return
        if kind == "S":
            if unit == "ap":
                q0().wait_recv()
            qt_f[k] = slab_source(unit)
        elif kind == "r":
            to = int(rest)
            parts = [qt_f.at[k, to * low : (to + 1) * low]]
            if to >= uc and uc > 0:
                remote(qt_s.at[k, to], qt_o.at[k, to], "r" + unit + rest, "r" + unit + rest + "o", outward).wait_recv()
                parts.append(qt_o.at[k, to])
            if to <= uc and uc < line - 1:
                remote(qt_s.at[k, to], qt_i.at[k, to], "r" + unit + rest, "r" + unit + rest + "i", inner).wait_recv()
                parts.append(qt_i.at[k, to])
            combine(qt_s.at[k, to], parts, low)
            post(uc, lambda: reduce(to))
        else:
            source = int(rest)
            if source == uc:
                reduce(uc).wait_recv()
                combine(quarter_of(unit, uc), [qt_s.at[k, uc], qt_x.at[k]], low)
            else:
                wave(source, "o", outward).wait_recv()
            if source <= uc and uc < line - 1:
                post(uc, lambda: wave(source, "o", outward))
            if source >= uc and uc > 0:
                post(uc, lambda: wave(source, "i", inner))

    steps = step_names(line, near)
    shared = [steps[i] for i in SHARED]
    parts = [segments([steps[i] for i in o], shared) for o in ORDERS]
    started = [False]
    for k, name in enumerate(shared + [None]):
        for uc in range(line):
            if parts[uc][k]:

                @pl.when(u == uc)
                def _():
                    for each in parts[uc][k]:
                        light(uc, each)

        if name is None:
            break
        if name[0] in "XO" and not started[0]:
            started[0] = True
            loads[3].wait()
            loads[4].wait()
            setup()
            loads[2].wait()
        heavy(name)

    @pl.when(u >= near)
    def _():
        pc().wait_recv()

    combine(attn_o.at[0], [attn_v], rows)
    a2().wait_recv()
    b2().wait_recv()
    for k in range(4):
        here = slice(k * width, (k + 1) * width)
        attn_o[1, :, here] = jnp.where(swap, attn_y[(k + 2) % 4], attn_y[k])

    for unit in HALVED:
        k = UNITS.index(unit)
        m, b = 0 if unit[0] == "a" else 1, 0 if unit[1] == "o" else 1
        where = slab_o[m].at[b, pl.ds(pl.multiple_of((1 - x) * tall, tall), tall)]
        remote(where, where, "b" + unit, "b" + unit, x_peer).wait_recv()
    for source in range(near):
        for b in set(range(2)) - set(CROSSED):
            spot = jnp.where(d == 0, source, near - 1 - source) * 2 + 1 - x
            where = rot_o.at[b, :, pl.ds(pl.multiple_of(spot * share, share), share)]
            key = "gx" + str(source) + str(b)
            remote(where, where, key, key, x_peer).wait_recv()

    for make in sent[None]:
        make().wait_send()
    for uc in range(line):

        @pl.when(u == uc)
        def _():
            for make in sent[uc]:
                make().wait_send()

    @pl.when(s == 0)
    def _():
        lift(0, res_v).wait_send()
        lift(1, res_y).wait_send()


SEMAPHORES = 160
ROOM = 64


def exchanged(*operands):
    attn, res, ffn, gain, mixing, blocks = operands
    n = lax.axis_size("tensor")
    rows, features = attn.shape
    share, width = BLK // n, HBLK // 2
    line = n // 2
    groups = ffn.shape[1] // (GROUP * KB)
    halved = len(UNITS)
    units = 1 if len(HALVED) == len(UNITS) else len(UNITS)
    f32, bf16 = jnp.float32, jnp.bfloat16
    vmem = pl.BlockSpec(memory_space=pltpu.VMEM)
    return pl.pallas_call(
        functools.partial(exchange_kernel, n, groups),
        out_shape=[
            jax.ShapeDtypeStruct((2, rows, features), bf16),
            jax.ShapeDtypeStruct((2, rows, features), bf16),
            jax.ShapeDtypeStruct((2, rows, width), bf16),
            jax.ShapeDtypeStruct((2, rows, width), bf16),
            jax.ShapeDtypeStruct((2, rows, BLK // 2), bf16),
            jax.ShapeDtypeStruct((2, rows, share), bf16),
        ],
        in_specs=[pl.BlockSpec(memory_space=pltpu.HBM)] * 6,
        out_specs=[vmem] * 6,
        scratch_shapes=[
            pltpu.VMEM((rows, features), bf16),
            pltpu.VMEM((rows, features), bf16),
            pltpu.VMEM(ffn.shape, bf16),
            pltpu.VMEM((4, rows, width), bf16),
            pltpu.VMEM((4, rows, width), bf16),
            pltpu.VMEM((rows, features), bf16),
            pltpu.VMEM((2, rows, features), bf16),
            pltpu.VMEM((line, rows, share), f32),
            pltpu.VMEM((line, rows, share), f32),
            pltpu.VMEM((line, rows, share), f32),
            pltpu.VMEM((line, rows, share), f32),
            pltpu.VMEM((line, rows, share), f32),
            pltpu.VMEM((rows, 128), f32),
            pltpu.VMEM((8, rows), f32),
            pltpu.VMEM((n, 8, rows), f32),
            pltpu.VMEM((8, rows), f32),
            pltpu.VMEM((8, rows), f32),
            pltpu.VMEM((2, rows, 128), f32),
            pltpu.VMEM((halved, rows // 2, width), bf16),
            pltpu.VMEM((halved, rows // 2, width), bf16),
            pltpu.VMEM((halved, rows // 2, width), bf16),
            pltpu.VMEM((halved, rows // 2, width), bf16),
            pltpu.VMEM((halved, 2, rows // 2, width), bf16),
            pltpu.VMEM((halved, 2, rows // 2, width), bf16),
            pltpu.VMEM(gain.shape, f32),
            pltpu.VMEM(mixing.shape, bf16),
            pltpu.SMEM(blocks.shape, jnp.int32),
            pltpu.VMEM((units, rows, width), bf16),
            pltpu.VMEM((units, line, rows // line, width), bf16),
            pltpu.VMEM((units, line, rows // line, width), bf16),
            pltpu.VMEM((units, line, rows // line, width), bf16),
            pltpu.VMEM((units, rows // line, width), bf16),
            pltpu.VMEM((ROOM, 128), bf16),
            pltpu.VMEM((4 * KB, 4 * ROOM), bf16),
            pltpu.VMEM((GROUP, share), f32),
            pltpu.VMEM((4 * ROOM, share), bf16),
            pltpu.VMEM((GROUP * KB, share), bf16),
            pltpu.SemaphoreType.DMA((6,)),
            pltpu.SemaphoreType.DMA((SEMAPHORES,)),
            pltpu.SemaphoreType.DMA((SEMAPHORES,)),
        ],
        compiler_params=pltpu.CompilerParams(
            collective_id=2, has_side_effects=True, vmem_limit_bytes=40 << 20
        ),
    )(*[pltpu.with_memory_space_constraint(v, pltpu.HBM) for v in operands])


def parity_sign(values):
    return (1 - 2 * (lax.population_count(values) & 1)).astype(jnp.float32)


def gram(left, right):
    return lax.dot_general(
        left, right, (((0,), (0,)), ((), ())), preferred_element_type=jnp.float32
    )


def general(residual_parts, attn_out, ffn_input, norm_gain, mixing, blocks):
    local_d = residual_parts.shape[2]
    local_f = ffn_input.shape[2]
    token_rows = residual_parts.shape[1]
    dp_count = lax.axis_size("dp")
    dp_member = lax.axis_index("dp")
    tensor_count = lax.axis_size("tensor")
    member = lax.axis_index("tensor")
    own_part = residual_parts[0]
    parts = gathered(own_part, "dp")
    attention = jnp.concatenate(gathered(attn_out[0], "dp"), axis=0)
    earlier = [passed_along(part, "section", 1) for part in parts]
    layers = [
        e.astype(jnp.float32) + p.astype(jnp.float32) for e, p in zip(earlier, parts)
    ]
    squares = jnp.sum(layers[0] * layers[0], axis=1).reshape(token_rows // 128, 128)

    a_local = local_f // KB
    order_a = a_local * tensor_count
    deep = GROUP * KB
    column = blocks[0, 1] * BLK + jnp.arange(BLK, dtype=jnp.int32)
    a_col, c_col = column // KB, column % KB
    pick = (jnp.arange(KB, dtype=jnp.int32)[:, None] == c_col[None, :]).astype(jnp.bfloat16)
    spread = jnp.dot(
        jnp.tile(mixing[0], (GROUP, 1)), pick, preferred_element_type=jnp.float32
    )
    row_a = jnp.arange(deep, dtype=jnp.int32) // KB
    base = (spread * parity_sign(row_a[:, None] & a_col[None, :])).astype(jnp.bfloat16)
    term = None
    for g in range(a_local // GROUP):
        sign = parity_sign((member * a_local + g * GROUP) & a_col) / math.sqrt(order_a)
        piece = jnp.dot(
            ffn_input[0, :, g * deep : (g + 1) * deep], base, preferred_element_type=jnp.float32
        )
        piece = piece * sign[None, :]
        term = piece if term is None else term + piece

    rotated, square_own = tensor_sum(term, squares, 0)

    square_total = gathered(square_own, "dp")
    rotated, square_total = lax.optimization_barrier((rotated, square_total))
    square_total = [s.reshape(token_rows) for s in square_total]
    share = BLK // tensor_count
    own_cols = lax.dynamic_slice_in_dim(rotated, member * share, share, 1)
    part_down = gram(own_cols, rotated)
    half = BLK // dp_count
    if dp_count == 2:
        kept = lax.dynamic_slice_in_dim(part_down, dp_member * half, half, 1)
        sent = lax.dynamic_slice_in_dim(part_down, (1 - dp_member) * half, half, 1)
        sum_down = kept + shifted(sent, "dp", 1)
    else:
        sum_down = lax.psum_scatter(part_down, "dp", scatter_dimension=1, tiled=True)

    normed = jnp.concatenate(
        [
            (x * lax.rsqrt(s / D + EPS)[:, None] * norm_gain[0][None, :]).astype(jnp.bfloat16)
            for x, s in zip(layers, square_total)
        ],
        axis=0,
    )
    first_col = blocks[0, 0] * HBLK
    width = HBLK // dp_count
    offset = first_col % local_d + dp_member * width
    owned = first_col // local_d == member
    slab = jnp.concatenate(
        [
            lax.dynamic_slice_in_dim(normed, offset, width, 1),
            lax.dynamic_slice_in_dim(attention, offset, width, 1),
        ],
        axis=0,
    )
    slab = jnp.where(owned, slab, 0).astype(jnp.bfloat16)
    (got,) = tensor_sum(slab, None, 1)
    tokens = token_rows * dp_count
    scale = 2.0 / tokens
    hess_in = (scale * gram(normed, got[:tokens]))[None]
    hess_o = (scale * gram(attention, got[tokens:]))[None]
    hess_down = (scale * sum_down)[None]
    return (hess_in, hess_o, hess_down)


def paired(residual_parts, attn_out, ffn_input, norm_gain, mixing, blocks):
    local_d = residual_parts.shape[2]
    token_rows = residual_parts.shape[1]
    share = BLK // lax.axis_size("tensor")
    attention, normed, slab_a, slab_n, rotated, own = exchanged(
        attn_out[0], residual_parts[0], ffn_input[0], norm_gain, mixing, blocks
    )
    tokens = token_rows * 2
    scale = 2.0 / tokens
    attention, normed = attention.reshape(tokens, local_d), normed.reshape(tokens, local_d)
    slab_a, slab_n = slab_a.reshape(tokens, HBLK // 2), slab_n.reshape(tokens, HBLK // 2)
    hess_down = (scale * gram(own.reshape(tokens, share), rotated.reshape(tokens, BLK // 2)))[None]
    hess_in = (scale * gram(normed, slab_n))[None]
    hess_o = (scale * gram(attention, slab_a))[None]
    return (hess_in, hess_o, hess_down)


def local(*arguments):
    n = lax.axis_size("tensor")
    by_pairs = lax.axis_size("dp") == 2 and lax.axis_size("section") == 2 and n == 2 * len(ORDERS)
    if by_pairs and arguments[0].shape[2] == 2 * HBLK:
        return paired(*arguments)
    return general(*arguments)


def solution(mesh):
    return jax.shard_map(
        local,
        mesh=mesh,
        in_specs=(
            P("section", "dp", "tensor"),
            P("section", "dp", "tensor"),
            P("section", "dp", "tensor"),
            P("section", "tensor"),
            P("section", None, None),
            P("section", None),
        ),
        out_specs=(
            P("section", "tensor", "dp"),
            P("section", "tensor", "dp"),
            P("section", "tensor", "dp"),
        ),
        check_vma=False,
    )
```

```python
import functools
import math

import jax
import jax.numpy as jnp
from jax import lax
from jax.experimental import pallas as pl
from jax.experimental.pallas import tpu as pltpu
from jax.sharding import PartitionSpec as P

D = 16384
KB = 52
HBLK = 1024
BLK = 2048
GROUP = 32


EPS = 1e-05

MESH = pl.DeviceIdType.MESH


def passed_along(x, axis, by):
    devices = lax.axis_size(axis)
    pairs = [(i, i + by) for i in range(devices) if 0 <= i + by < devices]
    return lax.ppermute(x, axis, pairs)


def shifted(x, axis, by):
    devices = lax.axis_size(axis)
    return lax.ppermute(x, axis, [(i, (i + by) % devices) for i in range(devices)])


def gathered(x, axis):
    return [x] + [shifted(x, axis, by) for by in range(1, lax.axis_size(axis))]


def reduce_kernel(n, extras, *refs):
    x_ref, refs = refs[0], refs[1:]
    e_ref, refs = (refs[0], refs[1:]) if extras else (None, refs)
    out_ref, refs = refs[0], refs[1:]
    eout_ref, refs = (refs[0], refs[1:]) if extras else (None, refs)
    recv, mine, send_a, recv_a, send_b, recv_b = refs[:6]
    me = lax.axis_index("tensor")

    barrier = pltpu.get_barrier_semaphore()
    for k in range(1, n):
        pl.semaphore_signal(
            barrier, inc=1, device_id={"tensor": lax.rem(me + k, n)}, device_id_type=MESH
        )
    pl.semaphore_wait(barrier, n - 1)

    def remote(src, dst, send, receive, k):
        return pltpu.make_async_remote_copy(
            src_ref=src,
            dst_ref=dst,
            send_sem=send.at[k],
            recv_sem=receive.at[k],
            device_id={"tensor": lax.rem(me + k, n)},
            device_id_type=MESH,
        )

    order = sorted(range(1, n), key=lambda k: -min(k, n - k))
    extra = []
    if extras:
        erecv, send_e, recv_e = refs[6:]
        extra = [remote(e_ref, erecv.at[k], send_e, recv_e, k) for k in order]
    first = [remote(x_ref.at[lax.rem(me + k, n)], recv.at[k], send_a, recv_a, k) for k in order]
    for copy in extra + first:
        copy.start()
    if extras:
        for copy in extra:
            copy.wait()
        eout_ref[...] = e_ref[...] + functools.reduce(
            lambda a, k: a + erecv[k], range(2, n), erecv[1]
        )
    for copy in first:
        copy.wait()
    total = x_ref[me].astype(jnp.float32)
    for k in range(1, n):
        total = total + recv[k].astype(jnp.float32)
    mine[...] = total.astype(mine.dtype)
    out_ref[me] = total.astype(mine.dtype)
    partner = me + 1 - 2 * lax.rem(me, 2)
    half = n // 2

    def placed(src, slot, index, target):
        return pltpu.make_async_remote_copy(
            src_ref=src,
            dst_ref=out_ref.at[slot],
            send_sem=send_b.at[index],
            recv_sem=recv_b.at[index],
            device_id={"tensor": target},
            device_id_type=MESH,
        )

    ring = sorted(range(1, half), key=lambda k: -min(k, half - k))
    along = {k: placed(mine, me, k, lax.rem(me + 2 * k, n)) for k in ring}
    across = [placed(mine, me, 0, partner)]
    for copy in list(along.values()) + across:
        copy.start()
    for k in sorted(range(1, half), key=lambda k: min(k, half - k)):
        along[k].wait_recv()
        source = lax.rem(me + n - 2 * k, n)
        copy = placed(out_ref.at[source], source, half - 1 + k, partner)
        copy.start()
        across.append(copy)
    for copy in along.values():
        copy.wait_send()
    for copy in across:
        copy.wait()


def tensor_sum(x, extra, ident):
    n = lax.axis_size("tensor")
    rows, columns = x.shape
    x = x.reshape(n, rows // n, columns)
    vmem = pl.BlockSpec(memory_space=pltpu.VMEM)
    operands = [x] + ([extra] if extra is not None else [])
    shapes = [jax.ShapeDtypeStruct(x.shape, jnp.bfloat16)]
    scratch = [
        pltpu.VMEM(x.shape, x.dtype),
        pltpu.VMEM(x.shape[1:], jnp.bfloat16),
    ] + [pltpu.SemaphoreType.DMA((n,))] * 4
    if extra is not None:
        shapes.append(jax.ShapeDtypeStruct(extra.shape, extra.dtype))
        scratch += [pltpu.VMEM((n,) + extra.shape, extra.dtype)]
        scratch += [pltpu.SemaphoreType.DMA((n,))] * 2
    out = pl.pallas_call(
        functools.partial(reduce_kernel, n, extra is not None),
        out_shape=shapes,
        in_specs=[vmem] * len(operands),
        out_specs=[vmem] * len(shapes),
        scratch_shapes=scratch,
        compiler_params=pltpu.CompilerParams(
            collective_id=ident, has_side_effects=True, vmem_limit_bytes=32 << 20
        ),
        cost_estimate=pl.CostEstimate(flops=0, bytes_accessed=100 << 20, transcendentals=0),
    )(*operands)
    return [out[0].reshape(rows, columns)] + list(out[1:])


UNITS = ("ao", "no", "ap", "np", "nq",)
HALVED = ("ao", "no", "ap", "np", "nq",)
DEFERRED = (3, 0,)
CROSSED = ()
SHARED = (
    10, 6, 14, 11, 15, 7, 8, 12, 16, 13, 17, 9,
)
ORDERS = (
    (
        1, 10, 26, 42, 6, 14, 22, 11, 19, 47, 15, 7, 8, 43, 12, 20, 52, 16, 23, 13, 17, 48, 53,
        0, 24, 29, 4, 2, 9, 46, 45, 44, 25, 30, 5, 34, 51, 56, 50, 55, 3, 62, 49, 32, 54, 36,
        31, 35, 66, 63, 33, 37, 65, 64,
    ),
    (
        1, 10, 42, 6, 14, 11, 47, 15, 26, 7, 8, 43, 12, 20, 16, 22, 13, 27, 21, 48, 17, 52, 0,
        23, 24, 4, 57, 62, 2, 53, 9, 46, 45, 44, 25, 51, 32, 36, 5, 50, 58, 3, 63, 30, 56, 49,
        34, 61, 55, 60, 33, 66, 54, 37, 31, 35, 59, 65, 64,
    ),
    (
        1, 10, 42, 6, 14, 11, 47, 15, 26, 7, 8, 43, 12, 20, 16, 22, 13, 27, 21, 48, 17, 57, 0,
        23, 24, 4, 52, 62, 2, 58, 9, 46, 45, 44, 25, 51, 5, 50, 53, 63, 3, 61, 60, 49, 32, 36,
        30, 34, 59, 56, 66, 55, 65, 33, 37, 54, 64, 31, 35,
    ),
    (
        1, 10, 26, 42, 6, 14, 22, 11, 19, 47, 15, 7, 8, 43, 12, 20, 57, 16, 23, 13, 17, 48, 58,
        0, 24, 29, 4, 2, 9, 46, 45, 44, 25, 5, 51, 61, 62, 50, 60, 3, 49, 59, 63, 32, 36, 30,
        34, 66, 65, 33, 37, 64, 31, 35,
    ),
)


def step_names(line, near):
    numbers = [str(i) for i in range(line)]
    pairs = [str(a) + str(b) for a in range(near) for b in range(2)]
    names = ["q0", "res", "A2", "B", "lift2s", "pc", "stat", "statr", "normo", "normp"]
    names += [k + i for k in ("X", "O", "xs", "I", "J") for i in numbers]
    names += [k + p for k in ("G", "GX", "H") for p in pairs]
    names += [k + unit for k in ("S", "P", "fo", "fi", "e") for unit in UNITS]
    return names + [k + unit + i for k in ("r", "v") for unit in UNITS for i in numbers]


def chosen(index, values):
    picked = values[0]
    for place, value in enumerate(values[1:], 1):
        picked = jnp.where(index == place, value, picked)
    return picked


def line_order(count):
    def edge(c):
        return min(c, count - 1 - c)

    return [
        sorted(range(count), key=lambda c: (-abs(c - z), edge(c))) for z in range(count)
    ]


def segments(order, shared):
    parts, rest = [], list(order)
    for heavy in shared:
        at = rest.index(heavy)
        parts.append(rest[:at])
        rest = rest[at + 1 :]
    return parts + [rest]


def exchange_kernel(n, groups, *refs):
    attn_h, res_h, ffn_h, gain_h, mixing_h, blocks_h = refs[:6]
    attn_o, norm_o, slab_a, slab_n, rot_o, own_o = refs[6:12]
    (
        attn_v, res_v, ffn_v, attn_s, attn_y, res_y, rc, xs, xr, zs, onto, into, onto_x, into_x,
        sq_col, sq_s, sq_r, tot_s, tot_r, inv, sl_k, sl_s, sl_x, sl_p, fl_s, fl_r,
        gain, mixing, blocks, qt_f, qt_s, qt_o, qt_i, qt_x, mix, pattern, flips, base,
        local_sem, send_sem, recv_sem,
    ) = refs[12:]
    rows, features = attn_v.shape
    deep = ffn_v.shape[1] // groups
    share = xs.shape[2]
    half = features // 2
    width = slab_a.shape[2]
    slab_o = (slab_a, slab_n)
    line = n // 2
    near = line // 2
    f32, bf16 = jnp.float32, jnp.bfloat16

    s = lax.axis_index("section")
    d = lax.axis_index("dp")
    t = lax.axis_index("tensor")
    z = t // 2
    x = t - 2 * z
    u = jnp.where(d == 0, z, line - 1 - z)
    toward = 2 - 4 * d
    outward = {"tensor": t + toward}
    inner = {"tensor": t - toward}
    x_peer = {"tensor": t + 1 - 2 * x}
    y_peer = {"dp": 1 - d}
    c_peer = {"section": 1 - s}
    order = line_order(line)
    names = {}

    def sem(name):
        return names.setdefault(name, len(names))

    def remote(source, target, send, receive, device):
        return pltpu.make_async_remote_copy(
            src_ref=source,
            dst_ref=target,
            send_sem=send_sem.at[sem(send)],
            recv_sem=recv_sem.at[sem(receive)],
            device_id=device,
            device_id_type=MESH,
        )

    sent = {}

    def post(uc, make):
        make().start()
        sent.setdefault(uc, []).append(make)

    def combine(target, parts, count, kind=None, strip=48):
        def step(b, carry):
            at = pl.ds(pl.multiple_of(b * strip, strip), strip)
            total = parts[0][at, :]
            for part in parts[1:]:
                total = total + part[at, :]
            target[at, :] = total if kind is None else total.astype(kind)
            return carry

        lax.fori_loop(0, count // strip, step, 0)

    pairs = [(attn_h, attn_v), (res_h, res_v), (ffn_h, ffn_v)]
    pairs += [(gain_h, gain), (mixing_h, mixing), (blocks_h, blocks)]
    loads = [pltpu.make_async_copy(a, b, local_sem.at[i]) for i, (a, b) in enumerate(pairs)]
    for i in (5, 0, 1, 2, 3, 4):
        loads[i].start()

    barrier = pltpu.get_barrier_semaphore()
    others = [{"tensor": lax.rem(t + k, n)} for k in range(1, n)] + [y_peer, c_peer]
    for device in others:
        pl.semaphore_signal(barrier, inc=1, device_id=device, device_id_type=MESH)
    pl.semaphore_wait(barrier, n + 1)

    loads[5].wait()
    per = features // HBLK
    swap = lax.rem(blocks[0, 0], per) > 0
    owned = lax.div(blocks[0, 0], per) == t

    def q0():
        return remote(attn_s.at[1 - d], attn_y.at[1 - d], "q0", "q0", y_peer)

    def a2():
        return remote(attn_s.at[d], attn_y.at[d], "A2", "A2", y_peer)

    def b2():
        return remote(attn_s.at[2:4], attn_y.at[2:4], "B", "B", y_peer)

    def res():
        return remote(res_h, res_y, "res", "res", y_peer)

    def tot():
        return remote(tot_s, tot_r, "tot", "tot", y_peer)

    def pc():
        return remote(own_o.at[0], own_o.at[1], "pc", "pc", y_peer)

    def lift(slot, source):
        return remote(source, rc.at[slot], "lift" + str(slot), "lift" + str(slot), c_peer)

    @pl.when(s == 0)
    def _():
        lift(0, res_h).start()
        rc[...] = jnp.zeros_like(rc)

    loads[0].wait()
    for k in range(4):
        here = slice(k * width, (k + 1) * width)
        there = slice((k + 2) % 4 * width, ((k + 2) % 4 + 1) * width)
        attn_s[k] = jnp.where(swap, attn_v[:, there], attn_v[:, here])

    def destination(i):
        flat = [order[a][i] for a in range(line)]
        to = chosen(u, flat)
        return jnp.where(d == 0, to, line - 1 - to)

    def setup():
        mix[...] = jnp.zeros_like(mix)
        mix[:KB, :KB] = mixing[0]
        row = lax.broadcasted_iota(jnp.int32, pattern.shape, 0)
        lane = lax.broadcasted_iota(jnp.int32, pattern.shape, 1)
        inside = jnp.bitwise_and(lane, ROOM - 1)
        hit = (row == (lane // ROOM) * KB + inside) & (inside < KB)
        pattern[...] = jnp.where(hit, 1.0, 0.0).astype(bf16)

    def odd(values):
        for shift in (8, 4, 2, 1):
            values = jnp.bitwise_xor(values, jnp.right_shift(values, shift))
        return (1 - 2 * jnp.bitwise_and(values, 1)).astype(f32)

    def rotate(target, j):
        lane = lax.broadcasted_iota(jnp.int32, (8, share), 1)
        column = blocks[0, 1] * BLK + j * share + lane
        a_col = ((column.astype(f32) + 0.5) / KB).astype(jnp.int32)
        c_col = column - a_col * KB
        depth = mix.shape[1]
        row = lax.broadcasted_iota(jnp.int32, (depth, share), 0)
        pick = jnp.where(row == c_col[:1, :], 1.0, 0.0).astype(bf16)
        mixed = jnp.dot(mix[...], pick, preferred_element_type=f32)
        for start in range(0, GROUP, 8):
            rank = start + lax.broadcasted_iota(jnp.int32, (8, share), 0)
            flips[start : start + 8, :] = odd(jnp.bitwise_and(rank, a_col))
        quad = pattern.shape[0] // KB

        for q in range(GROUP // quad):
            wide = [(mixed * flips[r : r + 1, :]).astype(bf16) for r in range(q * quad, (q + 1) * quad)]
            base[q * quad * KB : (q + 1) * quad * KB, :] = jnp.dot(
                pattern[...], jnp.concatenate(wide, axis=0), preferred_element_type=f32
            ).astype(bf16)
        a_local = groups * GROUP
        total = None
        for g in range(groups):
            part = jnp.dot(
                ffn_v[:, g * deep : (g + 1) * deep], base[...], preferred_element_type=f32
            )
            sign = odd(jnp.bitwise_and(t * a_local + g * GROUP, a_col)) / math.sqrt(a_local * n)
            part = part * sign[:1, :]
            total = part if total is None else total + part
        target[...] = total

    strip = 64

    def stat():
        loads[1].wait()

        @pl.when(s > 0)
        def _():
            lift(0, res_h).wait_recv()

        def squares(b, carry):
            at = pl.ds(pl.multiple_of(b * strip, strip), strip)
            acc = jnp.zeros((strip, 128), f32)
            for c in range(features // 128):
                lanes = slice(c * 128, (c + 1) * 128)
                v = res_v[at, lanes].astype(f32) + rc[0, at, lanes].astype(f32)
                acc = acc + v * v
            sq_col[at, :] = jnp.broadcast_to(jnp.sum(acc, axis=1, keepdims=True), (strip, 128))
            return carry

        lax.fori_loop(0, rows // strip, squares, 0)
        sq_s[...] = jnp.transpose(sq_col[...])[:8, :]
        for i in range(1, n):
            post(None, functools.partial(stat_copy, i))

    def stat_copy(i):
        name = "stat" + str(i)
        return remote(sq_s, sq_r.at[i], name, name, {"tensor": lax.rem(t + i, n)})

    def inverse(slot, sums):
        spread = jnp.broadcast_to(sums[:1, :], (128, rows))
        inv[slot] = lax.rsqrt(jnp.transpose(spread) / (n * features) + EPS)

    def stats_in():
        total = sq_s[...]
        for i in range(1, n):
            stat_copy(i).wait_recv()
            total = total + sq_r[i]
        tot_s[...] = total
        post(None, tot)
        inverse(0, total)

    def normalize(slot, part):
        def step(b, carry):
            at = pl.ds(pl.multiple_of(b * strip, strip), strip)
            by = inv[slot, at, :]
            for c in range(features // 128):
                lanes = slice(c * 128, (c + 1) * 128)
                v = part[at, lanes].astype(f32) + rc[slot, at, lanes].astype(f32)
                norm_o[slot, at, lanes] = (v * by * gain[:, lanes]).astype(bf16)
            return carry

        lax.fori_loop(0, rows // strip, step, 0)

    def normalize_peer():
        tot().wait_recv()
        inverse(1, tot_r[...])

        @pl.when(s > 0)
        def _():
            res().wait_recv()
            lift(1, res_y).wait_recv()

        normalize(1, res_y)

    def heavy(name):
        if name[0] in "XO":
            i = int(name[1:])
            column = 1 - x if name[0] == "X" else x
            rotate((xs if name[0] == "X" else zs).at[i], 2 * destination(i) + column)
        elif name == "stat":
            stat()
        elif name == "statr":
            stats_in()
        elif name == "normo":
            normalize(0, res_v)
        else:
            normalize_peer()

    mine = pl.ds(pl.multiple_of(d * width, width), width)
    upper = pl.ds(pl.multiple_of(half + d * width, width), width)

    def slab_source(name):
        slot = 0 if name[1] == "o" else 1
        start, count = span(name)
        at = slice(start, start + count)
        if name[0] == "a":
            value = attn_s[d, at] if slot == 0 else attn_y[d, at]
        else:
            value = jnp.where(swap, norm_o[slot, at, upper], norm_o[slot, at, mine])
        return jnp.where(owned, value, jnp.zeros_like(value))

    def span(unit):
        whole = unit[1] == "o" or unit[0] + "q" not in UNITS
        count = rows if whole else rows // 2
        return (rows // 2 if unit[1] == "q" else 0), count

    low = rows // line
    paired_up = set()

    def attn_ready(uc, unit):
        if unit[0] == "a" and unit[1] != "o" and ("q0", uc) not in paired_up:
            paired_up.add(("q0", uc))
            q0().wait_recv()

    def own_ready(uc, b):
        if b == 1 and uc not in paired_up:
            paired_up.add(uc)
            pc().wait_recv()

    def light(uc, name):
        def slab(unit):
            return slab_o[0 if unit[0] == "a" else 1].at[0 if unit[1] == "o" else 1]

        def half_of(unit, column):
            start, count = span(unit)
            tall = count // 2
            return slab(unit).at[pl.ds(pl.multiple_of(start + column * tall, tall), tall)]

        def quarter_of(unit, to):
            return slab(unit).at[to * low : (to + 1) * low]

        def place(source, column, b):
            spot = jnp.where(d == 0, source, near - 1 - source) * 2 + column
            return rot_o.at[b, :, pl.ds(pl.multiple_of(spot * share, share), share)]

        def shared_from(uc, source, b):
            return own_o.at[b] if uc == source else place(source, x, b)

        def gather(source, b, way, device):
            name = "g" + str(source) + str(b)
            where = place(source, x, b)
            return remote(shared_from(uc, source, b), where, name + way, name, device)

        if name == "q0":
            post(uc, q0)
        elif name == "res":
            post(uc, res)
        elif name == "A2":
            post(uc, a2)
        elif name == "B":
            post(uc, b2)
        elif name == "lift2s":

            @pl.when(s == 0)
            def _():
                res().wait_recv()
                lift(1, res_y).start()

        elif name == "pc":
            post(uc, pc)
        elif name[:2] == "xs":
            i = int(name[2:])
            post(uc, lambda: remote(xs.at[i], xr.at[i], "x" + str(i), "x" + str(i), x_peer))
        elif name[0] in "IJ":
            i = int(name[1:])
            to = order[uc][i]
            own = name[0] == "I"
            store = zs if own else xs
            held = store.at[i]
            parts = [held]

            def across():
                return remote(xs.at[i], xr.at[i], "x" + str(i), "x" + str(i), x_peer)

            def along(way):
                key = ("L" if way == 0 else "R") + ("" if own else "x") + str(to)
                slots = (onto if own else onto_x) if way == 0 else (into if own else into_x)
                send = ("zs" if own else "xs") + str(i)
                return remote(store.at[i], slots.at[to], send, key, outward if way == 0 else inner)

            if own and (to == uc or to not in DEFERRED):
                across().wait_recv()
                parts.append(xr.at[i])
            if to >= uc and uc > 0:
                along(0).wait_recv()
                parts.append((onto if own else onto_x).at[to])
            if to <= uc and uc < line - 1:
                along(1).wait_recv()
                parts.append((into if own else into_x).at[to])
            if own and to == uc:
                combine(own_o.at[0], parts, rows, bf16)
            elif len(parts) > 1:
                combine(held, parts, rows)
            if to > uc:
                post(uc, lambda: along(0))
            elif to < uc:
                post(uc, lambda: along(1))
            elif not own:
                post(uc, across)
        elif name[:2] == "GX":
            source, b = int(name[2]), int(name[3])
            key = "gx" + name[2:]
            if b in CROSSED:
                own_ready(uc, b)
            post(uc, lambda: remote(shared_from(uc, source, b), place(source, x, b), key, key, x_peer))
        elif name[0] == "H":
            source, b = int(name[1]), int(name[2])
            where, key = place(source, 1 - x, b), "h" + name[1:]
            if uc == source:
                remote(where, where, "gx" + name[1:], "gx" + name[1:], x_peer).wait_recv()
            else:
                remote(where, where, key + "o", key, outward).wait_recv()

            def ahead(way, device):
                spot = place(source, 1 - x, b)
                return remote(spot, spot, key + way, key, device)

            if uc >= source and uc < line - 1:
                post(uc, lambda: ahead("o", outward))
            if uc <= source and uc > 0:
                post(uc, lambda: ahead("i", inner))
        elif name[0] == "G":
            source, b = int(name[1]), int(name[2])
            if uc == source:
                own_ready(uc, b)
            else:
                gather(source, b, "o", outward).wait_recv()
            if uc >= source and uc < line - 1:
                post(uc, lambda: gather(source, b, "o", outward))
            if uc <= source and uc > 0:
                post(uc, lambda: gather(source, b, "i", inner))
            if uc == source:
                combine(place(source, x, b), [own_o.at[b]], rows)
        else:
            slabs(uc, name, half_of, quarter_of)

    def slabs(uc, name, half_of, quarter_of):
        unit = next(k for k in UNITS if k in name)
        kind, rest = name.split(unit)
        k = UNITS.index(unit)
        tall = span(unit)[1] // 2
        used = slice(0, tall)

        def cross():
            return remote(sl_s.at[k, used], sl_x.at[k, used], "S" + unit, "S" + unit, x_peer)

        def flood(way):
            key = "fo" if way == 0 else "fi"
            device = outward if way == 0 else inner
            return remote(fl_s.at[k, way, used], fl_r.at[k, way, used], key + unit, key + unit, device)

        def back():
            return remote(half_of(unit, x), half_of(unit, x), "b" + unit, "b" + unit, x_peer)

        def reduce(to):
            key = "r" + unit + str(to)
            if to > uc:
                return remote(qt_s.at[k, to], qt_o.at[k, to], key, key + "o", outward)
            if to < uc:
                return remote(qt_s.at[k, to], qt_i.at[k, to], key, key + "i", inner)
            return remote(qt_s.at[k, to], qt_x.at[k], key, "rx" + unit, x_peer)

        def wave(source, way, device):
            key = "w" + unit + str(source)
            return remote(quarter_of(unit, source), quarter_of(unit, source), key + way, key, device)

        if unit in HALVED:
            if kind == "S":
                attn_ready(uc, unit)
                value = slab_source(unit)
                first, second = value[:tall], value[tall:]
                sl_k[k, used] = jnp.where(x == 0, first, second)
                sl_s[k, used] = jnp.where(x == 0, second, first)
                post(uc, cross)
            elif kind == "P":
                cross().wait_recv()
                combine(sl_p.at[k], [sl_k.at[k], sl_x.at[k]], tall)
            elif kind == "fo":
                parts = [sl_p.at[k]]
                if uc > 0:
                    flood(0).wait_recv()
                    parts.append(fl_r.at[k, 0])
                combine(fl_s.at[k, 0], parts, tall)
                post(uc, lambda: flood(0))
            elif kind == "fi":
                parts = [sl_p.at[k]]
                if uc < line - 1:
                    flood(1).wait_recv()
                    parts.append(fl_r.at[k, 1])
                combine(fl_s.at[k, 1], parts, tall)
                post(uc, lambda: flood(1))
            else:
                parts = [sl_p.at[k]]
                if uc > 0:
                    parts.append(fl_r.at[k, 0])
                    if uc == line - 1:
                        flood(0).wait_recv()
                if uc < line - 1:
                    parts.append(fl_r.at[k, 1])
                    if uc == 0:
                        flood(1).wait_recv()
                combine(half_of(unit, x), parts, tall)
                post(uc, back)
            return
        if kind == "S":
            attn_ready(uc, unit)
            qt_f[k] = slab_source(unit)
        elif kind == "r":
            to = int(rest)
            parts = [qt_f.at[k, to * low : (to + 1) * low]]
            if to >= uc and uc > 0:
                remote(qt_s.at[k, to], qt_o.at[k, to], "r" + unit + rest, "r" + unit + rest + "o", outward).wait_recv()
                parts.append(qt_o.at[k, to])
            if to <= uc and uc < line - 1:
                remote(qt_s.at[k, to], qt_i.at[k, to], "r" + unit + rest, "r" + unit + rest + "i", inner).wait_recv()
                parts.append(qt_i.at[k, to])
            combine(qt_s.at[k, to], parts, low)
            post(uc, lambda: reduce(to))
        else:
            source = int(rest)
            if source == uc:
                reduce(uc).wait_recv()
                combine(quarter_of(unit, uc), [qt_s.at[k, uc], qt_x.at[k]], low)
            else:
                wave(source, "o", outward).wait_recv()
            if source <= uc and uc < line - 1:
                post(uc, lambda: wave(source, "o", outward))
            if source >= uc and uc > 0:
                post(uc, lambda: wave(source, "i", inner))

    steps = step_names(line, near)
    shared = [steps[i] for i in SHARED]
    parts = [segments([steps[i] for i in o], shared) for o in ORDERS]
    started = [False]
    for k, name in enumerate(shared + [None]):
        for uc in range(line):
            if parts[uc][k]:

                @pl.when(u == uc)
                def _():
                    for each in parts[uc][k]:
                        light(uc, each)

        if name is None:
            break
        if name[0] in "XO" and not started[0]:
            started[0] = True
            loads[3].wait()
            loads[4].wait()
            setup()
            loads[2].wait()
        heavy(name)

    @pl.when(u >= near)
    def _():
        pc().wait_recv()

    assert len(names) <= SEMAPHORES, len(names)

    combine(attn_o.at[0], [attn_v], rows)
    a2().wait_recv()
    b2().wait_recv()
    for k in range(4):
        here = slice(k * width, (k + 1) * width)
        attn_o[1, :, here] = jnp.where(swap, attn_y[(k + 2) % 4], attn_y[k])

    for unit in HALVED:
        m, b = 0 if unit[0] == "a" else 1, 0 if unit[1] == "o" else 1
        start, count = span(unit)
        tall = count // 2
        where = slab_o[m].at[b, pl.ds(pl.multiple_of(start + (1 - x) * tall, tall), tall)]
        remote(where, where, "b" + unit, "b" + unit, x_peer).wait_recv()
    for source in range(near):
        for b in set(range(2)) - set(CROSSED):
            spot = jnp.where(d == 0, source, near - 1 - source) * 2 + 1 - x
            where = rot_o.at[b, :, pl.ds(pl.multiple_of(spot * share, share), share)]
            key = "gx" + str(source) + str(b)
            remote(where, where, key, key, x_peer).wait_recv()

    for make in sent[None]:
        make().wait_send()
    for uc in range(line):

        @pl.when(u == uc)
        def _():
            for make in sent[uc]:
                make().wait_send()

    @pl.when(s == 0)
    def _():
        lift(0, res_h).wait_send()
        lift(1, res_y).wait_send()


SEMAPHORES = 192
ROOM = 64


def exchanged(*operands):
    attn, res, ffn, gain, mixing, blocks = operands
    n = lax.axis_size("tensor")
    rows, features = attn.shape
    share, width = BLK // n, HBLK // 2
    line = n // 2
    groups = ffn.shape[1] // (GROUP * KB)
    halved = len(UNITS)
    units = 1 if len(HALVED) == len(UNITS) else len(UNITS)
    f32, bf16 = jnp.float32, jnp.bfloat16
    vmem = pl.BlockSpec(memory_space=pltpu.VMEM)
    return pl.pallas_call(
        functools.partial(exchange_kernel, n, groups),
        out_shape=[
            jax.ShapeDtypeStruct((2, rows, features), bf16),
            jax.ShapeDtypeStruct((2, rows, features), bf16),
            jax.ShapeDtypeStruct((2, rows, width), bf16),
            jax.ShapeDtypeStruct((2, rows, width), bf16),
            jax.ShapeDtypeStruct((2, rows, BLK // 2), bf16),
            jax.ShapeDtypeStruct((2, rows, share), bf16),
        ],
        in_specs=[pl.BlockSpec(memory_space=pltpu.HBM)] * 6,
        out_specs=[vmem] * 6,
        scratch_shapes=[
            pltpu.VMEM((rows, features), bf16),
            pltpu.VMEM((rows, features), bf16),
            pltpu.VMEM(ffn.shape, bf16),
            pltpu.VMEM((4, rows, width), bf16),
            pltpu.VMEM((4, rows, width), bf16),
            pltpu.VMEM((rows, features), bf16),
            pltpu.VMEM((2, rows, features), bf16),
            pltpu.VMEM((line, rows, share), f32),
            pltpu.VMEM((line, rows, share), f32),
            pltpu.VMEM((line, rows, share), f32),
            pltpu.VMEM((line, rows, share), f32),
            pltpu.VMEM((line, rows, share), f32),
            pltpu.VMEM((line if DEFERRED else 1, rows, share), f32),
            pltpu.VMEM((line if DEFERRED else 1, rows, share), f32),
            pltpu.VMEM((rows, 128), f32),
            pltpu.VMEM((8, rows), f32),
            pltpu.VMEM((n, 8, rows), f32),
            pltpu.VMEM((8, rows), f32),
            pltpu.VMEM((8, rows), f32),
            pltpu.VMEM((2, rows, 128), f32),
            pltpu.VMEM((halved, rows // 2, width), bf16),
            pltpu.VMEM((halved, rows // 2, width), bf16),
            pltpu.VMEM((halved, rows // 2, width), bf16),
            pltpu.VMEM((halved, rows // 2, width), bf16),
            pltpu.VMEM((halved, 2, rows // 2, width), bf16),
            pltpu.VMEM((halved, 2, rows // 2, width), bf16),
            pltpu.VMEM(gain.shape, f32),
            pltpu.VMEM(mixing.shape, bf16),
            pltpu.SMEM(blocks.shape, jnp.int32),
            pltpu.VMEM((units, rows, width), bf16),
            pltpu.VMEM((units, line, rows // line, width), bf16),
            pltpu.VMEM((units, line, rows // line, width), bf16),
            pltpu.VMEM((units, line, rows // line, width), bf16),
            pltpu.VMEM((units, rows // line, width), bf16),
            pltpu.VMEM((ROOM, 128), bf16),
            pltpu.VMEM((4 * KB, 4 * ROOM), bf16),
            pltpu.VMEM((GROUP, share), f32),
            pltpu.VMEM((GROUP * KB, share), bf16),
            pltpu.SemaphoreType.DMA((6,)),
            pltpu.SemaphoreType.DMA((SEMAPHORES,)),
            pltpu.SemaphoreType.DMA((SEMAPHORES,)),
        ],
        compiler_params=pltpu.CompilerParams(
            collective_id=2, has_side_effects=True, vmem_limit_bytes=43 << 20
        ),
    )(*[pltpu.with_memory_space_constraint(v, pltpu.HBM) for v in operands])


def parity_sign(values):
    return (1 - 2 * (lax.population_count(values) & 1)).astype(jnp.float32)


def gram(left, right):
    return lax.dot_general(
        left, right, (((0,), (0,)), ((), ())), preferred_element_type=jnp.float32
    )


def general(residual_parts, attn_out, ffn_input, norm_gain, mixing, blocks):
    local_d = residual_parts.shape[2]
    local_f = ffn_input.shape[2]
    token_rows = residual_parts.shape[1]
    dp_count = lax.axis_size("dp")
    dp_member = lax.axis_index("dp")
    tensor_count = lax.axis_size("tensor")
    member = lax.axis_index("tensor")
    own_part = residual_parts[0]
    parts = gathered(own_part, "dp")
    attention = jnp.concatenate(gathered(attn_out[0], "dp"), axis=0)
    earlier = [passed_along(part, "section", 1) for part in parts]
    layers = [
        e.astype(jnp.float32) + p.astype(jnp.float32) for e, p in zip(earlier, parts)
    ]
    squares = jnp.sum(layers[0] * layers[0], axis=1).reshape(token_rows // 128, 128)

    a_local = local_f // KB
    order_a = a_local * tensor_count
    deep = GROUP * KB
    column = blocks[0, 1] * BLK + jnp.arange(BLK, dtype=jnp.int32)
    a_col, c_col = column // KB, column % KB
    pick = (jnp.arange(KB, dtype=jnp.int32)[:, None] == c_col[None, :]).astype(jnp.bfloat16)
    spread = jnp.dot(
        jnp.tile(mixing[0], (GROUP, 1)), pick, preferred_element_type=jnp.float32
    )
    row_a = jnp.arange(deep, dtype=jnp.int32) // KB
    base = (spread * parity_sign(row_a[:, None] & a_col[None, :])).astype(jnp.bfloat16)
    term = None
    for g in range(a_local // GROUP):
        sign = parity_sign((member * a_local + g * GROUP) & a_col) / math.sqrt(order_a)
        piece = jnp.dot(
            ffn_input[0, :, g * deep : (g + 1) * deep], base, preferred_element_type=jnp.float32
        )
        piece = piece * sign[None, :]
        term = piece if term is None else term + piece

    rotated, square_own = tensor_sum(term, squares, 0)

    square_total = gathered(square_own, "dp")
    rotated, square_total = lax.optimization_barrier((rotated, square_total))
    square_total = [s.reshape(token_rows) for s in square_total]
    share = BLK // tensor_count
    own_cols = lax.dynamic_slice_in_dim(rotated, member * share, share, 1)
    part_down = gram(own_cols, rotated)
    half = BLK // dp_count
    if dp_count == 2:
        kept = lax.dynamic_slice_in_dim(part_down, dp_member * half, half, 1)
        sent = lax.dynamic_slice_in_dim(part_down, (1 - dp_member) * half, half, 1)
        sum_down = kept + shifted(sent, "dp", 1)
    else:
        sum_down = lax.psum_scatter(part_down, "dp", scatter_dimension=1, tiled=True)

    normed = jnp.concatenate(
        [
            (x * lax.rsqrt(s / D + EPS)[:, None] * norm_gain[0][None, :]).astype(jnp.bfloat16)
            for x, s in zip(layers, square_total)
        ],
        axis=0,
    )
    first_col = blocks[0, 0] * HBLK
    width = HBLK // dp_count
    offset = first_col % local_d + dp_member * width
    owned = first_col // local_d == member
    slab = jnp.concatenate(
        [
            lax.dynamic_slice_in_dim(normed, offset, width, 1),
            lax.dynamic_slice_in_dim(attention, offset, width, 1),
        ],
        axis=0,
    )
    slab = jnp.where(owned, slab, 0).astype(jnp.bfloat16)
    (got,) = tensor_sum(slab, None, 1)
    tokens = token_rows * dp_count
    scale = 2.0 / tokens
    hess_in = (scale * gram(normed, got[:tokens]))[None]
    hess_o = (scale * gram(attention, got[tokens:]))[None]
    hess_down = (scale * sum_down)[None]
    return (hess_in, hess_o, hess_down)


def paired(residual_parts, attn_out, ffn_input, norm_gain, mixing, blocks):
    local_d = residual_parts.shape[2]
    token_rows = residual_parts.shape[1]
    share = BLK // lax.axis_size("tensor")
    attention, normed, slab_a, slab_n, rotated, own = exchanged(
        attn_out[0], residual_parts[0], ffn_input[0], norm_gain, mixing, blocks
    )
    tokens = token_rows * 2
    scale = 2.0 / tokens
    attention, normed = attention.reshape(tokens, local_d), normed.reshape(tokens, local_d)
    slab_a, slab_n = slab_a.reshape(tokens, HBLK // 2), slab_n.reshape(tokens, HBLK // 2)
    hess_down = (scale * gram(own.reshape(tokens, share), rotated.reshape(tokens, BLK // 2)))[None]
    hess_in = (scale * gram(normed, slab_n))[None]
    hess_o = (scale * gram(attention, slab_a))[None]
    return (hess_in, hess_o, hess_down)


def local(*arguments):
    n = lax.axis_size("tensor")
    by_pairs = lax.axis_size("dp") == 2 and lax.axis_size("section") == 2 and n == 2 * len(ORDERS)
    if by_pairs and arguments[0].shape[2] == 2 * HBLK:
        return paired(*arguments)
    return general(*arguments)


def solution(mesh):
    return jax.shard_map(
        local,
        mesh=mesh,
        in_specs=(
            P("section", "dp", "tensor"),
            P("section", "dp", "tensor"),
            P("section", "dp", "tensor"),
            P("section", "tensor"),
            P("section", None, None),
            P("section", None),
        ),
        out_specs=(
            P("section", "tensor", "dp"),
            P("section", "tensor", "dp"),
            P("section", "tensor", "dp"),
        ),
        check_vma=False,
    )
```

```python
import functools
import math

import jax
import jax.numpy as jnp
from jax import lax
from jax.experimental import pallas as pl
from jax.experimental.pallas import tpu as pltpu
from jax.sharding import PartitionSpec as P

D = 16384
KB = 52
HBLK = 1024
BLK = 2048
GROUP = 32


EPS = 1e-05

MESH = pl.DeviceIdType.MESH


def passed_along(x, axis, by):
    devices = lax.axis_size(axis)
    pairs = [(i, i + by) for i in range(devices) if 0 <= i + by < devices]
    return lax.ppermute(x, axis, pairs)


def shifted(x, axis, by):
    devices = lax.axis_size(axis)
    return lax.ppermute(x, axis, [(i, (i + by) % devices) for i in range(devices)])


def gathered(x, axis):
    return [x] + [shifted(x, axis, by) for by in range(1, lax.axis_size(axis))]


def reduce_kernel(n, extras, *refs):
    x_ref, refs = refs[0], refs[1:]
    e_ref, refs = (refs[0], refs[1:]) if extras else (None, refs)
    out_ref, refs = refs[0], refs[1:]
    eout_ref, refs = (refs[0], refs[1:]) if extras else (None, refs)
    recv, mine, send_a, recv_a, send_b, recv_b = refs[:6]
    me = lax.axis_index("tensor")

    barrier = pltpu.get_barrier_semaphore()
    for k in range(1, n):
        pl.semaphore_signal(
            barrier, inc=1, device_id={"tensor": lax.rem(me + k, n)}, device_id_type=MESH
        )
    pl.semaphore_wait(barrier, n - 1)

    def remote(src, dst, send, receive, k):
        return pltpu.make_async_remote_copy(
            src_ref=src,
            dst_ref=dst,
            send_sem=send.at[k],
            recv_sem=receive.at[k],
            device_id={"tensor": lax.rem(me + k, n)},
            device_id_type=MESH,
        )

    order = sorted(range(1, n), key=lambda k: -min(k, n - k))
    extra = []
    if extras:
        erecv, send_e, recv_e = refs[6:]
        extra = [remote(e_ref, erecv.at[k], send_e, recv_e, k) for k in order]
    first = [remote(x_ref.at[lax.rem(me + k, n)], recv.at[k], send_a, recv_a, k) for k in order]
    for copy in extra + first:
        copy.start()
    if extras:
        for copy in extra:
            copy.wait()
        eout_ref[...] = e_ref[...] + functools.reduce(
            lambda a, k: a + erecv[k], range(2, n), erecv[1]
        )
    for copy in first:
        copy.wait()
    total = x_ref[me].astype(jnp.float32)
    for k in range(1, n):
        total = total + recv[k].astype(jnp.float32)
    mine[...] = total.astype(mine.dtype)
    out_ref[me] = total.astype(mine.dtype)
    partner = me + 1 - 2 * lax.rem(me, 2)
    half = n // 2

    def placed(src, slot, index, target):
        return pltpu.make_async_remote_copy(
            src_ref=src,
            dst_ref=out_ref.at[slot],
            send_sem=send_b.at[index],
            recv_sem=recv_b.at[index],
            device_id={"tensor": target},
            device_id_type=MESH,
        )

    ring = sorted(range(1, half), key=lambda k: -min(k, half - k))
    along = {k: placed(mine, me, k, lax.rem(me + 2 * k, n)) for k in ring}
    across = [placed(mine, me, 0, partner)]
    for copy in list(along.values()) + across:
        copy.start()
    for k in sorted(range(1, half), key=lambda k: min(k, half - k)):
        along[k].wait_recv()
        source = lax.rem(me + n - 2 * k, n)
        copy = placed(out_ref.at[source], source, half - 1 + k, partner)
        copy.start()
        across.append(copy)
    for copy in along.values():
        copy.wait_send()
    for copy in across:
        copy.wait()


def tensor_sum(x, extra, ident):
    n = lax.axis_size("tensor")
    rows, columns = x.shape
    x = x.reshape(n, rows // n, columns)
    vmem = pl.BlockSpec(memory_space=pltpu.VMEM)
    operands = [x] + ([extra] if extra is not None else [])
    shapes = [jax.ShapeDtypeStruct(x.shape, jnp.bfloat16)]
    scratch = [
        pltpu.VMEM(x.shape, x.dtype),
        pltpu.VMEM(x.shape[1:], jnp.bfloat16),
    ] + [pltpu.SemaphoreType.DMA((n,))] * 4
    if extra is not None:
        shapes.append(jax.ShapeDtypeStruct(extra.shape, extra.dtype))
        scratch += [pltpu.VMEM((n,) + extra.shape, extra.dtype)]
        scratch += [pltpu.SemaphoreType.DMA((n,))] * 2
    out = pl.pallas_call(
        functools.partial(reduce_kernel, n, extra is not None),
        out_shape=shapes,
        in_specs=[vmem] * len(operands),
        out_specs=[vmem] * len(shapes),
        scratch_shapes=scratch,
        compiler_params=pltpu.CompilerParams(
            collective_id=ident, has_side_effects=True, vmem_limit_bytes=32 << 20
        ),
        cost_estimate=pl.CostEstimate(flops=0, bytes_accessed=100 << 20, transcendentals=0),
    )(*operands)
    return [out[0].reshape(rows, columns)] + list(out[1:])


UNITS = ("ao", "no", "ap", "np", "nq",)
HALVED = ("ao", "no", "ap", "np", "nq",)
DEFERRED = (3, 0,)
CROSSED = ()
SHARED = (
    10, 6, 14, 11, 15, 7, 8, 12, 16, 13, 17, 9,
)
ORDERS = (
    (
        1, 10, 26, 42, 6, 14, 22, 11, 19, 47, 15, 7, 8, 43, 12, 20, 52, 16, 23, 13, 17, 48, 53,
        0, 24, 29, 4, 2, 9, 46, 45, 44, 25, 30, 5, 34, 51, 56, 50, 55, 3, 62, 49, 32, 54, 36,
        31, 35, 66, 63, 33, 37, 65, 64,
    ),
    (
        1, 10, 42, 6, 14, 11, 47, 15, 26, 7, 8, 43, 12, 20, 16, 22, 13, 27, 21, 48, 17, 52, 0,
        23, 24, 4, 57, 62, 2, 53, 9, 46, 45, 44, 25, 51, 32, 36, 5, 50, 58, 3, 63, 30, 56, 49,
        34, 61, 55, 60, 33, 66, 54, 37, 31, 35, 59, 65, 64,
    ),
    (
        1, 10, 42, 6, 14, 11, 47, 15, 26, 7, 8, 43, 12, 20, 16, 22, 13, 27, 21, 48, 17, 57, 0,
        23, 24, 4, 52, 62, 2, 58, 9, 46, 45, 44, 25, 51, 5, 50, 53, 63, 3, 61, 60, 49, 32, 36,
        30, 34, 59, 56, 66, 55, 65, 33, 37, 54, 64, 31, 35,
    ),
    (
        1, 10, 26, 42, 6, 14, 22, 11, 19, 47, 15, 7, 8, 43, 12, 20, 57, 16, 23, 13, 17, 48, 58,
        0, 24, 29, 4, 2, 9, 46, 45, 44, 25, 5, 51, 61, 62, 50, 60, 3, 49, 59, 63, 32, 36, 30,
        34, 66, 65, 33, 37, 64, 31, 35,
    ),
)


def step_names(line, near):
    numbers = [str(i) for i in range(line)]
    pairs = [str(a) + str(b) for a in range(near) for b in range(2)]
    names = ["q0", "res", "A2", "B", "lift2s", "pc", "stat", "statr", "normo", "normp"]
    names += [k + i for k in ("X", "O", "xs", "I", "J") for i in numbers]
    names += [k + p for k in ("G", "GX", "H") for p in pairs]
    names += [k + unit for k in ("S", "P", "fo", "fi", "e") for unit in UNITS]
    return names + [k + unit + i for k in ("r", "v") for unit in UNITS for i in numbers]


def chosen(index, values):
    picked = values[0]
    for place, value in enumerate(values[1:], 1):
        picked = jnp.where(index == place, value, picked)
    return picked


def line_order(count):
    def edge(c):
        return min(c, count - 1 - c)

    return [
        sorted(range(count), key=lambda c: (-abs(c - z), edge(c))) for z in range(count)
    ]


def segments(order, shared):
    parts, rest = [], list(order)
    for heavy in shared:
        at = rest.index(heavy)
        parts.append(rest[:at])
        rest = rest[at + 1 :]
    return parts + [rest]


def exchange_kernel(n, groups, *refs):
    attn_h, res_h, ffn_h, gain_h, mixing_h, blocks_h = refs[:6]
    attn_o, norm_o, slab_a, slab_n, rot_o, own_o = refs[6:12]
    (
        attn_v, res_v, ffn_v, attn_s, attn_y, res_y, rc, xs, xr, zs, onto, into, onto_x, into_x,
        sq_col, sq_s, sq_r, tot_s, tot_r, inv, sl_k, sl_s, sl_x, sl_p, fl_s, fl_r,
        gain, mixing, blocks, qt_f, qt_s, qt_o, qt_i, qt_x, mix, pattern, flips, base,
        local_sem, send_sem, recv_sem,
    ) = refs[12:]
    rows, features = attn_v.shape
    deep = ffn_v.shape[1] // groups
    share = xs.shape[2]
    half = features // 2
    width = slab_a.shape[2]
    slab_o = (slab_a, slab_n)
    line = n // 2
    near = line // 2
    f32, bf16 = jnp.float32, jnp.bfloat16

    s = lax.axis_index("section")
    d = lax.axis_index("dp")
    t = lax.axis_index("tensor")
    z = t // 2
    x = t - 2 * z
    u = jnp.where(d == 0, z, line - 1 - z)
    toward = 2 - 4 * d
    outward = {"tensor": t + toward}
    inner = {"tensor": t - toward}
    x_peer = {"tensor": t + 1 - 2 * x}
    y_peer = {"dp": 1 - d}
    c_peer = {"section": 1 - s}
    order = line_order(line)
    names = {}

    def sem(name):
        return names.setdefault(name, len(names))

    def remote(source, target, send, receive, device):
        return pltpu.make_async_remote_copy(
            src_ref=source,
            dst_ref=target,
            send_sem=send_sem.at[sem(send)],
            recv_sem=recv_sem.at[sem(receive)],
            device_id=device,
            device_id_type=MESH,
        )

    sent = {}

    def post(uc, make):
        make().start()
        sent.setdefault(uc, []).append(make)

    def combine(target, parts, count, kind=None, strip=48):
        def step(b, carry):
            at = pl.ds(pl.multiple_of(b * strip, strip), strip)
            total = parts[0][at, :]
            for part in parts[1:]:
                total = total + part[at, :]
            target[at, :] = total if kind is None else total.astype(kind)
            return carry

        lax.fori_loop(0, count // strip, step, 0)

    pairs = [(attn_h, attn_v), (res_h, res_v), (ffn_h, ffn_v)]
    pairs += [(gain_h, gain), (mixing_h, mixing), (blocks_h, blocks)]
    loads = [pltpu.make_async_copy(a, b, local_sem.at[i]) for i, (a, b) in enumerate(pairs)]
    for i in (5, 0, 1, 2, 3, 4):
        loads[i].start()

    barrier = pltpu.get_barrier_semaphore()
    others = [{"tensor": lax.rem(t + k, n)} for k in range(1, n)] + [y_peer, c_peer]
    for device in others:
        pl.semaphore_signal(barrier, inc=1, device_id=device, device_id_type=MESH)
    pl.semaphore_wait(barrier, n + 1)

    loads[5].wait()
    per = features // HBLK
    swap = lax.rem(blocks[0, 0], per) > 0
    owned = lax.div(blocks[0, 0], per) == t

    def q0():
        return remote(attn_s.at[1 - d], attn_y.at[1 - d], "q0", "q0", y_peer)

    def a2():
        return remote(attn_s.at[d], attn_y.at[d], "A2", "A2", y_peer)

    def b2():
        return remote(attn_s.at[2:4], attn_y.at[2:4], "B", "B", y_peer)

    def res():
        return remote(res_h, res_y, "res", "res", y_peer)

    def tot():
        return remote(tot_s, tot_r, "tot", "tot", y_peer)

    def pc():
        return remote(own_o.at[0], own_o.at[1], "pc", "pc", y_peer)

    def lift(slot, source):
        return remote(source, rc.at[slot], "lift" + str(slot), "lift" + str(slot), c_peer)

    @pl.when(s == 0)
    def _():
        lift(0, res_h).start()
        rc[...] = jnp.zeros_like(rc)

    loads[0].wait()
    for k in range(4):
        here = slice(k * width, (k + 1) * width)
        there = slice((k + 2) % 4 * width, ((k + 2) % 4 + 1) * width)
        attn_s[k] = jnp.where(swap, attn_v[:, there], attn_v[:, here])

    def destination(i):
        flat = [order[a][i] for a in range(line)]
        to = chosen(u, flat)
        return jnp.where(d == 0, to, line - 1 - to)

    def setup():
        mix[...] = jnp.zeros_like(mix)
        mix[:KB, :KB] = mixing[0]
        row = lax.broadcasted_iota(jnp.int32, pattern.shape, 0)
        lane = lax.broadcasted_iota(jnp.int32, pattern.shape, 1)
        inside = jnp.bitwise_and(lane, ROOM - 1)
        hit = (row == (lane // ROOM) * KB + inside) & (inside < KB)
        pattern[...] = jnp.where(hit, 1.0, 0.0).astype(bf16)

    def odd(values):
        for shift in (8, 4, 2, 1):
            values = jnp.bitwise_xor(values, jnp.right_shift(values, shift))
        return (1 - 2 * jnp.bitwise_and(values, 1)).astype(f32)

    def rotate(target, j):
        lane = lax.broadcasted_iota(jnp.int32, (8, share), 1)
        column = blocks[0, 1] * BLK + j * share + lane
        a_col = ((column.astype(f32) + 0.5) / KB).astype(jnp.int32)
        c_col = column - a_col * KB
        depth = mix.shape[1]
        row = lax.broadcasted_iota(jnp.int32, (depth, share), 0)
        pick = jnp.where(row == c_col[:1, :], 1.0, 0.0).astype(bf16)
        mixed = jnp.dot(mix[...], pick, preferred_element_type=f32)
        for start in range(0, GROUP, 8):
            rank = start + lax.broadcasted_iota(jnp.int32, (8, share), 0)
            flips[start : start + 8, :] = odd(jnp.bitwise_and(rank, a_col))
        quad = pattern.shape[0] // KB

        for q in range(GROUP // quad):
            wide = [(mixed * flips[r : r + 1, :]).astype(bf16) for r in range(q * quad, (q + 1) * quad)]
            base[q * quad * KB : (q + 1) * quad * KB, :] = jnp.dot(
                pattern[...], jnp.concatenate(wide, axis=0), preferred_element_type=f32
            ).astype(bf16)
        a_local = groups * GROUP
        total = None
        for g in range(groups):
            part = jnp.dot(
                ffn_v[:, g * deep : (g + 1) * deep], base[...], preferred_element_type=f32
            )
            sign = odd(jnp.bitwise_and(t * a_local + g * GROUP, a_col)) / math.sqrt(a_local * n)
            part = part * sign[:1, :]
            total = part if total is None else total + part
        target[...] = total

    strip = 64

    def stat():
        loads[1].wait()

        @pl.when(s > 0)
        def _():
            lift(0, res_h).wait_recv()

        def squares(b, carry):
            at = pl.ds(pl.multiple_of(b * strip, strip), strip)
            acc = jnp.zeros((strip, 128), f32)
            for c in range(features // 128):
                lanes = slice(c * 128, (c + 1) * 128)
                v = res_v[at, lanes].astype(f32) + rc[0, at, lanes].astype(f32)
                acc = acc + v * v
            sq_col[at, :] = jnp.broadcast_to(jnp.sum(acc, axis=1, keepdims=True), (strip, 128))
            return carry

        lax.fori_loop(0, rows // strip, squares, 0)
        sq_s[...] = jnp.transpose(sq_col[...])[:8, :]
        for i in range(1, n):
            post(None, functools.partial(stat_copy, i))

    def stat_copy(i):
        name = "stat" + str(i)
        return remote(sq_s, sq_r.at[i], name, name, {"tensor": lax.rem(t + i, n)})

    def inverse(slot, sums):
        spread = jnp.broadcast_to(sums[:1, :], (128, rows))
        inv[slot] = lax.rsqrt(jnp.transpose(spread) / (n * features) + EPS)

    def stats_in():
        total = sq_s[...]
        for i in range(1, n):
            stat_copy(i).wait_recv()
            total = total + sq_r[i]
        tot_s[...] = total
        post(None, tot)
        inverse(0, total)

    def normalize(slot, part):
        def step(b, carry):
            at = pl.ds(pl.multiple_of(b * strip, strip), strip)
            by = inv[slot, at, :]
            for c in range(features // 128):
                lanes = slice(c * 128, (c + 1) * 128)
                v = part[at, lanes].astype(f32) + rc[slot, at, lanes].astype(f32)
                norm_o[slot, at, lanes] = (v * by * gain[:, lanes]).astype(bf16)
            return carry

        lax.fori_loop(0, rows // strip, step, 0)

    def normalize_peer():
        tot().wait_recv()
        inverse(1, tot_r[...])

        @pl.when(s > 0)
        def _():
            res().wait_recv()
            lift(1, res_y).wait_recv()

        normalize(1, res_y)

    def heavy(name):
        if name[0] in "XO":
            i = int(name[1:])
            column = 1 - x if name[0] == "X" else x
            rotate((xs if name[0] == "X" else zs).at[i], 2 * destination(i) + column)
        elif name == "stat":
            stat()
        elif name == "statr":
            stats_in()
        elif name == "normo":
            normalize(0, res_v)
        else:
            normalize_peer()

    mine = pl.ds(pl.multiple_of(d * width, width), width)
    upper = pl.ds(pl.multiple_of(half + d * width, width), width)

    def slab_source(name):
        slot = 0 if name[1] == "o" else 1
        start, count = span(name)
        at = slice(start, start + count)
        if name[0] == "a":
            value = attn_s[d, at] if slot == 0 else attn_y[d, at]
        else:
            value = jnp.where(swap, norm_o[slot, at, upper], norm_o[slot, at, mine])
        return jnp.where(owned, value, jnp.zeros_like(value))

    def span(unit):
        whole = unit[1] == "o" or unit[0] + "q" not in UNITS
        count = rows if whole else rows // 2
        return (rows // 2 if unit[1] == "q" else 0), count

    low = rows // line
    paired_up = set()

    def attn_ready(uc, unit):
        if unit[0] == "a" and unit[1] != "o" and ("q0", uc) not in paired_up:
            paired_up.add(("q0", uc))
            q0().wait_recv()

    def own_ready(uc, b):
        if b == 1 and uc not in paired_up:
            paired_up.add(uc)
            pc().wait_recv()

    def light(uc, name):
        def slab(unit):
            return slab_o[0 if unit[0] == "a" else 1].at[0 if unit[1] == "o" else 1]

        def half_of(unit, column):
            start, count = span(unit)
            tall = count // 2
            return slab(unit).at[pl.ds(pl.multiple_of(start + column * tall, tall), tall)]

        def quarter_of(unit, to):
            return slab(unit).at[to * low : (to + 1) * low]

        def place(source, column, b):
            spot = jnp.where(d == 0, source, near - 1 - source) * 2 + column
            return rot_o.at[b, :, pl.ds(pl.multiple_of(spot * share, share), share)]

        def shared_from(uc, source, b):
            return own_o.at[b] if uc == source else place(source, x, b)

        def gather(source, b, way, device):
            name = "g" + str(source) + str(b)
            where = place(source, x, b)
            return remote(shared_from(uc, source, b), where, name + way, name, device)

        if name == "q0":
            post(uc, q0)
        elif name == "res":
            post(uc, res)
        elif name == "A2":
            post(uc, a2)
        elif name == "B":
            post(uc, b2)
        elif name == "lift2s":

            @pl.when(s == 0)
            def _():
                res().wait_recv()
                lift(1, res_y).start()

        elif name == "pc":
            post(uc, pc)
        elif name[:2] == "xs":
            i = int(name[2:])
            post(uc, lambda: remote(xs.at[i], xr.at[i], "x" + str(i), "x" + str(i), x_peer))
        elif name[0] in "IJ":
            i = int(name[1:])
            to = order[uc][i]
            own = name[0] == "I"
            store = zs if own else xs
            held = store.at[i]
            parts = [held]

            def across():
                return remote(xs.at[i], xr.at[i], "x" + str(i), "x" + str(i), x_peer)

            def along(way):
                key = ("L" if way == 0 else "R") + ("" if own else "x") + str(to)
                slots = (onto if own else onto_x) if way == 0 else (into if own else into_x)
                send = ("zs" if own else "xs") + str(i)
                return remote(store.at[i], slots.at[to], send, key, outward if way == 0 else inner)

            if own and (to == uc or to not in DEFERRED):
                across().wait_recv()
                parts.append(xr.at[i])
            if to >= uc and uc > 0:
                along(0).wait_recv()
                parts.append((onto if own else onto_x).at[to])
            if to <= uc and uc < line - 1:
                along(1).wait_recv()
                parts.append((into if own else into_x).at[to])
            if own and to == uc:
                combine(own_o.at[0], parts, rows, bf16)
            elif len(parts) > 1:
                combine(held, parts, rows)
            if to > uc:
                post(uc, lambda: along(0))
            elif to < uc:
                post(uc, lambda: along(1))
            elif not own:
                post(uc, across)
        elif name[:2] == "GX":
            source, b = int(name[2]), int(name[3])
            key = "gx" + name[2:]
            if b in CROSSED:
                own_ready(uc, b)
            post(uc, lambda: remote(shared_from(uc, source, b), place(source, x, b), key, key, x_peer))
        elif name[0] == "H":
            source, b = int(name[1]), int(name[2])
            where, key = place(source, 1 - x, b), "h" + name[1:]
            if uc == source:
                remote(where, where, "gx" + name[1:], "gx" + name[1:], x_peer).wait_recv()
            else:
                remote(where, where, key + "o", key, outward).wait_recv()

            def ahead(way, device):
                spot = place(source, 1 - x, b)
                return remote(spot, spot, key + way, key, device)

            if uc >= source and uc < line - 1:
                post(uc, lambda: ahead("o", outward))
            if uc <= source and uc > 0:
                post(uc, lambda: ahead("i", inner))
        elif name[0] == "G":
            source, b = int(name[1]), int(name[2])
            if uc == source:
                own_ready(uc, b)
            else:
                gather(source, b, "o", outward).wait_recv()
            if uc >= source and uc < line - 1:
                post(uc, lambda: gather(source, b, "o", outward))
            if uc <= source and uc > 0:
                post(uc, lambda: gather(source, b, "i", inner))
            if uc == source:
                combine(place(source, x, b), [own_o.at[b]], rows)
        else:
            slabs(uc, name, half_of, quarter_of)

    def slabs(uc, name, half_of, quarter_of):
        unit = next(k for k in UNITS if k in name)
        kind, rest = name.split(unit)
        k = UNITS.index(unit)
        tall = span(unit)[1] // 2
        used = slice(0, tall)

        def cross():
            return remote(sl_s.at[k, used], sl_x.at[k, used], "S" + unit, "S" + unit, x_peer)

        def flood(way):
            key = "fo" if way == 0 else "fi"
            device = outward if way == 0 else inner
            return remote(fl_s.at[k, way, used], fl_r.at[k, way, used], key + unit, key + unit, device)

        def back():
            return remote(half_of(unit, x), half_of(unit, x), "b" + unit, "b" + unit, x_peer)

        def reduce(to):
            key = "r" + unit + str(to)
            if to > uc:
                return remote(qt_s.at[k, to], qt_o.at[k, to], key, key + "o", outward)
            if to < uc:
                return remote(qt_s.at[k, to], qt_i.at[k, to], key, key + "i", inner)
            return remote(qt_s.at[k, to], qt_x.at[k], key, "rx" + unit, x_peer)

        def wave(source, way, device):
            key = "w" + unit + str(source)
            return remote(quarter_of(unit, source), quarter_of(unit, source), key + way, key, device)

        if unit in HALVED:
            if kind == "S":
                attn_ready(uc, unit)
                value = slab_source(unit)
                first, second = value[:tall], value[tall:]
                sl_k[k, used] = jnp.where(x == 0, first, second)
                sl_s[k, used] = jnp.where(x == 0, second, first)
                post(uc, cross)
            elif kind == "P":
                cross().wait_recv()
                combine(sl_p.at[k], [sl_k.at[k], sl_x.at[k]], tall)
            elif kind == "fo":
                parts = [sl_p.at[k]]
                if uc > 0:
                    flood(0).wait_recv()
                    parts.append(fl_r.at[k, 0])
                combine(fl_s.at[k, 0], parts, tall)
                post(uc, lambda: flood(0))
            elif kind == "fi":
                parts = [sl_p.at[k]]
                if uc < line - 1:
                    flood(1).wait_recv()
                    parts.append(fl_r.at[k, 1])
                combine(fl_s.at[k, 1], parts, tall)
                post(uc, lambda: flood(1))
            else:
                parts = [sl_p.at[k]]
                if uc > 0:
                    parts.append(fl_r.at[k, 0])
                    if uc == line - 1:
                        flood(0).wait_recv()
                if uc < line - 1:
                    parts.append(fl_r.at[k, 1])
                    if uc == 0:
                        flood(1).wait_recv()
                combine(half_of(unit, x), parts, tall)
                post(uc, back)
            return
        if kind == "S":
            attn_ready(uc, unit)
            qt_f[k] = slab_source(unit)
        elif kind == "r":
            to = int(rest)
            parts = [qt_f.at[k, to * low : (to + 1) * low]]
            if to >= uc and uc > 0:
                remote(qt_s.at[k, to], qt_o.at[k, to], "r" + unit + rest, "r" + unit + rest + "o", outward).wait_recv()
                parts.append(qt_o.at[k, to])
            if to <= uc and uc < line - 1:
                remote(qt_s.at[k, to], qt_i.at[k, to], "r" + unit + rest, "r" + unit + rest + "i", inner).wait_recv()
                parts.append(qt_i.at[k, to])
            combine(qt_s.at[k, to], parts, low)
            post(uc, lambda: reduce(to))
        else:
            source = int(rest)
            if source == uc:
                reduce(uc).wait_recv()
                combine(quarter_of(unit, uc), [qt_s.at[k, uc], qt_x.at[k]], low)
            else:
                wave(source, "o", outward).wait_recv()
            if source <= uc and uc < line - 1:
                post(uc, lambda: wave(source, "o", outward))
            if source >= uc and uc > 0:
                post(uc, lambda: wave(source, "i", inner))

    steps = step_names(line, near)
    shared = [steps[i] for i in SHARED]
    parts = [segments([steps[i] for i in o], shared) for o in ORDERS]
    started = [False]
    for k, name in enumerate(shared + [None]):
        for uc in range(line):
            if parts[uc][k]:

                @pl.when(u == uc)
                def _():
                    for each in parts[uc][k]:
                        light(uc, each)

        if name is None:
            break
        if name[0] in "XO" and not started[0]:
            started[0] = True
            loads[3].wait()
            loads[4].wait()
            setup()
            loads[2].wait()
        heavy(name)

    @pl.when(u >= near)
    def _():
        pc().wait_recv()

    assert len(names) <= SEMAPHORES, len(names)

    combine(attn_o.at[0], [attn_v], rows)
    a2().wait_recv()
    b2().wait_recv()
    for k in range(4):
        here = slice(k * width, (k + 1) * width)
        attn_o[1, :, here] = jnp.where(swap, attn_y[(k + 2) % 4], attn_y[k])

    for unit in HALVED:
        m, b = 0 if unit[0] == "a" else 1, 0 if unit[1] == "o" else 1
        start, count = span(unit)
        tall = count // 2
        where = slab_o[m].at[b, pl.ds(pl.multiple_of(start + (1 - x) * tall, tall), tall)]
        remote(where, where, "b" + unit, "b" + unit, x_peer).wait_recv()
    for source in range(near):
        for b in set(range(2)) - set(CROSSED):
            spot = jnp.where(d == 0, source, near - 1 - source) * 2 + 1 - x
            where = rot_o.at[b, :, pl.ds(pl.multiple_of(spot * share, share), share)]
            key = "gx" + str(source) + str(b)
            remote(where, where, key, key, x_peer).wait_recv()

    for make in sent[None]:
        make().wait_send()
    for uc in range(line):

        @pl.when(u == uc)
        def _():
            for make in sent[uc]:
                make().wait_send()

    @pl.when(s == 0)
    def _():
        lift(0, res_h).wait_send()
        lift(1, res_y).wait_send()


SEMAPHORES = 192
ROOM = 64


def exchanged(*operands):
    attn, res, ffn, gain, mixing, blocks = operands
    n = lax.axis_size("tensor")
    rows, features = attn.shape
    share, width = BLK // n, HBLK // 2
    line = n // 2
    groups = ffn.shape[1] // (GROUP * KB)
    halved = len(UNITS)
    units = 1 if len(HALVED) == len(UNITS) else len(UNITS)
    f32, bf16 = jnp.float32, jnp.bfloat16
    vmem = pl.BlockSpec(memory_space=pltpu.VMEM)
    return pl.pallas_call(
        functools.partial(exchange_kernel, n, groups),
        out_shape=[
            jax.ShapeDtypeStruct((2, rows, features), bf16),
            jax.ShapeDtypeStruct((2, rows, features), bf16),
            jax.ShapeDtypeStruct((2, rows, width), bf16),
            jax.ShapeDtypeStruct((2, rows, width), bf16),
            jax.ShapeDtypeStruct((2, rows, BLK // 2), bf16),
            jax.ShapeDtypeStruct((2, rows, share), bf16),
        ],
        in_specs=[pl.BlockSpec(memory_space=pltpu.HBM)] * 6,
        out_specs=[vmem] * 6,
        scratch_shapes=[
            pltpu.VMEM((rows, features), bf16),
            pltpu.VMEM((rows, features), bf16),
            pltpu.VMEM(ffn.shape, bf16),
            pltpu.VMEM((4, rows, width), bf16),
            pltpu.VMEM((4, rows, width), bf16),
            pltpu.VMEM((rows, features), bf16),
            pltpu.VMEM((2, rows, features), bf16),
            pltpu.VMEM((line, rows, share), f32),
            pltpu.VMEM((line, rows, share), f32),
            pltpu.VMEM((line, rows, share), f32),
            pltpu.VMEM((line, rows, share), f32),
            pltpu.VMEM((line, rows, share), f32),
            pltpu.VMEM((line if DEFERRED else 1, rows, share), f32),
            pltpu.VMEM((line if DEFERRED else 1, rows, share), f32),
            pltpu.VMEM((rows, 128), f32),
            pltpu.VMEM((8, rows), f32),
            pltpu.VMEM((n, 8, rows), f32),
            pltpu.VMEM((8, rows), f32),
            pltpu.VMEM((8, rows), f32),
            pltpu.VMEM((2, rows, 128), f32),
            pltpu.VMEM((halved, rows // 2, width), bf16),
            pltpu.VMEM((halved, rows // 2, width), bf16),
            pltpu.VMEM((halved, rows // 2, width), bf16),
            pltpu.VMEM((halved, rows // 2, width), bf16),
            pltpu.VMEM((halved, 2, rows // 2, width), bf16),
            pltpu.VMEM((halved, 2, rows // 2, width), bf16),
            pltpu.VMEM(gain.shape, f32),
            pltpu.VMEM(mixing.shape, bf16),
            pltpu.SMEM(blocks.shape, jnp.int32),
            pltpu.VMEM((units, rows, width), bf16),
            pltpu.VMEM((units, line, rows // line, width), bf16),
            pltpu.VMEM((units, line, rows // line, width), bf16),
            pltpu.VMEM((units, line, rows // line, width), bf16),
            pltpu.VMEM((units, rows // line, width), bf16),
            pltpu.VMEM((ROOM, 128), bf16),
            pltpu.VMEM((4 * KB, 4 * ROOM), bf16),
            pltpu.VMEM((GROUP, share), f32),
            pltpu.VMEM((GROUP * KB, share), bf16),
            pltpu.SemaphoreType.DMA((6,)),
            pltpu.SemaphoreType.DMA((SEMAPHORES,)),
            pltpu.SemaphoreType.DMA((SEMAPHORES,)),
        ],
        compiler_params=pltpu.CompilerParams(
            collective_id=2, has_side_effects=True, vmem_limit_bytes=43 << 20
        ),
    )(*[pltpu.with_memory_space_constraint(v, pltpu.HBM) for v in operands])


def parity_sign(values):
    return (1 - 2 * (lax.population_count(values) & 1)).astype(jnp.float32)


def gram(left, right):
    return lax.dot_general(
        left, right, (((0,), (0,)), ((), ())), preferred_element_type=jnp.float32
    )


def general(residual_parts, attn_out, ffn_input, norm_gain, mixing, blocks):
    local_d = residual_parts.shape[2]
    local_f = ffn_input.shape[2]
    token_rows = residual_parts.shape[1]
    dp_count = lax.axis_size("dp")
    dp_member = lax.axis_index("dp")
    tensor_count = lax.axis_size("tensor")
    member = lax.axis_index("tensor")
    own_part = residual_parts[0]
    parts = gathered(own_part, "dp")
    attention = jnp.concatenate(gathered(attn_out[0], "dp"), axis=0)
    earlier = [passed_along(part, "section", 1) for part in parts]
    layers = [
        e.astype(jnp.float32) + p.astype(jnp.float32) for e, p in zip(earlier, parts)
    ]
    squares = jnp.sum(layers[0] * layers[0], axis=1).reshape(token_rows // 128, 128)

    a_local = local_f // KB
    order_a = a_local * tensor_count
    deep = GROUP * KB
    column = blocks[0, 1] * BLK + jnp.arange(BLK, dtype=jnp.int32)
    a_col, c_col = column // KB, column % KB
    pick = (jnp.arange(KB, dtype=jnp.int32)[:, None] == c_col[None, :]).astype(jnp.bfloat16)
    spread = jnp.dot(
        jnp.tile(mixing[0], (GROUP, 1)), pick, preferred_element_type=jnp.float32
    )
    row_a = jnp.arange(deep, dtype=jnp.int32) // KB
    base = (spread * parity_sign(row_a[:, None] & a_col[None, :])).astype(jnp.bfloat16)
    term = None
    for g in range(a_local // GROUP):
        sign = parity_sign((member * a_local + g * GROUP) & a_col) / math.sqrt(order_a)
        piece = jnp.dot(
            ffn_input[0, :, g * deep : (g + 1) * deep], base, preferred_element_type=jnp.float32
        )
        piece = piece * sign[None, :]
        term = piece if term is None else term + piece

    rotated, square_own = tensor_sum(term, squares, 0)

    square_total = gathered(square_own, "dp")
    rotated, square_total = lax.optimization_barrier((rotated, square_total))
    square_total = [s.reshape(token_rows) for s in square_total]
    share = BLK // tensor_count
    own_cols = lax.dynamic_slice_in_dim(rotated, member * share, share, 1)
    part_down = gram(own_cols, rotated)
    half = BLK // dp_count
    if dp_count == 2:
        kept = lax.dynamic_slice_in_dim(part_down, dp_member * half, half, 1)
        sent = lax.dynamic_slice_in_dim(part_down, (1 - dp_member) * half, half, 1)
        sum_down = kept + shifted(sent, "dp", 1)
    else:
        sum_down = lax.psum_scatter(part_down, "dp", scatter_dimension=1, tiled=True)

    normed = jnp.concatenate(
        [
            (x * lax.rsqrt(s / D + EPS)[:, None] * norm_gain[0][None, :]).astype(jnp.bfloat16)
            for x, s in zip(layers, square_total)
        ],
        axis=0,
    )
    first_col = blocks[0, 0] * HBLK
    width = HBLK // dp_count
    offset = first_col % local_d + dp_member * width
    owned = first_col // local_d == member
    slab = jnp.concatenate(
        [
            lax.dynamic_slice_in_dim(normed, offset, width, 1),
            lax.dynamic_slice_in_dim(attention, offset, width, 1),
        ],
        axis=0,
    )
    slab = jnp.where(owned, slab, 0).astype(jnp.bfloat16)
    (got,) = tensor_sum(slab, None, 1)
    tokens = token_rows * dp_count
    scale = 2.0 / tokens
    hess_in = (scale * gram(normed, got[:tokens]))[None]
    hess_o = (scale * gram(attention, got[tokens:]))[None]
    hess_down = (scale * sum_down)[None]
    return (hess_in, hess_o, hess_down)


STRIPS = 4


def gram_kernel(scale, attn, normed, slab_a, slab_n, rotated, own, *refs):
    out_in, out_o, out_down, held, held_down, done = refs

    def put(target, at, place):
        return pltpu.make_async_copy(held.at[place], target.at[at], done.at[place])

    held_down[...] = scale * gram(own[...], rotated[...])
    down = pltpu.make_async_copy(held_down, out_down, done.at[2 * STRIPS])
    down.start()
    tall = normed.shape[1] // STRIPS
    copies = []
    for k, (left, right, target) in enumerate([(attn, slab_a, out_o), (normed, slab_n, out_in)]):
        for strip in range(STRIPS):
            at = slice(strip * tall, (strip + 1) * tall)
            place = k * STRIPS + strip
            held[place] = scale * gram(left[:, at], right[...])
            copies.append(put(target, pl.ds(strip * tall, tall), place))
            copies[-1].start()
    for copy in copies + [down]:
        copy.wait()


def grams(scale, attn, normed, slab_a, slab_n, rotated, own):
    features, width = normed.shape[1], slab_n.shape[1]
    down = (own.shape[1], rotated.shape[1])
    f32 = jnp.float32
    return pl.pallas_call(
        functools.partial(gram_kernel, scale),
        out_shape=[
            jax.ShapeDtypeStruct((features, width), f32),
            jax.ShapeDtypeStruct((features, width), f32),
            jax.ShapeDtypeStruct(down, f32),
        ],
        in_specs=[pl.BlockSpec(memory_space=pltpu.VMEM)] * 6,
        out_specs=[pl.BlockSpec(memory_space=pl.ANY)] * 3,
        scratch_shapes=[
            pltpu.VMEM((2 * STRIPS, features // STRIPS, width), f32),
            pltpu.VMEM(down, f32),
            pltpu.SemaphoreType.DMA((2 * STRIPS + 1,)),
        ],
        compiler_params=pltpu.CompilerParams(vmem_limit_bytes=20 << 20),
    )(attn, normed, slab_a, slab_n, rotated, own)


def paired(residual_parts, attn_out, ffn_input, norm_gain, mixing, blocks):
    local_d = residual_parts.shape[2]
    token_rows = residual_parts.shape[1]
    share = BLK // lax.axis_size("tensor")
    attention, normed, slab_a, slab_n, rotated, own = exchanged(
        attn_out[0], residual_parts[0], ffn_input[0], norm_gain, mixing, blocks
    )
    tokens = token_rows * 2
    scale = 2.0 / tokens
    attention, normed = attention.reshape(tokens, local_d), normed.reshape(tokens, local_d)
    slab_a, slab_n = slab_a.reshape(tokens, HBLK // 2), slab_n.reshape(tokens, HBLK // 2)
    hess_in, hess_o, hess_down = grams(
        scale,
        attention,
        normed,
        slab_a,
        slab_n,
        rotated.reshape(tokens, BLK // 2),
        own.reshape(tokens, share),
    )
    return (hess_in[None], hess_o[None], hess_down[None])


def local(*arguments):
    n = lax.axis_size("tensor")
    by_pairs = lax.axis_size("dp") == 2 and lax.axis_size("section") == 2 and n == 2 * len(ORDERS)
    if by_pairs and arguments[0].shape[2] == 2 * HBLK:
        return paired(*arguments)
    return general(*arguments)


def solution(mesh):
    return jax.shard_map(
        local,
        mesh=mesh,
        in_specs=(
            P("section", "dp", "tensor"),
            P("section", "dp", "tensor"),
            P("section", "dp", "tensor"),
            P("section", "tensor"),
            P("section", None, None),
            P("section", None),
        ),
        out_specs=(
            P("section", "tensor", "dp"),
            P("section", "tensor", "dp"),
            P("section", "tensor", "dp"),
        ),
        check_vma=False,
    )
```

```python
import functools
import math

import jax
import jax.numpy as jnp
from jax import lax
from jax.experimental import pallas as pl
from jax.experimental.pallas import tpu as pltpu
from jax.sharding import PartitionSpec as P

D = 16384
KB = 52
HBLK = 1024
BLK = 2048
GROUP = 32


EPS = 1e-05

MESH = pl.DeviceIdType.MESH


def passed_along(x, axis, by):
    devices = lax.axis_size(axis)
    pairs = [(i, i + by) for i in range(devices) if 0 <= i + by < devices]
    return lax.ppermute(x, axis, pairs)


def shifted(x, axis, by):
    devices = lax.axis_size(axis)
    return lax.ppermute(x, axis, [(i, (i + by) % devices) for i in range(devices)])


def gathered(x, axis):
    return [x] + [shifted(x, axis, by) for by in range(1, lax.axis_size(axis))]


def reduce_kernel(n, extras, *refs):
    x_ref, refs = refs[0], refs[1:]
    e_ref, refs = (refs[0], refs[1:]) if extras else (None, refs)
    out_ref, refs = refs[0], refs[1:]
    eout_ref, refs = (refs[0], refs[1:]) if extras else (None, refs)
    recv, mine, send_a, recv_a, send_b, recv_b = refs[:6]
    me = lax.axis_index("tensor")

    barrier = pltpu.get_barrier_semaphore()
    for k in range(1, n):
        pl.semaphore_signal(
            barrier, inc=1, device_id={"tensor": lax.rem(me + k, n)}, device_id_type=MESH
        )
    pl.semaphore_wait(barrier, n - 1)

    def remote(src, dst, send, receive, k):
        return pltpu.make_async_remote_copy(
            src_ref=src,
            dst_ref=dst,
            send_sem=send.at[k],
            recv_sem=receive.at[k],
            device_id={"tensor": lax.rem(me + k, n)},
            device_id_type=MESH,
        )

    order = sorted(range(1, n), key=lambda k: -min(k, n - k))
    extra = []
    if extras:
        erecv, send_e, recv_e = refs[6:]
        extra = [remote(e_ref, erecv.at[k], send_e, recv_e, k) for k in order]
    first = [remote(x_ref.at[lax.rem(me + k, n)], recv.at[k], send_a, recv_a, k) for k in order]
    for copy in extra + first:
        copy.start()
    if extras:
        for copy in extra:
            copy.wait()
        eout_ref[...] = e_ref[...] + functools.reduce(
            lambda a, k: a + erecv[k], range(2, n), erecv[1]
        )
    for copy in first:
        copy.wait()
    total = x_ref[me].astype(jnp.float32)
    for k in range(1, n):
        total = total + recv[k].astype(jnp.float32)
    mine[...] = total.astype(mine.dtype)
    out_ref[me] = total.astype(mine.dtype)
    partner = me + 1 - 2 * lax.rem(me, 2)
    half = n // 2

    def placed(src, slot, index, target):
        return pltpu.make_async_remote_copy(
            src_ref=src,
            dst_ref=out_ref.at[slot],
            send_sem=send_b.at[index],
            recv_sem=recv_b.at[index],
            device_id={"tensor": target},
            device_id_type=MESH,
        )

    ring = sorted(range(1, half), key=lambda k: -min(k, half - k))
    along = {k: placed(mine, me, k, lax.rem(me + 2 * k, n)) for k in ring}
    across = [placed(mine, me, 0, partner)]
    for copy in list(along.values()) + across:
        copy.start()
    for k in sorted(range(1, half), key=lambda k: min(k, half - k)):
        along[k].wait_recv()
        source = lax.rem(me + n - 2 * k, n)
        copy = placed(out_ref.at[source], source, half - 1 + k, partner)
        copy.start()
        across.append(copy)
    for copy in along.values():
        copy.wait_send()
    for copy in across:
        copy.wait()


def tensor_sum(x, extra, ident):
    n = lax.axis_size("tensor")
    rows, columns = x.shape
    x = x.reshape(n, rows // n, columns)
    vmem = pl.BlockSpec(memory_space=pltpu.VMEM)
    operands = [x] + ([extra] if extra is not None else [])
    shapes = [jax.ShapeDtypeStruct(x.shape, jnp.bfloat16)]
    scratch = [
        pltpu.VMEM(x.shape, x.dtype),
        pltpu.VMEM(x.shape[1:], jnp.bfloat16),
    ] + [pltpu.SemaphoreType.DMA((n,))] * 4
    if extra is not None:
        shapes.append(jax.ShapeDtypeStruct(extra.shape, extra.dtype))
        scratch += [pltpu.VMEM((n,) + extra.shape, extra.dtype)]
        scratch += [pltpu.SemaphoreType.DMA((n,))] * 2
    out = pl.pallas_call(
        functools.partial(reduce_kernel, n, extra is not None),
        out_shape=shapes,
        in_specs=[vmem] * len(operands),
        out_specs=[vmem] * len(shapes),
        scratch_shapes=scratch,
        compiler_params=pltpu.CompilerParams(
            collective_id=ident, has_side_effects=True, vmem_limit_bytes=32 << 20
        ),
        cost_estimate=pl.CostEstimate(flops=0, bytes_accessed=100 << 20, transcendentals=0),
    )(*operands)
    return [out[0].reshape(rows, columns)] + list(out[1:])


UNITS = ("ao", "no", "ap", "np", "nq",)
HALVED = ("ao", "no", "ap", "np", "nq",)
DEFERRED = (3,)
CROSSED = ()
SHARED = (
    10, 11, 6, 12, 14, 13, 7, 8, 15, 16, 17, 9,
)
ORDERS = (
    (
        42, 10, 26, 11, 19, 6, 47, 12, 52, 14, 20, 13, 22, 7, 8, 15, 43, 16, 23, 17, 21, 48,
        53, 0, 62, 24, 4, 9, 46, 45, 44, 51, 56, 25, 5, 50, 55, 30, 34, 3, 49, 54, 32, 36, 31,
        35, 63, 33, 37, 2, 64, 66, 65,
    ),
    (
        42, 10, 11, 19, 6, 47, 12, 14, 20, 13, 26, 7, 8, 15, 43, 52, 57, 16, 17, 62, 22, 21,
        48, 0, 24, 4, 23, 9, 53, 46, 45, 44, 25, 51, 5, 32, 36, 3, 50, 58, 56, 63, 55, 49, 33,
        37, 30, 34, 54, 59, 64, 2, 31, 61, 60, 66, 65, 35,
    ),
    (
        42, 10, 18, 11, 6, 47, 12, 14, 20, 13, 57, 7, 8, 15, 43, 16, 17, 21, 27, 22, 48, 52, 0,
        62, 4, 24, 23, 9, 58, 46, 45, 44, 51, 25, 5, 53, 63, 50, 3, 49, 32, 36, 56, 55, 59, 61,
        66, 33, 37, 60, 65, 30, 34, 2, 54, 64, 31, 35,
    ),
    (
        42, 10, 18, 11, 6, 47, 57, 12, 14, 19, 13, 7, 8, 22, 15, 43, 16, 17, 23, 20, 48, 58, 0,
        29, 4, 24, 62, 9, 44, 25, 5, 46, 3, 45, 49, 59, 51, 61, 63, 50, 60, 32, 36, 66, 65, 2,
        33, 37, 30, 34, 64, 31, 35,
    ),
)


def step_names(line, near):
    numbers = [str(i) for i in range(line)]
    pairs = [str(a) + str(b) for a in range(near) for b in range(2)]
    names = ["q0", "res", "A2", "B", "lift2s", "pc", "stat", "statr", "normo", "normp"]
    names += [k + i for k in ("X", "O", "xs", "I", "J") for i in numbers]
    names += [k + p for k in ("G", "GX", "H") for p in pairs]
    names += [k + unit for k in ("S", "P", "fo", "fi", "e") for unit in UNITS]
    return names + [k + unit + i for k in ("r", "v") for unit in UNITS for i in numbers]


def chosen(index, values):
    picked = values[0]
    for place, value in enumerate(values[1:], 1):
        picked = jnp.where(index == place, value, picked)
    return picked


def line_order(count):
    def edge(c):
        return min(c, count - 1 - c)

    return [
        sorted(range(count), key=lambda c: (-abs(c - z), edge(c))) for z in range(count)
    ]


def segments(order, shared):
    parts, rest = [], list(order)
    for heavy in shared:
        at = rest.index(heavy)
        parts.append(rest[:at])
        rest = rest[at + 1 :]
    return parts + [rest]


def exchange_kernel(n, groups, *refs):
    attn_h, res_h, ffn_h, gain_h, mixing_h, blocks_h = refs[:6]
    attn_o, norm_o, slab_a, slab_n, rot_o, own_o = refs[6:12]
    (
        attn_v, res_v, ffn_v, attn_s, attn_y, res_y, rc, xs, xr, zs, onto, into, onto_x, into_x,
        sq_col, sq_s, sq_r, tot_s, tot_r, inv, sl_k, sl_s, sl_x, sl_p, fl_s, fl_r,
        gain, mixing, blocks, qt_f, qt_s, qt_o, qt_i, qt_x, mix, pattern, flips, base,
        local_sem, send_sem, recv_sem,
    ) = refs[12:]
    rows, features = attn_v.shape
    deep = ffn_v.shape[1] // groups
    share = xs.shape[2]
    half = features // 2
    width = slab_a.shape[2]
    slab_o = (slab_a, slab_n)
    line = n // 2
    near = line // 2
    f32, bf16 = jnp.float32, jnp.bfloat16

    s = lax.axis_index("section")
    d = lax.axis_index("dp")
    t = lax.axis_index("tensor")
    z = t // 2
    x = t - 2 * z
    u = jnp.where(d == 0, z, line - 1 - z)
    toward = 2 - 4 * d
    outward = {"tensor": t + toward}
    inner = {"tensor": t - toward}
    x_peer = {"tensor": t + 1 - 2 * x}
    y_peer = {"dp": 1 - d}
    c_peer = {"section": 1 - s}
    order = line_order(line)
    names = {}

    def sem(name):
        return names.setdefault(name, len(names))

    def remote(source, target, send, receive, device):
        return pltpu.make_async_remote_copy(
            src_ref=source,
            dst_ref=target,
            send_sem=send_sem.at[sem(send)],
            recv_sem=recv_sem.at[sem(receive)],
            device_id=device,
            device_id_type=MESH,
        )

    sent = {}

    def post(uc, make):
        make().start()
        sent.setdefault(uc, []).append(make)

    def combine(target, parts, count, kind=None, strip=48):
        def step(b, carry):
            at = pl.ds(pl.multiple_of(b * strip, strip), strip)
            total = parts[0][at, :]
            for part in parts[1:]:
                total = total + part[at, :]
            target[at, :] = total if kind is None else total.astype(kind)
            return carry

        lax.fori_loop(0, count // strip, step, 0)

    pairs = [(attn_h, attn_v), (res_h, res_v), (ffn_h, ffn_v)]
    pairs += [(gain_h, gain), (mixing_h, mixing), (blocks_h, blocks)]
    loads = [pltpu.make_async_copy(a, b, local_sem.at[i]) for i, (a, b) in enumerate(pairs)]
    for i in (5, 0, 1, 2, 3, 4):
        loads[i].start()

    barrier = pltpu.get_barrier_semaphore()
    others = [{"tensor": lax.rem(t + k, n)} for k in range(1, n)] + [y_peer, c_peer]
    for device in others:
        pl.semaphore_signal(barrier, inc=1, device_id=device, device_id_type=MESH)
    pl.semaphore_wait(barrier, n + 1)

    loads[5].wait()
    per = features // HBLK
    swap = lax.rem(blocks[0, 0], per) > 0
    owned = lax.div(blocks[0, 0], per) == t

    def q0():
        return remote(attn_s.at[1 - d], attn_y.at[1 - d], "q0", "q0", y_peer)

    def a2():
        return remote(attn_s.at[d], attn_y.at[d], "A2", "A2", y_peer)

    def b2():
        return remote(attn_s.at[2:4], attn_y.at[2:4], "B", "B", y_peer)

    def res():
        return remote(res_h, res_y, "res", "res", y_peer)

    def tot():
        return remote(tot_s, tot_r, "tot", "tot", y_peer)

    def pc():
        return remote(own_o.at[0], own_o.at[1], "pc", "pc", y_peer)

    def lift(slot, source):
        return remote(source, rc.at[slot], "lift" + str(slot), "lift" + str(slot), c_peer)

    post(None, res)

    @pl.when(s == 0)
    def _():
        lift(0, res_h).start()

    loads[0].wait()
    for k in range(4):
        here = slice(k * width, (k + 1) * width)
        there = slice((k + 2) % 4 * width, ((k + 2) % 4 + 1) * width)
        attn_s[k] = jnp.where(swap, attn_v[:, there], attn_v[:, here])

    def destination(i):
        flat = [order[a][i] for a in range(line)]
        to = chosen(u, flat)
        return jnp.where(d == 0, to, line - 1 - to)

    def setup():
        mix[...] = jnp.zeros_like(mix)
        mix[:KB, :KB] = mixing[0]
        row = lax.broadcasted_iota(jnp.int32, pattern.shape, 0)
        lane = lax.broadcasted_iota(jnp.int32, pattern.shape, 1)
        inside = jnp.bitwise_and(lane, ROOM - 1)
        hit = (row == (lane // ROOM) * KB + inside) & (inside < KB)
        pattern[...] = jnp.where(hit, 1.0, 0.0).astype(bf16)

    def odd(values):
        for shift in (8, 4, 2, 1):
            values = jnp.bitwise_xor(values, jnp.right_shift(values, shift))
        return (1 - 2 * jnp.bitwise_and(values, 1)).astype(f32)

    def rotate(target, j):
        lane = lax.broadcasted_iota(jnp.int32, (8, share), 1)
        column = blocks[0, 1] * BLK + j * share + lane
        a_col = ((column.astype(f32) + 0.5) / KB).astype(jnp.int32)
        c_col = column - a_col * KB
        depth = mix.shape[1]
        row = lax.broadcasted_iota(jnp.int32, (depth, share), 0)
        pick = jnp.where(row == c_col[:1, :], 1.0, 0.0).astype(bf16)
        mixed = jnp.dot(mix[...], pick, preferred_element_type=f32)
        for start in range(0, GROUP, 8):
            rank = start + lax.broadcasted_iota(jnp.int32, (8, share), 0)
            flips[start : start + 8, :] = odd(jnp.bitwise_and(rank, a_col))
        quad = pattern.shape[0] // KB

        for q in range(GROUP // quad):
            wide = [(mixed * flips[r : r + 1, :]).astype(bf16) for r in range(q * quad, (q + 1) * quad)]
            base[q * quad * KB : (q + 1) * quad * KB, :] = jnp.dot(
                pattern[...], jnp.concatenate(wide, axis=0), preferred_element_type=f32
            ).astype(bf16)
        a_local = groups * GROUP
        total = None
        for g in range(groups):
            part = jnp.dot(
                ffn_v[:, g * deep : (g + 1) * deep], base[...], preferred_element_type=f32
            )
            sign = odd(jnp.bitwise_and(t * a_local + g * GROUP, a_col)) / math.sqrt(a_local * n)
            part = part * sign[:1, :]
            total = part if total is None else total + part
        target[...] = total

    strip = 64

    def stat():
        loads[1].wait()

        @pl.when(s == 0)
        def _():
            rc[...] = jnp.zeros_like(rc)

        @pl.when(s > 0)
        def _():
            lift(0, res_h).wait_recv()

        def squares(b, carry):
            at = pl.ds(pl.multiple_of(b * strip, strip), strip)
            acc = jnp.zeros((strip, 128), f32)
            for c in range(features // 128):
                lanes = slice(c * 128, (c + 1) * 128)
                v = res_v[at, lanes].astype(f32) + rc[0, at, lanes].astype(f32)
                acc = acc + v * v
            sq_col[at, :] = jnp.broadcast_to(jnp.sum(acc, axis=1, keepdims=True), (strip, 128))
            return carry

        lax.fori_loop(0, rows // strip, squares, 0)
        sq_s[...] = jnp.transpose(sq_col[...])[:8, :]
        for i in range(1, n):
            post(None, functools.partial(stat_copy, i))

    def stat_copy(i):
        name = "stat" + str(i)
        return remote(sq_s, sq_r.at[i], name, name, {"tensor": lax.rem(t + i, n)})

    def inverse(slot, sums):
        spread = jnp.broadcast_to(sums[:1, :], (128, rows))
        inv[slot] = lax.rsqrt(jnp.transpose(spread) / (n * features) + EPS)

    def stats_in():
        total = sq_s[...]
        for i in range(1, n):
            stat_copy(i).wait_recv()
            total = total + sq_r[i]
        tot_s[...] = total
        post(None, tot)
        inverse(0, total)

    def normalize(slot, part):
        def step(b, carry):
            at = pl.ds(pl.multiple_of(b * strip, strip), strip)
            by = inv[slot, at, :]
            for c in range(features // 128):
                lanes = slice(c * 128, (c + 1) * 128)
                v = part[at, lanes].astype(f32) + rc[slot, at, lanes].astype(f32)
                norm_o[slot, at, lanes] = (v * by * gain[:, lanes]).astype(bf16)
            return carry

        lax.fori_loop(0, rows // strip, step, 0)

    def normalize_peer():
        tot().wait_recv()
        inverse(1, tot_r[...])

        @pl.when(s > 0)
        def _():
            res().wait_recv()
            lift(1, res_y).wait_recv()

        normalize(1, res_y)

    def heavy(name):
        if name[0] in "XO":
            i = int(name[1:])
            column = 1 - x if name[0] == "X" else x
            rotate((xs if name[0] == "X" else zs).at[i], 2 * destination(i) + column)
        elif name == "stat":
            stat()
        elif name == "statr":
            stats_in()
        elif name == "normo":
            normalize(0, res_v)
        else:
            normalize_peer()

    mine = pl.ds(pl.multiple_of(d * width, width), width)
    upper = pl.ds(pl.multiple_of(half + d * width, width), width)

    def slab_source(name):
        slot = 0 if name[1] == "o" else 1
        start, count = span(name)
        at = slice(start, start + count)
        if name[0] == "a":
            value = attn_s[d, at] if slot == 0 else attn_y[d, at]
        else:
            value = jnp.where(swap, norm_o[slot, at, upper], norm_o[slot, at, mine])
        return jnp.where(owned, value, jnp.zeros_like(value))

    def span(unit):
        whole = unit[1] == "o" or unit[0] + "q" not in UNITS
        count = rows if whole else rows // 2
        return (rows // 2 if unit[1] == "q" else 0), count

    low = rows // line
    paired_up = set()

    def attn_ready(uc, unit):
        if unit[0] == "a" and unit[1] != "o" and ("q0", uc) not in paired_up:
            paired_up.add(("q0", uc))
            q0().wait_recv()

    def own_ready(uc, b):
        if b == 1 and uc not in paired_up:
            paired_up.add(uc)
            pc().wait_recv()

    def light(uc, name):
        def slab(unit):
            return slab_o[0 if unit[0] == "a" else 1].at[0 if unit[1] == "o" else 1]

        def half_of(unit, column):
            start, count = span(unit)
            tall = count // 2
            return slab(unit).at[pl.ds(pl.multiple_of(start + column * tall, tall), tall)]

        def quarter_of(unit, to):
            return slab(unit).at[to * low : (to + 1) * low]

        def place(source, column, b):
            spot = jnp.where(d == 0, source, near - 1 - source) * 2 + column
            return rot_o.at[b, :, pl.ds(pl.multiple_of(spot * share, share), share)]

        def shared_from(uc, source, b):
            return own_o.at[b] if uc == source else place(source, x, b)

        def gather(source, b, way, device):
            name = "g" + str(source) + str(b)
            where = place(source, x, b)
            return remote(shared_from(uc, source, b), where, name + way, name, device)

        if name == "q0":
            post(uc, q0)
        elif name == "A2":
            post(uc, a2)
        elif name == "B":
            post(uc, b2)
        elif name == "lift2s":

            @pl.when(s == 0)
            def _():
                res().wait_recv()
                lift(1, res_y).start()

        elif name == "pc":
            post(uc, pc)
        elif name[:2] == "xs":
            i = int(name[2:])
            post(uc, lambda: remote(xs.at[i], xr.at[i], "x" + str(i), "x" + str(i), x_peer))
        elif name[0] in "IJ":
            i = int(name[1:])
            to = order[uc][i]
            own = name[0] == "I"
            store = zs if own else xs
            held = store.at[i]
            parts = [held]

            def across():
                return remote(xs.at[i], xr.at[i], "x" + str(i), "x" + str(i), x_peer)

            def along(way):
                key = ("L" if way == 0 else "R") + ("" if own else "x") + str(to)
                slots = (onto if own else onto_x) if way == 0 else (into if own else into_x)
                send = ("zs" if own else "xs") + str(i)
                return remote(store.at[i], slots.at[to], send, key, outward if way == 0 else inner)

            if own and (to == uc or to not in DEFERRED):
                across().wait_recv()
                parts.append(xr.at[i])
            if to >= uc and uc > 0:
                along(0).wait_recv()
                parts.append((onto if own else onto_x).at[to])
            if to <= uc and uc < line - 1:
                along(1).wait_recv()
                parts.append((into if own else into_x).at[to])
            if own and to == uc:
                combine(own_o.at[0], parts, rows, bf16)
            elif len(parts) > 1:
                combine(held, parts, rows)
            if to > uc:
                post(uc, lambda: along(0))
            elif to < uc:
                post(uc, lambda: along(1))
            elif not own:
                post(uc, across)
        elif name[:2] == "GX":
            source, b = int(name[2]), int(name[3])
            key = "gx" + name[2:]
            if b in CROSSED:
                own_ready(uc, b)
            post(uc, lambda: remote(shared_from(uc, source, b), place(source, x, b), key, key, x_peer))
        elif name[0] == "H":
            source, b = int(name[1]), int(name[2])
            where, key = place(source, 1 - x, b), "h" + name[1:]
            if uc == source:
                remote(where, where, "gx" + name[1:], "gx" + name[1:], x_peer).wait_recv()
            else:
                remote(where, where, key + "o", key, outward).wait_recv()

            def ahead(way, device):
                spot = place(source, 1 - x, b)
                return remote(spot, spot, key + way, key, device)

            if uc >= source and uc < line - 1:
                post(uc, lambda: ahead("o", outward))
            if uc <= source and uc > 0:
                post(uc, lambda: ahead("i", inner))
        elif name[0] == "G":
            source, b = int(name[1]), int(name[2])
            if uc == source:
                own_ready(uc, b)
            else:
                gather(source, b, "o", outward).wait_recv()
            if uc >= source and uc < line - 1:
                post(uc, lambda: gather(source, b, "o", outward))
            if uc <= source and uc > 0:
                post(uc, lambda: gather(source, b, "i", inner))
            if uc == source:
                combine(place(source, x, b), [own_o.at[b]], rows)
        else:
            slabs(uc, name, half_of, quarter_of)

    def slabs(uc, name, half_of, quarter_of):
        unit = next(k for k in UNITS if k in name)
        kind, rest = name.split(unit)
        k = UNITS.index(unit)
        tall = span(unit)[1] // 2
        used = slice(0, tall)

        def cross():
            return remote(sl_s.at[k, used], sl_x.at[k, used], "S" + unit, "S" + unit, x_peer)

        def flood(way):
            key = "fo" if way == 0 else "fi"
            device = outward if way == 0 else inner
            return remote(fl_s.at[k, way, used], fl_r.at[k, way, used], key + unit, key + unit, device)

        def back():
            return remote(half_of(unit, x), half_of(unit, x), "b" + unit, "b" + unit, x_peer)

        def reduce(to):
            key = "r" + unit + str(to)
            if to > uc:
                return remote(qt_s.at[k, to], qt_o.at[k, to], key, key + "o", outward)
            if to < uc:
                return remote(qt_s.at[k, to], qt_i.at[k, to], key, key + "i", inner)
            return remote(qt_s.at[k, to], qt_x.at[k], key, "rx" + unit, x_peer)

        def wave(source, way, device):
            key = "w" + unit + str(source)
            return remote(quarter_of(unit, source), quarter_of(unit, source), key + way, key, device)

        if unit in HALVED:
            if kind == "S":
                attn_ready(uc, unit)
                value = slab_source(unit)
                first, second = value[:tall], value[tall:]
                sl_k[k, used] = jnp.where(x == 0, first, second)
                sl_s[k, used] = jnp.where(x == 0, second, first)
                post(uc, cross)
            elif kind == "P":
                cross().wait_recv()
                combine(sl_p.at[k], [sl_k.at[k], sl_x.at[k]], tall)
            elif kind == "fo":
                parts = [sl_p.at[k]]
                if uc > 0:
                    flood(0).wait_recv()
                    parts.append(fl_r.at[k, 0])
                combine(fl_s.at[k, 0], parts, tall)
                post(uc, lambda: flood(0))
            elif kind == "fi":
                parts = [sl_p.at[k]]
                if uc < line - 1:
                    flood(1).wait_recv()
                    parts.append(fl_r.at[k, 1])
                combine(fl_s.at[k, 1], parts, tall)
                post(uc, lambda: flood(1))
            else:
                parts = [sl_p.at[k]]
                if uc > 0:
                    parts.append(fl_r.at[k, 0])
                    if uc == line - 1:
                        flood(0).wait_recv()
                if uc < line - 1:
                    parts.append(fl_r.at[k, 1])
                    if uc == 0:
                        flood(1).wait_recv()
                combine(half_of(unit, x), parts, tall)
                post(uc, back)
            return
        if kind == "S":
            attn_ready(uc, unit)
            qt_f[k] = slab_source(unit)
        elif kind == "r":
            to = int(rest)
            parts = [qt_f.at[k, to * low : (to + 1) * low]]
            if to >= uc and uc > 0:
                remote(qt_s.at[k, to], qt_o.at[k, to], "r" + unit + rest, "r" + unit + rest + "o", outward).wait_recv()
                parts.append(qt_o.at[k, to])
            if to <= uc and uc < line - 1:
                remote(qt_s.at[k, to], qt_i.at[k, to], "r" + unit + rest, "r" + unit + rest + "i", inner).wait_recv()
                parts.append(qt_i.at[k, to])
            combine(qt_s.at[k, to], parts, low)
            post(uc, lambda: reduce(to))
        else:
            source = int(rest)
            if source == uc:
                reduce(uc).wait_recv()
                combine(quarter_of(unit, uc), [qt_s.at[k, uc], qt_x.at[k]], low)
            else:
                wave(source, "o", outward).wait_recv()
            if source <= uc and uc < line - 1:
                post(uc, lambda: wave(source, "o", outward))
            if source >= uc and uc > 0:
                post(uc, lambda: wave(source, "i", inner))

    steps = step_names(line, near)
    shared = [steps[i] for i in SHARED]
    parts = [segments([steps[i] for i in o], shared) for o in ORDERS]
    started = [False]
    for k, name in enumerate(shared + [None]):
        for uc in range(line):
            if parts[uc][k]:

                @pl.when(u == uc)
                def _():
                    for each in parts[uc][k]:
                        light(uc, each)

        if name is None:
            break
        if name[0] in "XO" and not started[0]:
            started[0] = True
            loads[3].wait()
            loads[4].wait()
            setup()
            loads[2].wait()
        heavy(name)

    @pl.when(u >= near)
    def _():
        pc().wait_recv()

    assert len(names) <= SEMAPHORES, len(names)

    combine(attn_o.at[0], [attn_v], rows)
    a2().wait_recv()
    b2().wait_recv()
    for k in range(4):
        here = slice(k * width, (k + 1) * width)
        attn_o[1, :, here] = jnp.where(swap, attn_y[(k + 2) % 4], attn_y[k])

    for unit in HALVED:
        m, b = 0 if unit[0] == "a" else 1, 0 if unit[1] == "o" else 1
        start, count = span(unit)
        tall = count // 2
        where = slab_o[m].at[b, pl.ds(pl.multiple_of(start + (1 - x) * tall, tall), tall)]
        remote(where, where, "b" + unit, "b" + unit, x_peer).wait_recv()
    for source in range(near):
        for b in set(range(2)) - set(CROSSED):
            spot = jnp.where(d == 0, source, near - 1 - source) * 2 + 1 - x
            where = rot_o.at[b, :, pl.ds(pl.multiple_of(spot * share, share), share)]
            key = "gx" + str(source) + str(b)
            remote(where, where, key, key, x_peer).wait_recv()

    for make in sent[None]:
        make().wait_send()
    for uc in range(line):

        @pl.when(u == uc)
        def _():
            for make in sent[uc]:
                make().wait_send()

    @pl.when(s == 0)
    def _():
        lift(0, res_h).wait_send()
        lift(1, res_y).wait_send()


SEMAPHORES = 192
ROOM = 64


def exchanged(*operands):
    attn, res, ffn, gain, mixing, blocks = operands
    n = lax.axis_size("tensor")
    rows, features = attn.shape
    share, width = BLK // n, HBLK // 2
    line = n // 2
    groups = ffn.shape[1] // (GROUP * KB)
    halved = len(UNITS)
    units = 1 if len(HALVED) == len(UNITS) else len(UNITS)
    f32, bf16 = jnp.float32, jnp.bfloat16
    vmem = pl.BlockSpec(memory_space=pltpu.VMEM)
    return pl.pallas_call(
        functools.partial(exchange_kernel, n, groups),
        out_shape=[
            jax.ShapeDtypeStruct((2, rows, features), bf16),
            jax.ShapeDtypeStruct((2, rows, features), bf16),
            jax.ShapeDtypeStruct((2, rows, width), bf16),
            jax.ShapeDtypeStruct((2, rows, width), bf16),
            jax.ShapeDtypeStruct((2, rows, BLK // 2), bf16),
            jax.ShapeDtypeStruct((2, rows, share), bf16),
        ],
        in_specs=[pl.BlockSpec(memory_space=pltpu.HBM)] * 6,
        out_specs=[vmem] * 6,
        scratch_shapes=[
            pltpu.VMEM((rows, features), bf16),
            pltpu.VMEM((rows, features), bf16),
            pltpu.VMEM(ffn.shape, bf16),
            pltpu.VMEM((4, rows, width), bf16),
            pltpu.VMEM((4, rows, width), bf16),
            pltpu.VMEM((rows, features), bf16),
            pltpu.VMEM((2, rows, features), bf16),
            pltpu.VMEM((line, rows, share), f32),
            pltpu.VMEM((line, rows, share), f32),
            pltpu.VMEM((line, rows, share), f32),
            pltpu.VMEM((line, rows, share), f32),
            pltpu.VMEM((line, rows, share), f32),
            pltpu.VMEM((line if DEFERRED else 1, rows, share), f32),
            pltpu.VMEM((line if DEFERRED else 1, rows, share), f32),
            pltpu.VMEM((rows, 128), f32),
            pltpu.VMEM((8, rows), f32),
            pltpu.VMEM((n, 8, rows), f32),
            pltpu.VMEM((8, rows), f32),
            pltpu.VMEM((8, rows), f32),
            pltpu.VMEM((2, rows, 128), f32),
            pltpu.VMEM((halved, rows // 2, width), bf16),
            pltpu.VMEM((halved, rows // 2, width), bf16),
            pltpu.VMEM((halved, rows // 2, width), bf16),
            pltpu.VMEM((halved, rows // 2, width), bf16),
            pltpu.VMEM((halved, 2, rows // 2, width), bf16),
            pltpu.VMEM((halved, 2, rows // 2, width), bf16),
            pltpu.VMEM(gain.shape, f32),
            pltpu.VMEM(mixing.shape, bf16),
            pltpu.SMEM(blocks.shape, jnp.int32),
            pltpu.VMEM((units, rows, width), bf16),
            pltpu.VMEM((units, line, rows // line, width), bf16),
            pltpu.VMEM((units, line, rows // line, width), bf16),
            pltpu.VMEM((units, line, rows // line, width), bf16),
            pltpu.VMEM((units, rows // line, width), bf16),
            pltpu.VMEM((ROOM, 128), bf16),
            pltpu.VMEM((4 * KB, 4 * ROOM), bf16),
            pltpu.VMEM((GROUP, share), f32),
            pltpu.VMEM((GROUP * KB, share), bf16),
            pltpu.SemaphoreType.DMA((6,)),
            pltpu.SemaphoreType.DMA((SEMAPHORES,)),
            pltpu.SemaphoreType.DMA((SEMAPHORES,)),
        ],
        compiler_params=pltpu.CompilerParams(
            collective_id=2, has_side_effects=True, vmem_limit_bytes=43 << 20
        ),
    )(*[pltpu.with_memory_space_constraint(v, pltpu.HBM) for v in operands])


def parity_sign(values):
    return (1 - 2 * (lax.population_count(values) & 1)).astype(jnp.float32)


def gram(left, right):
    return lax.dot_general(
        left, right, (((0,), (0,)), ((), ())), preferred_element_type=jnp.float32
    )


def general(residual_parts, attn_out, ffn_input, norm_gain, mixing, blocks):
    local_d = residual_parts.shape[2]
    local_f = ffn_input.shape[2]
    token_rows = residual_parts.shape[1]
    dp_count = lax.axis_size("dp")
    dp_member = lax.axis_index("dp")
    tensor_count = lax.axis_size("tensor")
    member = lax.axis_index("tensor")
    own_part = residual_parts[0]
    parts = gathered(own_part, "dp")
    attention = jnp.concatenate(gathered(attn_out[0], "dp"), axis=0)
    earlier = [passed_along(part, "section", 1) for part in parts]
    layers = [
        e.astype(jnp.float32) + p.astype(jnp.float32) for e, p in zip(earlier, parts)
    ]
    squares = jnp.sum(layers[0] * layers[0], axis=1).reshape(token_rows // 128, 128)

    a_local = local_f // KB
    order_a = a_local * tensor_count
    deep = GROUP * KB
    column = blocks[0, 1] * BLK + jnp.arange(BLK, dtype=jnp.int32)
    a_col, c_col = column // KB, column % KB
    pick = (jnp.arange(KB, dtype=jnp.int32)[:, None] == c_col[None, :]).astype(jnp.bfloat16)
    spread = jnp.dot(
        jnp.tile(mixing[0], (GROUP, 1)), pick, preferred_element_type=jnp.float32
    )
    row_a = jnp.arange(deep, dtype=jnp.int32) // KB
    base = (spread * parity_sign(row_a[:, None] & a_col[None, :])).astype(jnp.bfloat16)
    term = None
    for g in range(a_local // GROUP):
        sign = parity_sign((member * a_local + g * GROUP) & a_col) / math.sqrt(order_a)
        piece = jnp.dot(
            ffn_input[0, :, g * deep : (g + 1) * deep], base, preferred_element_type=jnp.float32
        )
        piece = piece * sign[None, :]
        term = piece if term is None else term + piece

    rotated, square_own = tensor_sum(term, squares, 0)

    square_total = gathered(square_own, "dp")
    rotated, square_total = lax.optimization_barrier((rotated, square_total))
    square_total = [s.reshape(token_rows) for s in square_total]
    share = BLK // tensor_count
    own_cols = lax.dynamic_slice_in_dim(rotated, member * share, share, 1)
    part_down = gram(own_cols, rotated)
    half = BLK // dp_count
    if dp_count == 2:
        kept = lax.dynamic_slice_in_dim(part_down, dp_member * half, half, 1)
        sent = lax.dynamic_slice_in_dim(part_down, (1 - dp_member) * half, half, 1)
        sum_down = kept + shifted(sent, "dp", 1)
    else:
        sum_down = lax.psum_scatter(part_down, "dp", scatter_dimension=1, tiled=True)

    normed = jnp.concatenate(
        [
            (x * lax.rsqrt(s / D + EPS)[:, None] * norm_gain[0][None, :]).astype(jnp.bfloat16)
            for x, s in zip(layers, square_total)
        ],
        axis=0,
    )
    first_col = blocks[0, 0] * HBLK
    width = HBLK // dp_count
    offset = first_col % local_d + dp_member * width
    owned = first_col // local_d == member
    slab = jnp.concatenate(
        [
            lax.dynamic_slice_in_dim(normed, offset, width, 1),
            lax.dynamic_slice_in_dim(attention, offset, width, 1),
        ],
        axis=0,
    )
    slab = jnp.where(owned, slab, 0).astype(jnp.bfloat16)
    (got,) = tensor_sum(slab, None, 1)
    tokens = token_rows * dp_count
    scale = 2.0 / tokens
    hess_in = (scale * gram(normed, got[:tokens]))[None]
    hess_o = (scale * gram(attention, got[tokens:]))[None]
    hess_down = (scale * sum_down)[None]
    return (hess_in, hess_o, hess_down)


STRIPS = 4


def gram_kernel(scale, attn, normed, slab_a, slab_n, rotated, own, *refs):
    out_in, out_o, out_down, held, held_down, done = refs

    def put(target, at, place):
        return pltpu.make_async_copy(held.at[place], target.at[at], done.at[place])

    held_down[...] = scale * gram(own[...], rotated[...])
    down = pltpu.make_async_copy(held_down, out_down, done.at[2 * STRIPS])
    down.start()
    tall = normed.shape[1] // STRIPS
    copies = []
    for k, (left, right, target) in enumerate([(attn, slab_a, out_o), (normed, slab_n, out_in)]):
        for strip in range(STRIPS):
            at = slice(strip * tall, (strip + 1) * tall)
            place = k * STRIPS + strip
            held[place] = scale * gram(left[:, at], right[...])
            copies.append(put(target, pl.ds(strip * tall, tall), place))
            copies[-1].start()
    for copy in copies + [down]:
        copy.wait()


def grams(scale, attn, normed, slab_a, slab_n, rotated, own):
    features, width = normed.shape[1], slab_n.shape[1]
    down = (own.shape[1], rotated.shape[1])
    f32 = jnp.float32
    return pl.pallas_call(
        functools.partial(gram_kernel, scale),
        out_shape=[
            jax.ShapeDtypeStruct((features, width), f32),
            jax.ShapeDtypeStruct((features, width), f32),
            jax.ShapeDtypeStruct(down, f32),
        ],
        in_specs=[pl.BlockSpec(memory_space=pltpu.VMEM)] * 6,
        out_specs=[pl.BlockSpec(memory_space=pl.ANY)] * 3,
        scratch_shapes=[
            pltpu.VMEM((2 * STRIPS, features // STRIPS, width), f32),
            pltpu.VMEM(down, f32),
            pltpu.SemaphoreType.DMA((2 * STRIPS + 1,)),
        ],
        compiler_params=pltpu.CompilerParams(vmem_limit_bytes=20 << 20),
    )(attn, normed, slab_a, slab_n, rotated, own)


def paired(residual_parts, attn_out, ffn_input, norm_gain, mixing, blocks):
    local_d = residual_parts.shape[2]
    token_rows = residual_parts.shape[1]
    share = BLK // lax.axis_size("tensor")
    attention, normed, slab_a, slab_n, rotated, own = exchanged(
        attn_out[0], residual_parts[0], ffn_input[0], norm_gain, mixing, blocks
    )
    tokens = token_rows * 2
    scale = 2.0 / tokens
    attention, normed = attention.reshape(tokens, local_d), normed.reshape(tokens, local_d)
    slab_a, slab_n = slab_a.reshape(tokens, HBLK // 2), slab_n.reshape(tokens, HBLK // 2)
    hess_in, hess_o, hess_down = grams(
        scale,
        attention,
        normed,
        slab_a,
        slab_n,
        rotated.reshape(tokens, BLK // 2),
        own.reshape(tokens, share),
    )
    return (hess_in[None], hess_o[None], hess_down[None])


def local(*arguments):
    n = lax.axis_size("tensor")
    by_pairs = lax.axis_size("dp") == 2 and lax.axis_size("section") == 2 and n == 2 * len(ORDERS)
    if by_pairs and arguments[0].shape[2] == 2 * HBLK:
        return paired(*arguments)
    return general(*arguments)


def solution(mesh):
    return jax.shard_map(
        local,
        mesh=mesh,
        in_specs=(
            P("section", "dp", "tensor"),
            P("section", "dp", "tensor"),
            P("section", "dp", "tensor"),
            P("section", "tensor"),
            P("section", None, None),
            P("section", None),
        ),
        out_specs=(
            P("section", "tensor", "dp"),
            P("section", "tensor", "dp"),
            P("section", "tensor", "dp"),
        ),
        check_vma=False,
    )
```

```python
import functools
import math

import jax
import jax.numpy as jnp
from jax import lax
from jax.experimental import pallas as pl
from jax.experimental.pallas import tpu as pltpu
from jax.sharding import PartitionSpec as P

D = 16384
KB = 52
HBLK = 1024
BLK = 2048
GROUP = 32


EPS = 1e-05

MESH = pl.DeviceIdType.MESH


def passed_along(x, axis, by):
    devices = lax.axis_size(axis)
    pairs = [(i, i + by) for i in range(devices) if 0 <= i + by < devices]
    return lax.ppermute(x, axis, pairs)


def shifted(x, axis, by):
    devices = lax.axis_size(axis)
    return lax.ppermute(x, axis, [(i, (i + by) % devices) for i in range(devices)])


def gathered(x, axis):
    return [x] + [shifted(x, axis, by) for by in range(1, lax.axis_size(axis))]


def reduce_kernel(n, extras, *refs):
    x_ref, refs = refs[0], refs[1:]
    e_ref, refs = (refs[0], refs[1:]) if extras else (None, refs)
    out_ref, refs = refs[0], refs[1:]
    eout_ref, refs = (refs[0], refs[1:]) if extras else (None, refs)
    recv, mine, send_a, recv_a, send_b, recv_b = refs[:6]
    me = lax.axis_index("tensor")

    barrier = pltpu.get_barrier_semaphore()
    for k in range(1, n):
        pl.semaphore_signal(
            barrier, inc=1, device_id={"tensor": lax.rem(me + k, n)}, device_id_type=MESH
        )
    pl.semaphore_wait(barrier, n - 1)

    def remote(src, dst, send, receive, k):
        return pltpu.make_async_remote_copy(
            src_ref=src,
            dst_ref=dst,
            send_sem=send.at[k],
            recv_sem=receive.at[k],
            device_id={"tensor": lax.rem(me + k, n)},
            device_id_type=MESH,
        )

    order = sorted(range(1, n), key=lambda k: -min(k, n - k))
    extra = []
    if extras:
        erecv, send_e, recv_e = refs[6:]
        extra = [remote(e_ref, erecv.at[k], send_e, recv_e, k) for k in order]
    first = [remote(x_ref.at[lax.rem(me + k, n)], recv.at[k], send_a, recv_a, k) for k in order]
    for copy in extra + first:
        copy.start()
    if extras:
        for copy in extra:
            copy.wait()
        eout_ref[...] = e_ref[...] + functools.reduce(
            lambda a, k: a + erecv[k], range(2, n), erecv[1]
        )
    for copy in first:
        copy.wait()
    total = x_ref[me].astype(jnp.float32)
    for k in range(1, n):
        total = total + recv[k].astype(jnp.float32)
    mine[...] = total.astype(mine.dtype)
    out_ref[me] = total.astype(mine.dtype)
    partner = me + 1 - 2 * lax.rem(me, 2)
    half = n // 2

    def placed(src, slot, index, target):
        return pltpu.make_async_remote_copy(
            src_ref=src,
            dst_ref=out_ref.at[slot],
            send_sem=send_b.at[index],
            recv_sem=recv_b.at[index],
            device_id={"tensor": target},
            device_id_type=MESH,
        )

    ring = sorted(range(1, half), key=lambda k: -min(k, half - k))
    along = {k: placed(mine, me, k, lax.rem(me + 2 * k, n)) for k in ring}
    across = [placed(mine, me, 0, partner)]
    for copy in list(along.values()) + across:
        copy.start()
    for k in sorted(range(1, half), key=lambda k: min(k, half - k)):
        along[k].wait_recv()
        source = lax.rem(me + n - 2 * k, n)
        copy = placed(out_ref.at[source], source, half - 1 + k, partner)
        copy.start()
        across.append(copy)
    for copy in along.values():
        copy.wait_send()
    for copy in across:
        copy.wait()


def tensor_sum(x, extra, ident):
    n = lax.axis_size("tensor")
    rows, columns = x.shape
    x = x.reshape(n, rows // n, columns)
    vmem = pl.BlockSpec(memory_space=pltpu.VMEM)
    operands = [x] + ([extra] if extra is not None else [])
    shapes = [jax.ShapeDtypeStruct(x.shape, jnp.bfloat16)]
    scratch = [
        pltpu.VMEM(x.shape, x.dtype),
        pltpu.VMEM(x.shape[1:], jnp.bfloat16),
    ] + [pltpu.SemaphoreType.DMA((n,))] * 4
    if extra is not None:
        shapes.append(jax.ShapeDtypeStruct(extra.shape, extra.dtype))
        scratch += [pltpu.VMEM((n,) + extra.shape, extra.dtype)]
        scratch += [pltpu.SemaphoreType.DMA((n,))] * 2
    out = pl.pallas_call(
        functools.partial(reduce_kernel, n, extra is not None),
        out_shape=shapes,
        in_specs=[vmem] * len(operands),
        out_specs=[vmem] * len(shapes),
        scratch_shapes=scratch,
        compiler_params=pltpu.CompilerParams(
            collective_id=ident, has_side_effects=True, vmem_limit_bytes=32 << 20
        ),
        cost_estimate=pl.CostEstimate(flops=0, bytes_accessed=100 << 20, transcendentals=0),
    )(*operands)
    return [out[0].reshape(rows, columns)] + list(out[1:])


UNITS = ("ao", "no", "ap", "np", "nq",)
HALVED = ("ao", "no", "ap", "np", "nq",)
DEFERRED = (3,)
CROSSED = ((0, 1),)
SHARED = (
    10, 6, 14, 11, 15, 7, 8, 12, 16, 13, 17, 9,
)
ORDERS = (
    (
        42, 10, 26, 6, 47, 14, 52, 11, 19, 15, 7, 22, 8, 43, 12, 16, 20, 13, 23, 17, 48, 53,
        21, 0, 24, 4, 62, 9, 46, 45, 44, 25, 5, 51, 56, 2, 30, 34, 50, 55, 32, 36, 49, 54, 3,
        33, 31, 35, 37, 63, 39, 66, 64, 65,
    ),
    (
        42, 10, 6, 47, 14, 11, 19, 15, 26, 7, 8, 43, 12, 52, 57, 16, 20, 13, 17, 48, 22, 21, 0,
        24, 4, 62, 23, 53, 9, 46, 45, 44, 25, 32, 5, 2, 51, 36, 50, 33, 56, 37, 58, 49, 3, 61,
        30, 34, 55, 63, 54, 66, 31, 59, 64, 60, 65, 39,
    ),
    (
        42, 10, 18, 6, 47, 14, 11, 15, 57, 7, 8, 43, 12, 20, 16, 13, 48, 17, 21, 27, 22, 0, 52,
        62, 24, 4, 23, 9, 46, 45, 44, 25, 5, 2, 51, 58, 50, 53, 63, 61, 49, 32, 36, 3, 33, 37,
        56, 66, 59, 30, 34, 60, 55, 65, 54, 64, 31, 39,
    ),
    (
        42, 10, 18, 6, 47, 57, 14, 11, 19, 15, 7, 8, 22, 12, 20, 16, 13, 23, 17, 43, 0, 24, 4,
        48, 29, 58, 9, 46, 62, 44, 51, 61, 25, 5, 2, 45, 63, 49, 59, 3, 50, 60, 32, 36, 33, 37,
        66, 30, 34, 65, 64, 31, 39,
    ),
)


def step_names(line, near):
    numbers = [str(i) for i in range(line)]
    pairs = [str(a) + str(b) for a in range(near) for b in range(2)]
    names = ["q0", "res", "A2", "B", "lift2s", "pc", "stat", "statr", "normo", "normp"]
    names += [k + i for k in ("X", "O", "xs", "I", "J") for i in numbers]
    names += [k + p for k in ("G", "GX", "H") for p in pairs]
    names += [k + unit for k in ("S", "P", "fo", "fi", "e") for unit in UNITS]
    return names + [k + unit + i for k in ("r", "v") for unit in UNITS for i in numbers]


def chosen(index, values):
    picked = values[0]
    for place, value in enumerate(values[1:], 1):
        picked = jnp.where(index == place, value, picked)
    return picked


def line_order(count):
    def edge(c):
        return min(c, count - 1 - c)

    return [
        sorted(range(count), key=lambda c: (-abs(c - z), edge(c))) for z in range(count)
    ]


def segments(order, shared):
    parts, rest = [], list(order)
    for heavy in shared:
        at = rest.index(heavy)
        parts.append(rest[:at])
        rest = rest[at + 1 :]
    return parts + [rest]


def exchange_kernel(n, groups, *refs):
    attn_h, res_h, ffn_h, gain_h, mixing_h, blocks_h = refs[:6]
    attn_o, norm_o, slab_a, slab_n, rot_o, own_o = refs[6:12]
    (
        attn_v, res_v, ffn_v, attn_s, attn_y, res_y, rc, xs, xr, zs, onto, into, onto_x, into_x,
        sq_col, sq_s, sq_r, tot_s, tot_r, inv, sl_k, sl_s, sl_x, sl_p, fl_s, fl_r,
        gain, mixing, blocks, qt_f, qt_s, qt_o, qt_i, qt_x, mix, pattern, flips, base,
        local_sem, send_sem, recv_sem,
    ) = refs[12:]
    rows, features = attn_v.shape
    deep = ffn_v.shape[1] // groups
    share = xs.shape[2]
    half = features // 2
    width = slab_a.shape[2]
    slab_o = (slab_a, slab_n)
    line = n // 2
    near = line // 2
    f32, bf16 = jnp.float32, jnp.bfloat16

    s = lax.axis_index("section")
    d = lax.axis_index("dp")
    t = lax.axis_index("tensor")
    z = t // 2
    x = t - 2 * z
    u = jnp.where(d == 0, z, line - 1 - z)
    toward = 2 - 4 * d
    outward = {"tensor": t + toward}
    inner = {"tensor": t - toward}
    x_peer = {"tensor": t + 1 - 2 * x}
    y_peer = {"dp": 1 - d}
    c_peer = {"section": 1 - s}
    order = line_order(line)
    names = {}

    def sem(name):
        return names.setdefault(name, len(names))

    def remote(source, target, send, receive, device):
        return pltpu.make_async_remote_copy(
            src_ref=source,
            dst_ref=target,
            send_sem=send_sem.at[sem(send)],
            recv_sem=recv_sem.at[sem(receive)],
            device_id=device,
            device_id_type=MESH,
        )

    sent = {}

    def post(uc, make):
        make().start()
        sent.setdefault(uc, []).append(make)

    def combine(target, parts, count, kind=None, strip=48):
        def step(b, carry):
            at = pl.ds(pl.multiple_of(b * strip, strip), strip)
            total = parts[0][at, :]
            for part in parts[1:]:
                total = total + part[at, :]
            target[at, :] = total if kind is None else total.astype(kind)
            return carry

        lax.fori_loop(0, count // strip, step, 0)

    pairs = [(attn_h, attn_v), (res_h, res_v), (ffn_h, ffn_v)]
    pairs += [(gain_h, gain), (mixing_h, mixing), (blocks_h, blocks)]
    loads = [pltpu.make_async_copy(a, b, local_sem.at[i]) for i, (a, b) in enumerate(pairs)]
    for i in (5, 0, 1, 2, 3, 4):
        loads[i].start()

    barrier = pltpu.get_barrier_semaphore()
    others = [{"tensor": lax.rem(t + k, n)} for k in range(1, n)] + [y_peer, c_peer]
    for device in others:
        pl.semaphore_signal(barrier, inc=1, device_id=device, device_id_type=MESH)
    pl.semaphore_wait(barrier, n + 1)

    loads[5].wait()
    per = features // HBLK
    swap = lax.rem(blocks[0, 0], per) > 0
    owned = lax.div(blocks[0, 0], per) == t

    def q0():
        return remote(attn_s.at[1 - d], attn_y.at[1 - d], "q0", "q0", y_peer)

    def a2():
        return remote(attn_s.at[d], attn_y.at[d], "A2", "A2", y_peer)

    def b2():
        return remote(attn_s.at[2:4], attn_y.at[2:4], "B", "B", y_peer)

    def res():
        return remote(res_h, res_y, "res", "res", y_peer)

    def tot():
        return remote(tot_s, tot_r, "tot", "tot", y_peer)

    def pc():
        return remote(own_o.at[0], own_o.at[1], "pc", "pc", y_peer)

    def lift(slot, source):
        return remote(source, rc.at[slot], "lift" + str(slot), "lift" + str(slot), c_peer)

    post(None, res)

    @pl.when(s == 0)
    def _():
        lift(0, res_h).start()

    loads[0].wait()
    for k in range(4):
        here = slice(k * width, (k + 1) * width)
        there = slice((k + 2) % 4 * width, ((k + 2) % 4 + 1) * width)
        attn_s[k] = jnp.where(swap, attn_v[:, there], attn_v[:, here])

    def destination(i):
        flat = [order[a][i] for a in range(line)]
        to = chosen(u, flat)
        return jnp.where(d == 0, to, line - 1 - to)

    def setup():
        mix[...] = jnp.zeros_like(mix)
        mix[:KB, :KB] = mixing[0]
        row = lax.broadcasted_iota(jnp.int32, pattern.shape, 0)
        lane = lax.broadcasted_iota(jnp.int32, pattern.shape, 1)
        inside = jnp.bitwise_and(lane, ROOM - 1)
        hit = (row == (lane // ROOM) * KB + inside) & (inside < KB)
        pattern[...] = jnp.where(hit, 1.0, 0.0).astype(bf16)

    def odd(values):
        for shift in (8, 4, 2, 1):
            values = jnp.bitwise_xor(values, jnp.right_shift(values, shift))
        return (1 - 2 * jnp.bitwise_and(values, 1)).astype(f32)

    def rotate(target, j):
        lane = lax.broadcasted_iota(jnp.int32, (8, share), 1)
        column = blocks[0, 1] * BLK + j * share + lane
        a_col = ((column.astype(f32) + 0.5) / KB).astype(jnp.int32)
        c_col = column - a_col * KB
        depth = mix.shape[1]
        row = lax.broadcasted_iota(jnp.int32, (depth, share), 0)
        pick = jnp.where(row == c_col[:1, :], 1.0, 0.0).astype(bf16)
        mixed = jnp.dot(mix[...], pick, preferred_element_type=f32)
        for start in range(0, GROUP, 8):
            rank = start + lax.broadcasted_iota(jnp.int32, (8, share), 0)
            flips[start : start + 8, :] = odd(jnp.bitwise_and(rank, a_col))
        quad = pattern.shape[0] // KB

        for q in range(GROUP // quad):
            wide = [(mixed * flips[r : r + 1, :]).astype(bf16) for r in range(q * quad, (q + 1) * quad)]
            base[q * quad * KB : (q + 1) * quad * KB, :] = jnp.dot(
                pattern[...], jnp.concatenate(wide, axis=0), preferred_element_type=f32
            ).astype(bf16)
        a_local = groups * GROUP
        total = None
        for g in range(groups):
            part = jnp.dot(
                ffn_v[:, g * deep : (g + 1) * deep], base[...], preferred_element_type=f32
            )
            sign = odd(jnp.bitwise_and(t * a_local + g * GROUP, a_col)) / math.sqrt(a_local * n)
            part = part * sign[:1, :]
            total = part if total is None else total + part
        target[...] = total

    strip = 64

    def stat():
        loads[1].wait()

        @pl.when(s == 0)
        def _():
            rc[...] = jnp.zeros_like(rc)

        @pl.when(s > 0)
        def _():
            lift(0, res_h).wait_recv()

        def squares(b, carry):
            at = pl.ds(pl.multiple_of(b * strip, strip), strip)
            acc = jnp.zeros((strip, 128), f32)
            for c in range(features // 128):
                lanes = slice(c * 128, (c + 1) * 128)
                v = res_v[at, lanes].astype(f32) + rc[0, at, lanes].astype(f32)
                acc = acc + v * v
            sq_col[at, :] = jnp.broadcast_to(jnp.sum(acc, axis=1, keepdims=True), (strip, 128))
            return carry

        lax.fori_loop(0, rows // strip, squares, 0)
        sq_s[...] = jnp.transpose(sq_col[...])[:8, :]
        for i in range(1, n):
            post(None, functools.partial(stat_copy, i))

    def stat_copy(i):
        name = "stat" + str(i)
        return remote(sq_s, sq_r.at[i], name, name, {"tensor": lax.rem(t + i, n)})

    def inverse(slot, sums):
        spread = jnp.broadcast_to(sums[:1, :], (128, rows))
        inv[slot] = lax.rsqrt(jnp.transpose(spread) / (n * features) + EPS)

    def stats_in():
        total = sq_s[...]
        for i in range(1, n):
            stat_copy(i).wait_recv()
            total = total + sq_r[i]
        tot_s[...] = total
        post(None, tot)
        inverse(0, total)

    def normalize(slot, part):
        def step(b, carry):
            at = pl.ds(pl.multiple_of(b * strip, strip), strip)
            by = inv[slot, at, :]
            for c in range(features // 128):
                lanes = slice(c * 128, (c + 1) * 128)
                v = part[at, lanes].astype(f32) + rc[slot, at, lanes].astype(f32)
                norm_o[slot, at, lanes] = (v * by * gain[:, lanes]).astype(bf16)
            return carry

        lax.fori_loop(0, rows // strip, step, 0)

    def normalize_peer():
        tot().wait_recv()
        inverse(1, tot_r[...])

        @pl.when(s > 0)
        def _():
            res().wait_recv()
            lift(1, res_y).wait_recv()

        normalize(1, res_y)

    def heavy(name):
        if name[0] in "XO":
            i = int(name[1:])
            column = 1 - x if name[0] == "X" else x
            rotate((xs if name[0] == "X" else zs).at[i], 2 * destination(i) + column)
        elif name == "stat":
            stat()
        elif name == "statr":
            stats_in()
        elif name == "normo":
            normalize(0, res_v)
        else:
            normalize_peer()

    mine = pl.ds(pl.multiple_of(d * width, width), width)
    upper = pl.ds(pl.multiple_of(half + d * width, width), width)

    def slab_source(name):
        slot = 0 if name[1] == "o" else 1
        start, count = span(name)
        at = slice(start, start + count)
        if name[0] == "a":
            value = attn_s[d, at] if slot == 0 else attn_y[d, at]
        else:
            value = jnp.where(swap, norm_o[slot, at, upper], norm_o[slot, at, mine])
        return jnp.where(owned, value, jnp.zeros_like(value))

    def span(unit):
        whole = unit[1] == "o" or unit[0] + "q" not in UNITS
        count = rows if whole else rows // 2
        return (rows // 2 if unit[1] == "q" else 0), count

    low = rows // line
    paired_up = set()

    def attn_ready(uc, unit):
        if unit[0] == "a" and unit[1] != "o" and ("q0", uc) not in paired_up:
            paired_up.add(("q0", uc))
            q0().wait_recv()

    def own_ready(uc, b):
        if b == 1 and uc not in paired_up:
            paired_up.add(uc)
            pc().wait_recv()

    def light(uc, name):
        def slab(unit):
            return slab_o[0 if unit[0] == "a" else 1].at[0 if unit[1] == "o" else 1]

        def half_of(unit, column):
            start, count = span(unit)
            tall = count // 2
            return slab(unit).at[pl.ds(pl.multiple_of(start + column * tall, tall), tall)]

        def quarter_of(unit, to):
            return slab(unit).at[to * low : (to + 1) * low]

        def place(source, column, b):
            spot = jnp.where(d == 0, source, near - 1 - source) * 2 + column
            return rot_o.at[b, :, pl.ds(pl.multiple_of(spot * share, share), share)]

        def shared_from(uc, source, b):
            return own_o.at[b] if uc == source else place(source, x, b)

        def gather(source, b, way, device):
            name = "g" + str(source) + str(b)
            where = place(source, x, b)
            return remote(shared_from(uc, source, b), where, name + way, name, device)

        if name == "q0":
            post(uc, q0)
        elif name == "A2":
            post(uc, a2)
        elif name == "B":
            post(uc, b2)
        elif name == "lift2s":

            @pl.when(s == 0)
            def _():
                res().wait_recv()
                lift(1, res_y).start()

        elif name == "pc":
            post(uc, pc)
        elif name[:2] == "xs":
            i = int(name[2:])
            post(uc, lambda: remote(xs.at[i], xr.at[i], "x" + str(i), "x" + str(i), x_peer))
        elif name[0] in "IJ":
            i = int(name[1:])
            to = order[uc][i]
            own = name[0] == "I"
            store = zs if own else xs
            held = store.at[i]
            parts = [held]

            def across():
                return remote(xs.at[i], xr.at[i], "x" + str(i), "x" + str(i), x_peer)

            def along(way):
                key = ("L" if way == 0 else "R") + ("" if own else "x") + str(to)
                slots = (onto if own else onto_x) if way == 0 else (into if own else into_x)
                send = ("zs" if own else "xs") + str(i)
                return remote(store.at[i], slots.at[to], send, key, outward if way == 0 else inner)

            if own and (to == uc or to not in DEFERRED):
                across().wait_recv()
                parts.append(xr.at[i])
            if to >= uc and uc > 0:
                along(0).wait_recv()
                parts.append((onto if own else onto_x).at[to])
            if to <= uc and uc < line - 1:
                along(1).wait_recv()
                parts.append((into if own else into_x).at[to])
            if own and to == uc:
                combine(own_o.at[0], parts, rows, bf16)
            elif len(parts) > 1:
                combine(held, parts, rows)
            if to > uc:
                post(uc, lambda: along(0))
            elif to < uc:
                post(uc, lambda: along(1))
            elif not own:
                post(uc, across)
        elif name[:2] == "GX":
            source, b = int(name[2]), int(name[3])
            key = "gx" + name[2:]
            if (source, b) in CROSSED:
                own_ready(uc, b)
            post(uc, lambda: remote(shared_from(uc, source, b), place(source, x, b), key, key, x_peer))
        elif name[0] == "H":
            source, b = int(name[1]), int(name[2])
            where, key = place(source, 1 - x, b), "h" + name[1:]
            if uc == source:
                remote(where, where, "gx" + name[1:], "gx" + name[1:], x_peer).wait_recv()
            else:
                remote(where, where, key + "o", key, outward).wait_recv()

            def ahead(way, device):
                spot = place(source, 1 - x, b)
                return remote(spot, spot, key + way, key, device)

            if uc >= source and uc < line - 1:
                post(uc, lambda: ahead("o", outward))
            if uc <= source and uc > 0:
                post(uc, lambda: ahead("i", inner))
        elif name[0] == "G":
            source, b = int(name[1]), int(name[2])
            if uc == source:
                own_ready(uc, b)
            else:
                gather(source, b, "o", outward).wait_recv()
            if uc >= source and uc < line - 1:
                post(uc, lambda: gather(source, b, "o", outward))
            if uc <= source and uc > 0:
                post(uc, lambda: gather(source, b, "i", inner))
            if uc == source:
                combine(place(source, x, b), [own_o.at[b]], rows)
        else:
            slabs(uc, name, half_of, quarter_of)

    def slabs(uc, name, half_of, quarter_of):
        unit = next(k for k in UNITS if k in name)
        kind, rest = name.split(unit)
        k = UNITS.index(unit)
        tall = span(unit)[1] // 2
        used = slice(0, tall)

        def cross():
            return remote(sl_s.at[k, used], sl_x.at[k, used], "S" + unit, "S" + unit, x_peer)

        def flood(way):
            key = "fo" if way == 0 else "fi"
            device = outward if way == 0 else inner
            return remote(fl_s.at[k, way, used], fl_r.at[k, way, used], key + unit, key + unit, device)

        def back():
            return remote(half_of(unit, x), half_of(unit, x), "b" + unit, "b" + unit, x_peer)

        def reduce(to):
            key = "r" + unit + str(to)
            if to > uc:
                return remote(qt_s.at[k, to], qt_o.at[k, to], key, key + "o", outward)
            if to < uc:
                return remote(qt_s.at[k, to], qt_i.at[k, to], key, key + "i", inner)
            return remote(qt_s.at[k, to], qt_x.at[k], key, "rx" + unit, x_peer)

        def wave(source, way, device):
            key = "w" + unit + str(source)
            return remote(quarter_of(unit, source), quarter_of(unit, source), key + way, key, device)

        if unit in HALVED:
            if kind == "S":
                attn_ready(uc, unit)
                value = slab_source(unit)
                first, second = value[:tall], value[tall:]
                sl_k[k, used] = jnp.where(x == 0, first, second)
                sl_s[k, used] = jnp.where(x == 0, second, first)
                post(uc, cross)
            elif kind == "P":
                cross().wait_recv()
                combine(sl_p.at[k], [sl_k.at[k], sl_x.at[k]], tall)
            elif kind == "fo":
                parts = [sl_p.at[k]]
                if uc > 0:
                    flood(0).wait_recv()
                    parts.append(fl_r.at[k, 0])
                combine(fl_s.at[k, 0], parts, tall)
                post(uc, lambda: flood(0))
            elif kind == "fi":
                parts = [sl_p.at[k]]
                if uc < line - 1:
                    flood(1).wait_recv()
                    parts.append(fl_r.at[k, 1])
                combine(fl_s.at[k, 1], parts, tall)
                post(uc, lambda: flood(1))
            else:
                parts = [sl_p.at[k]]
                if uc > 0:
                    parts.append(fl_r.at[k, 0])
                    if uc == line - 1:
                        flood(0).wait_recv()
                if uc < line - 1:
                    parts.append(fl_r.at[k, 1])
                    if uc == 0:
                        flood(1).wait_recv()
                combine(half_of(unit, x), parts, tall)
                post(uc, back)
            return
        if kind == "S":
            attn_ready(uc, unit)
            qt_f[k] = slab_source(unit)
        elif kind == "r":
            to = int(rest)
            parts = [qt_f.at[k, to * low : (to + 1) * low]]
            if to >= uc and uc > 0:
                remote(qt_s.at[k, to], qt_o.at[k, to], "r" + unit + rest, "r" + unit + rest + "o", outward).wait_recv()
                parts.append(qt_o.at[k, to])
            if to <= uc and uc < line - 1:
                remote(qt_s.at[k, to], qt_i.at[k, to], "r" + unit + rest, "r" + unit + rest + "i", inner).wait_recv()
                parts.append(qt_i.at[k, to])
            combine(qt_s.at[k, to], parts, low)
            post(uc, lambda: reduce(to))
        else:
            source = int(rest)
            if source == uc:
                reduce(uc).wait_recv()
                combine(quarter_of(unit, uc), [qt_s.at[k, uc], qt_x.at[k]], low)
            else:
                wave(source, "o", outward).wait_recv()
            if source <= uc and uc < line - 1:
                post(uc, lambda: wave(source, "o", outward))
            if source >= uc and uc > 0:
                post(uc, lambda: wave(source, "i", inner))

    steps = step_names(line, near)
    shared = [steps[i] for i in SHARED]
    parts = [segments([steps[i] for i in o], shared) for o in ORDERS]
    started = [False]
    for k, name in enumerate(shared + [None]):
        for uc in range(line):
            if parts[uc][k]:

                @pl.when(u == uc)
                def _():
                    for each in parts[uc][k]:
                        light(uc, each)

        if name is None:
            break
        if name[0] in "XO" and not started[0]:
            started[0] = True
            loads[3].wait()
            loads[4].wait()
            setup()
            loads[2].wait()
        heavy(name)

    @pl.when(u >= near)
    def _():
        pc().wait_recv()

    assert len(names) <= SEMAPHORES, len(names)

    combine(attn_o.at[0], [attn_v], rows)
    a2().wait_recv()
    b2().wait_recv()
    for k in range(4):
        here = slice(k * width, (k + 1) * width)
        attn_o[1, :, here] = jnp.where(swap, attn_y[(k + 2) % 4], attn_y[k])

    for unit in HALVED:
        m, b = 0 if unit[0] == "a" else 1, 0 if unit[1] == "o" else 1
        start, count = span(unit)
        tall = count // 2
        where = slab_o[m].at[b, pl.ds(pl.multiple_of(start + (1 - x) * tall, tall), tall)]
        remote(where, where, "b" + unit, "b" + unit, x_peer).wait_recv()
    for source in range(near):
        for b in range(2):
            if (source, b) in CROSSED:
                continue
            spot = jnp.where(d == 0, source, near - 1 - source) * 2 + 1 - x
            where = rot_o.at[b, :, pl.ds(pl.multiple_of(spot * share, share), share)]
            key = "gx" + str(source) + str(b)
            remote(where, where, key, key, x_peer).wait_recv()

    for make in sent[None]:
        make().wait_send()
    for uc in range(line):

        @pl.when(u == uc)
        def _():
            for make in sent[uc]:
                make().wait_send()

    @pl.when(s == 0)
    def _():
        lift(0, res_h).wait_send()
        lift(1, res_y).wait_send()


SEMAPHORES = 192
ROOM = 64


def exchanged(*operands):
    attn, res, ffn, gain, mixing, blocks = operands
    n = lax.axis_size("tensor")
    rows, features = attn.shape
    share, width = BLK // n, HBLK // 2
    line = n // 2
    groups = ffn.shape[1] // (GROUP * KB)
    halved = len(UNITS)
    units = 1 if len(HALVED) == len(UNITS) else len(UNITS)
    f32, bf16 = jnp.float32, jnp.bfloat16
    vmem = pl.BlockSpec(memory_space=pltpu.VMEM)
    return pl.pallas_call(
        functools.partial(exchange_kernel, n, groups),
        out_shape=[
            jax.ShapeDtypeStruct((2, rows, features), bf16),
            jax.ShapeDtypeStruct((2, rows, features), bf16),
            jax.ShapeDtypeStruct((2, rows, width), bf16),
            jax.ShapeDtypeStruct((2, rows, width), bf16),
            jax.ShapeDtypeStruct((2, rows, BLK // 2), bf16),
            jax.ShapeDtypeStruct((2, rows, share), bf16),
        ],
        in_specs=[pl.BlockSpec(memory_space=pltpu.HBM)] * 6,
        out_specs=[vmem] * 6,
        scratch_shapes=[
            pltpu.VMEM((rows, features), bf16),
            pltpu.VMEM((rows, features), bf16),
            pltpu.VMEM(ffn.shape, bf16),
            pltpu.VMEM((4, rows, width), bf16),
            pltpu.VMEM((4, rows, width), bf16),
            pltpu.VMEM((rows, features), bf16),
            pltpu.VMEM((2, rows, features), bf16),
            pltpu.VMEM((line, rows, share), f32),
            pltpu.VMEM((line, rows, share), f32),
            pltpu.VMEM((line, rows, share), f32),
            pltpu.VMEM((line, rows, share), f32),
            pltpu.VMEM((line, rows, share), f32),
            pltpu.VMEM((line if DEFERRED else 1, rows, share), f32),
            pltpu.VMEM((line if DEFERRED else 1, rows, share), f32),
            pltpu.VMEM((rows, 128), f32),
            pltpu.VMEM((8, rows), f32),
            pltpu.VMEM((n, 8, rows), f32),
            pltpu.VMEM((8, rows), f32),
            pltpu.VMEM((8, rows), f32),
            pltpu.VMEM((2, rows, 128), f32),
            pltpu.VMEM((halved, rows // 2, width), bf16),
            pltpu.VMEM((halved, rows // 2, width), bf16),
            pltpu.VMEM((halved, rows // 2, width), bf16),
            pltpu.VMEM((halved, rows // 2, width), bf16),
            pltpu.VMEM((halved, 2, rows // 2, width), bf16),
            pltpu.VMEM((halved, 2, rows // 2, width), bf16),
            pltpu.VMEM(gain.shape, f32),
            pltpu.VMEM(mixing.shape, bf16),
            pltpu.SMEM(blocks.shape, jnp.int32),
            pltpu.VMEM((units, rows, width), bf16),
            pltpu.VMEM((units, line, rows // line, width), bf16),
            pltpu.VMEM((units, line, rows // line, width), bf16),
            pltpu.VMEM((units, line, rows // line, width), bf16),
            pltpu.VMEM((units, rows // line, width), bf16),
            pltpu.VMEM((ROOM, 128), bf16),
            pltpu.VMEM((4 * KB, 4 * ROOM), bf16),
            pltpu.VMEM((GROUP, share), f32),
            pltpu.VMEM((GROUP * KB, share), bf16),
            pltpu.SemaphoreType.DMA((6,)),
            pltpu.SemaphoreType.DMA((SEMAPHORES,)),
            pltpu.SemaphoreType.DMA((SEMAPHORES,)),
        ],
        compiler_params=pltpu.CompilerParams(
            collective_id=2, has_side_effects=True, vmem_limit_bytes=43 << 20
        ),
    )(*[pltpu.with_memory_space_constraint(v, pltpu.HBM) for v in operands])


def parity_sign(values):
    return (1 - 2 * (lax.population_count(values) & 1)).astype(jnp.float32)


def gram(left, right):
    return lax.dot_general(
        left, right, (((0,), (0,)), ((), ())), preferred_element_type=jnp.float32
    )


def general(residual_parts, attn_out, ffn_input, norm_gain, mixing, blocks):
    local_d = residual_parts.shape[2]
    local_f = ffn_input.shape[2]
    token_rows = residual_parts.shape[1]
    dp_count = lax.axis_size("dp")
    dp_member = lax.axis_index("dp")
    tensor_count = lax.axis_size("tensor")
    member = lax.axis_index("tensor")
    own_part = residual_parts[0]
    parts = gathered(own_part, "dp")
    attention = jnp.concatenate(gathered(attn_out[0], "dp"), axis=0)
    earlier = [passed_along(part, "section", 1) for part in parts]
    layers = [
        e.astype(jnp.float32) + p.astype(jnp.float32) for e, p in zip(earlier, parts)
    ]
    squares = jnp.sum(layers[0] * layers[0], axis=1).reshape(token_rows // 128, 128)

    a_local = local_f // KB
    order_a = a_local * tensor_count
    deep = GROUP * KB
    column = blocks[0, 1] * BLK + jnp.arange(BLK, dtype=jnp.int32)
    a_col, c_col = column // KB, column % KB
    pick = (jnp.arange(KB, dtype=jnp.int32)[:, None] == c_col[None, :]).astype(jnp.bfloat16)
    spread = jnp.dot(
        jnp.tile(mixing[0], (GROUP, 1)), pick, preferred_element_type=jnp.float32
    )
    row_a = jnp.arange(deep, dtype=jnp.int32) // KB
    base = (spread * parity_sign(row_a[:, None] & a_col[None, :])).astype(jnp.bfloat16)
    term = None
    for g in range(a_local // GROUP):
        sign = parity_sign((member * a_local + g * GROUP) & a_col) / math.sqrt(order_a)
        piece = jnp.dot(
            ffn_input[0, :, g * deep : (g + 1) * deep], base, preferred_element_type=jnp.float32
        )
        piece = piece * sign[None, :]
        term = piece if term is None else term + piece

    rotated, square_own = tensor_sum(term, squares, 0)

    square_total = gathered(square_own, "dp")
    rotated, square_total = lax.optimization_barrier((rotated, square_total))
    square_total = [s.reshape(token_rows) for s in square_total]
    share = BLK // tensor_count
    own_cols = lax.dynamic_slice_in_dim(rotated, member * share, share, 1)
    part_down = gram(own_cols, rotated)
    half = BLK // dp_count
    if dp_count == 2:
        kept = lax.dynamic_slice_in_dim(part_down, dp_member * half, half, 1)
        sent = lax.dynamic_slice_in_dim(part_down, (1 - dp_member) * half, half, 1)
        sum_down = kept + shifted(sent, "dp", 1)
    else:
        sum_down = lax.psum_scatter(part_down, "dp", scatter_dimension=1, tiled=True)

    normed = jnp.concatenate(
        [
            (x * lax.rsqrt(s / D + EPS)[:, None] * norm_gain[0][None, :]).astype(jnp.bfloat16)
            for x, s in zip(layers, square_total)
        ],
        axis=0,
    )
    first_col = blocks[0, 0] * HBLK
    width = HBLK // dp_count
    offset = first_col % local_d + dp_member * width
    owned = first_col // local_d == member
    slab = jnp.concatenate(
        [
            lax.dynamic_slice_in_dim(normed, offset, width, 1),
            lax.dynamic_slice_in_dim(attention, offset, width, 1),
        ],
        axis=0,
    )
    slab = jnp.where(owned, slab, 0).astype(jnp.bfloat16)
    (got,) = tensor_sum(slab, None, 1)
    tokens = token_rows * dp_count
    scale = 2.0 / tokens
    hess_in = (scale * gram(normed, got[:tokens]))[None]
    hess_o = (scale * gram(attention, got[tokens:]))[None]
    hess_down = (scale * sum_down)[None]
    return (hess_in, hess_o, hess_down)


STRIPS = 4


def gram_kernel(scale, attn, normed, slab_a, slab_n, rotated, own, *refs):
    out_in, out_o, out_down, held, held_down, done = refs

    def put(target, at, place):
        return pltpu.make_async_copy(held.at[place], target.at[at], done.at[place])

    held_down[...] = scale * gram(own[...], rotated[...])
    down = pltpu.make_async_copy(held_down, out_down, done.at[2 * STRIPS])
    down.start()
    tall = normed.shape[1] // STRIPS
    copies = []
    for k, (left, right, target) in enumerate([(attn, slab_a, out_o), (normed, slab_n, out_in)]):
        for strip in range(STRIPS):
            at = slice(strip * tall, (strip + 1) * tall)
            place = k * STRIPS + strip
            held[place] = scale * gram(left[:, at], right[...])
            copies.append(put(target, pl.ds(strip * tall, tall), place))
            copies[-1].start()
    for copy in copies + [down]:
        copy.wait()


def grams(scale, attn, normed, slab_a, slab_n, rotated, own):
    features, width = normed.shape[1], slab_n.shape[1]
    down = (own.shape[1], rotated.shape[1])
    f32 = jnp.float32
    return pl.pallas_call(
        functools.partial(gram_kernel, scale),
        out_shape=[
            jax.ShapeDtypeStruct((features, width), f32),
            jax.ShapeDtypeStruct((features, width), f32),
            jax.ShapeDtypeStruct(down, f32),
        ],
        in_specs=[pl.BlockSpec(memory_space=pltpu.VMEM)] * 6,
        out_specs=[pl.BlockSpec(memory_space=pl.ANY)] * 3,
        scratch_shapes=[
            pltpu.VMEM((2 * STRIPS, features // STRIPS, width), f32),
            pltpu.VMEM(down, f32),
            pltpu.SemaphoreType.DMA((2 * STRIPS + 1,)),
        ],
        compiler_params=pltpu.CompilerParams(vmem_limit_bytes=20 << 20),
    )(attn, normed, slab_a, slab_n, rotated, own)


def paired(residual_parts, attn_out, ffn_input, norm_gain, mixing, blocks):
    local_d = residual_parts.shape[2]
    token_rows = residual_parts.shape[1]
    share = BLK // lax.axis_size("tensor")
    attention, normed, slab_a, slab_n, rotated, own = exchanged(
        attn_out[0], residual_parts[0], ffn_input[0], norm_gain, mixing, blocks
    )
    tokens = token_rows * 2
    scale = 2.0 / tokens
    attention, normed = attention.reshape(tokens, local_d), normed.reshape(tokens, local_d)
    slab_a, slab_n = slab_a.reshape(tokens, HBLK // 2), slab_n.reshape(tokens, HBLK // 2)
    hess_in, hess_o, hess_down = grams(
        scale,
        attention,
        normed,
        slab_a,
        slab_n,
        rotated.reshape(tokens, BLK // 2),
        own.reshape(tokens, share),
    )
    return (hess_in[None], hess_o[None], hess_down[None])


def local(*arguments):
    n = lax.axis_size("tensor")
    by_pairs = lax.axis_size("dp") == 2 and lax.axis_size("section") == 2 and n == 2 * len(ORDERS)
    if by_pairs and arguments[0].shape[2] == 2 * HBLK:
        return paired(*arguments)
    return general(*arguments)


def solution(mesh):
    return jax.shard_map(
        local,
        mesh=mesh,
        in_specs=(
            P("section", "dp", "tensor"),
            P("section", "dp", "tensor"),
            P("section", "dp", "tensor"),
            P("section", "tensor"),
            P("section", None, None),
            P("section", None),
        ),
        out_specs=(
            P("section", "tensor", "dp"),
            P("section", "tensor", "dp"),
            P("section", "tensor", "dp"),
        ),
        check_vma=False,
    )
```

```python
import functools
import math

import jax
import jax.numpy as jnp
from jax import lax
from jax.experimental import pallas as pl
from jax.experimental.pallas import tpu as pltpu
from jax.sharding import PartitionSpec as P

D = 16384
KB = 52
HBLK = 1024
BLK = 2048
GROUP = 32


EPS = 1e-05

MESH = pl.DeviceIdType.MESH


def passed_along(x, axis, by):
    devices = lax.axis_size(axis)
    pairs = [(i, i + by) for i in range(devices) if 0 <= i + by < devices]
    return lax.ppermute(x, axis, pairs)


def shifted(x, axis, by):
    devices = lax.axis_size(axis)
    return lax.ppermute(x, axis, [(i, (i + by) % devices) for i in range(devices)])


def gathered(x, axis):
    return [x] + [shifted(x, axis, by) for by in range(1, lax.axis_size(axis))]


def reduce_kernel(n, extras, *refs):
    x_ref, refs = refs[0], refs[1:]
    e_ref, refs = (refs[0], refs[1:]) if extras else (None, refs)
    out_ref, refs = refs[0], refs[1:]
    eout_ref, refs = (refs[0], refs[1:]) if extras else (None, refs)
    recv, mine, send_a, recv_a, send_b, recv_b = refs[:6]
    me = lax.axis_index("tensor")

    barrier = pltpu.get_barrier_semaphore()
    for k in range(1, n):
        pl.semaphore_signal(
            barrier, inc=1, device_id={"tensor": lax.rem(me + k, n)}, device_id_type=MESH
        )
    pl.semaphore_wait(barrier, n - 1)

    def remote(src, dst, send, receive, k):
        return pltpu.make_async_remote_copy(
            src_ref=src,
            dst_ref=dst,
            send_sem=send.at[k],
            recv_sem=receive.at[k],
            device_id={"tensor": lax.rem(me + k, n)},
            device_id_type=MESH,
        )

    order = sorted(range(1, n), key=lambda k: -min(k, n - k))
    extra = []
    if extras:
        erecv, send_e, recv_e = refs[6:]
        extra = [remote(e_ref, erecv.at[k], send_e, recv_e, k) for k in order]
    first = [remote(x_ref.at[lax.rem(me + k, n)], recv.at[k], send_a, recv_a, k) for k in order]
    for copy in extra + first:
        copy.start()
    if extras:
        for copy in extra:
            copy.wait()
        eout_ref[...] = e_ref[...] + functools.reduce(
            lambda a, k: a + erecv[k], range(2, n), erecv[1]
        )
    for copy in first:
        copy.wait()
    total = x_ref[me].astype(jnp.float32)
    for k in range(1, n):
        total = total + recv[k].astype(jnp.float32)
    mine[...] = total.astype(mine.dtype)
    out_ref[me] = total.astype(mine.dtype)
    partner = me + 1 - 2 * lax.rem(me, 2)
    half = n // 2

    def placed(src, slot, index, target):
        return pltpu.make_async_remote_copy(
            src_ref=src,
            dst_ref=out_ref.at[slot],
            send_sem=send_b.at[index],
            recv_sem=recv_b.at[index],
            device_id={"tensor": target},
            device_id_type=MESH,
        )

    ring = sorted(range(1, half), key=lambda k: -min(k, half - k))
    along = {k: placed(mine, me, k, lax.rem(me + 2 * k, n)) for k in ring}
    across = [placed(mine, me, 0, partner)]
    for copy in list(along.values()) + across:
        copy.start()
    for k in sorted(range(1, half), key=lambda k: min(k, half - k)):
        along[k].wait_recv()
        source = lax.rem(me + n - 2 * k, n)
        copy = placed(out_ref.at[source], source, half - 1 + k, partner)
        copy.start()
        across.append(copy)
    for copy in along.values():
        copy.wait_send()
    for copy in across:
        copy.wait()


def tensor_sum(x, extra, ident):
    n = lax.axis_size("tensor")
    rows, columns = x.shape
    x = x.reshape(n, rows // n, columns)
    vmem = pl.BlockSpec(memory_space=pltpu.VMEM)
    operands = [x] + ([extra] if extra is not None else [])
    shapes = [jax.ShapeDtypeStruct(x.shape, jnp.bfloat16)]
    scratch = [
        pltpu.VMEM(x.shape, x.dtype),
        pltpu.VMEM(x.shape[1:], jnp.bfloat16),
    ] + [pltpu.SemaphoreType.DMA((n,))] * 4
    if extra is not None:
        shapes.append(jax.ShapeDtypeStruct(extra.shape, extra.dtype))
        scratch += [pltpu.VMEM((n,) + extra.shape, extra.dtype)]
        scratch += [pltpu.SemaphoreType.DMA((n,))] * 2
    out = pl.pallas_call(
        functools.partial(reduce_kernel, n, extra is not None),
        out_shape=shapes,
        in_specs=[vmem] * len(operands),
        out_specs=[vmem] * len(shapes),
        scratch_shapes=scratch,
        compiler_params=pltpu.CompilerParams(
            collective_id=ident, has_side_effects=True, vmem_limit_bytes=32 << 20
        ),
        cost_estimate=pl.CostEstimate(flops=0, bytes_accessed=100 << 20, transcendentals=0),
    )(*operands)
    return [out[0].reshape(rows, columns)] + list(out[1:])


UNITS = ("ao", "no", "ap", "np", "nq",)
HALVED = ("ao", "no", "ap", "np", "nq",)
DEFERRED = (3,)
CROSSED = ((0, 2),)
SHARED = (
    11, 12, 7, 13, 15, 14, 8, 9, 16, 17, 18, 10,
)
ORDERS = (
    (
        49, 11, 27, 12, 20, 7, 54, 13, 59, 15, 21, 14, 23, 8, 9, 16, 50, 17, 24, 18, 22, 55,
        60, 0, 69, 25, 4, 10, 52, 53, 51, 57, 62, 26, 31, 37, 5, 6, 58, 2, 63, 32, 38, 56, 34,
        61, 39, 40, 3, 33, 35, 41, 45, 36, 42, 70, 72, 71, 73,
    ),
    (
        49, 11, 12, 20, 7, 54, 13, 15, 21, 14, 27, 8, 9, 16, 50, 59, 17, 64, 18, 22, 23, 55, 0,
        69, 25, 4, 24, 60, 10, 52, 53, 51, 26, 34, 57, 40, 5, 6, 2, 58, 65, 62, 70, 35, 56, 36,
        31, 41, 3, 42, 63, 67, 37, 32, 61, 38, 72, 66, 33, 71, 45, 68, 73,
    ),
    (
        49, 11, 19, 12, 7, 54, 13, 15, 21, 14, 8, 64, 9, 16, 50, 17, 18, 22, 28, 23, 55, 59, 0,
        69, 25, 4, 24, 65, 10, 52, 53, 51, 57, 26, 5, 60, 70, 6, 2, 58, 34, 40, 56, 67, 62, 72,
        35, 3, 41, 36, 42, 66, 68, 31, 37, 63, 73, 32, 38, 61, 71, 33, 45,
    ),
    (
        49, 11, 19, 12, 7, 54, 64, 13, 15, 20, 14, 8, 9, 23, 16, 50, 17, 18, 24, 21, 55, 65, 0,
        30, 4, 25, 69, 10, 52, 51, 26, 5, 6, 2, 53, 57, 67, 56, 66, 70, 3, 58, 68, 34, 40, 72,
        35, 41, 36, 42, 31, 37, 73, 32, 38, 71, 33, 45,
    ),
)


def step_names(line, near):
    numbers = [str(i) for i in range(line)]
    pairs = [str(a) + str(b) for a in range(near) for b in range(3)]
    names = ["q0", "res", "A2", "B", "lift2s", "pc1", "pc2", "stat", "statr", "normo", "normp"]
    names += [k + i for k in ("X", "O", "xs", "I", "J") for i in numbers]
    names += [k + p for k in ("G", "GX", "H") for p in pairs]
    names += [k + unit for k in ("S", "P", "fo", "fi", "e") for unit in UNITS]
    return names + [k + unit + i for k in ("r", "v") for unit in UNITS for i in numbers]


def chosen(index, values):
    picked = values[0]
    for place, value in enumerate(values[1:], 1):
        picked = jnp.where(index == place, value, picked)
    return picked


def line_order(count):
    def edge(c):
        return min(c, count - 1 - c)

    return [
        sorted(range(count), key=lambda c: (-abs(c - z), edge(c))) for z in range(count)
    ]


def segments(order, shared):
    parts, rest = [], list(order)
    for heavy in shared:
        at = rest.index(heavy)
        parts.append(rest[:at])
        rest = rest[at + 1 :]
    return parts + [rest]


def exchange_kernel(n, groups, *refs):
    attn_h, res_h, ffn_h, gain_h, mixing_h, blocks_h = refs[:6]
    attn_o, norm_o, slab_a, slab_n, rot_o, own_o = refs[6:12]
    (
        attn_v, res_v, ffn_v, attn_s, attn_y, res_y, rc, xs, xr, zs, onto, into, onto_x, into_x,
        sq_col, sq_s, sq_r, tot_s, tot_r, inv, sl_k, sl_s, sl_x, sl_p, fl_s, fl_r,
        gain, mixing, blocks, qt_f, qt_s, qt_o, qt_i, qt_x, mix, pattern, flips, base,
        local_sem, send_sem, recv_sem,
    ) = refs[12:]
    rows, features = attn_v.shape
    deep = ffn_v.shape[1] // groups
    share = xs.shape[2]
    half = features // 2
    width = slab_a.shape[2]
    slab_o = (slab_a, slab_n)
    line = n // 2
    near = line // 2
    f32, bf16 = jnp.float32, jnp.bfloat16

    s = lax.axis_index("section")
    d = lax.axis_index("dp")
    t = lax.axis_index("tensor")
    z = t // 2
    x = t - 2 * z
    u = jnp.where(d == 0, z, line - 1 - z)
    toward = 2 - 4 * d
    outward = {"tensor": t + toward}
    inner = {"tensor": t - toward}
    x_peer = {"tensor": t + 1 - 2 * x}
    y_peer = {"dp": 1 - d}
    c_peer = {"section": 1 - s}
    order = line_order(line)
    names = {}

    def sem(name):
        return names.setdefault(name, len(names))

    def remote(source, target, send, receive, device):
        return pltpu.make_async_remote_copy(
            src_ref=source,
            dst_ref=target,
            send_sem=send_sem.at[sem(send)],
            recv_sem=recv_sem.at[sem(receive)],
            device_id=device,
            device_id_type=MESH,
        )

    sent = {}

    def post(uc, make):
        make().start()
        sent.setdefault(uc, []).append(make)

    def combine(target, parts, count, kind=None, strip=48):
        def step(b, carry):
            at = pl.ds(pl.multiple_of(b * strip, strip), strip)
            total = parts[0][at, :]
            for part in parts[1:]:
                total = total + part[at, :]
            target[at, :] = total if kind is None else total.astype(kind)
            return carry

        lax.fori_loop(0, count // strip, step, 0)

    pairs = [(attn_h, attn_v), (res_h, res_v), (ffn_h, ffn_v)]
    pairs += [(gain_h, gain), (mixing_h, mixing), (blocks_h, blocks)]
    loads = [pltpu.make_async_copy(a, b, local_sem.at[i]) for i, (a, b) in enumerate(pairs)]
    for i in (5, 0, 1, 2, 3, 4):
        loads[i].start()

    barrier = pltpu.get_barrier_semaphore()
    others = [{"tensor": lax.rem(t + k, n)} for k in range(1, n)] + [y_peer, c_peer]
    for device in others:
        pl.semaphore_signal(barrier, inc=1, device_id=device, device_id_type=MESH)
    pl.semaphore_wait(barrier, n + 1)

    loads[5].wait()
    per = features // HBLK
    swap = lax.rem(blocks[0, 0], per) > 0
    owned = lax.div(blocks[0, 0], per) == t

    def q0():
        return remote(attn_s.at[1 - d], attn_y.at[1 - d], "q0", "q0", y_peer)

    def a2():
        return remote(attn_s.at[d], attn_y.at[d], "A2", "A2", y_peer)

    def b2():
        return remote(attn_s.at[2:4], attn_y.at[2:4], "B", "B", y_peer)

    def res():
        return remote(res_h, res_y, "res", "res", y_peer)

    def tot():
        return remote(tot_s, tot_r, "tot", "tot", y_peer)

    def part(b):
        return (0, 0, rows) if b == 0 else (1, (b - 1) * (rows // 2), rows // 2)

    def pc(b):
        slot, start, count = part(b)
        at = pl.ds(start, count)
        return remote(own_o.at[0, at], own_o.at[1, at], "pc" + str(b), "pc" + str(b), y_peer)

    def lift(slot, source):
        return remote(source, rc.at[slot], "lift" + str(slot), "lift" + str(slot), c_peer)

    post(None, res)

    @pl.when(s == 0)
    def _():
        lift(0, res_h).start()

    loads[0].wait()
    for k in range(4):
        here = slice(k * width, (k + 1) * width)
        there = slice((k + 2) % 4 * width, ((k + 2) % 4 + 1) * width)
        attn_s[k] = jnp.where(swap, attn_v[:, there], attn_v[:, here])

    def destination(i):
        flat = [order[a][i] for a in range(line)]
        to = chosen(u, flat)
        return jnp.where(d == 0, to, line - 1 - to)

    def setup():
        mix[...] = jnp.zeros_like(mix)
        mix[:KB, :KB] = mixing[0]
        row = lax.broadcasted_iota(jnp.int32, pattern.shape, 0)
        lane = lax.broadcasted_iota(jnp.int32, pattern.shape, 1)
        inside = jnp.bitwise_and(lane, ROOM - 1)
        hit = (row == (lane // ROOM) * KB + inside) & (inside < KB)
        pattern[...] = jnp.where(hit, 1.0, 0.0).astype(bf16)

    def odd(values):
        for shift in (8, 4, 2, 1):
            values = jnp.bitwise_xor(values, jnp.right_shift(values, shift))
        return (1 - 2 * jnp.bitwise_and(values, 1)).astype(f32)

    def rotate(target, j):
        lane = lax.broadcasted_iota(jnp.int32, (8, share), 1)
        column = blocks[0, 1] * BLK + j * share + lane
        a_col = ((column.astype(f32) + 0.5) / KB).astype(jnp.int32)
        c_col = column - a_col * KB
        depth = mix.shape[1]
        row = lax.broadcasted_iota(jnp.int32, (depth, share), 0)
        pick = jnp.where(row == c_col[:1, :], 1.0, 0.0).astype(bf16)
        mixed = jnp.dot(mix[...], pick, preferred_element_type=f32)
        for start in range(0, GROUP, 8):
            rank = start + lax.broadcasted_iota(jnp.int32, (8, share), 0)
            flips[start : start + 8, :] = odd(jnp.bitwise_and(rank, a_col))
        quad = pattern.shape[0] // KB

        for q in range(GROUP // quad):
            wide = [(mixed * flips[r : r + 1, :]).astype(bf16) for r in range(q * quad, (q + 1) * quad)]
            base[q * quad * KB : (q + 1) * quad * KB, :] = jnp.dot(
                pattern[...], jnp.concatenate(wide, axis=0), preferred_element_type=f32
            ).astype(bf16)
        a_local = groups * GROUP
        total = None
        for g in range(groups):
            part = jnp.dot(
                ffn_v[:, g * deep : (g + 1) * deep], base[...], preferred_element_type=f32
            )
            sign = odd(jnp.bitwise_and(t * a_local + g * GROUP, a_col)) / math.sqrt(a_local * n)
            part = part * sign[:1, :]
            total = part if total is None else total + part
        target[...] = total

    strip = 64

    def stat():
        loads[1].wait()

        @pl.when(s == 0)
        def _():
            rc[...] = jnp.zeros_like(rc)

        @pl.when(s > 0)
        def _():
            lift(0, res_h).wait_recv()

        def squares(b, carry):
            at = pl.ds(pl.multiple_of(b * strip, strip), strip)
            acc = jnp.zeros((strip, 128), f32)
            for c in range(features // 128):
                lanes = slice(c * 128, (c + 1) * 128)
                v = res_v[at, lanes].astype(f32) + rc[0, at, lanes].astype(f32)
                acc = acc + v * v
            sq_col[at, :] = jnp.broadcast_to(jnp.sum(acc, axis=1, keepdims=True), (strip, 128))
            return carry

        lax.fori_loop(0, rows // strip, squares, 0)
        sq_s[...] = jnp.transpose(sq_col[...])[:8, :]
        for i in range(1, n):
            post(None, functools.partial(stat_copy, i))

    def stat_copy(i):
        name = "stat" + str(i)
        return remote(sq_s, sq_r.at[i], name, name, {"tensor": lax.rem(t + i, n)})

    def inverse(slot, sums):
        spread = jnp.broadcast_to(sums[:1, :], (128, rows))
        inv[slot] = lax.rsqrt(jnp.transpose(spread) / (n * features) + EPS)

    def stats_in():
        total = sq_s[...]
        for i in range(1, n):
            stat_copy(i).wait_recv()
            total = total + sq_r[i]
        tot_s[...] = total
        post(None, tot)
        inverse(0, total)

    def normalize(slot, part):
        def step(b, carry):
            at = pl.ds(pl.multiple_of(b * strip, strip), strip)
            by = inv[slot, at, :]
            for c in range(features // 128):
                lanes = slice(c * 128, (c + 1) * 128)
                v = part[at, lanes].astype(f32) + rc[slot, at, lanes].astype(f32)
                norm_o[slot, at, lanes] = (v * by * gain[:, lanes]).astype(bf16)
            return carry

        lax.fori_loop(0, rows // strip, step, 0)

    def normalize_peer():
        tot().wait_recv()
        inverse(1, tot_r[...])

        @pl.when(s > 0)
        def _():
            res().wait_recv()
            lift(1, res_y).wait_recv()

        normalize(1, res_y)

    def heavy(name):
        if name[0] in "XO":
            i = int(name[1:])
            column = 1 - x if name[0] == "X" else x
            rotate((xs if name[0] == "X" else zs).at[i], 2 * destination(i) + column)
        elif name == "stat":
            stat()
        elif name == "statr":
            stats_in()
        elif name == "normo":
            normalize(0, res_v)
        else:
            normalize_peer()

    mine = pl.ds(pl.multiple_of(d * width, width), width)
    upper = pl.ds(pl.multiple_of(half + d * width, width), width)

    def slab_source(name):
        slot = 0 if name[1] == "o" else 1
        start, count = span(name)
        at = slice(start, start + count)
        if name[0] == "a":
            value = attn_s[d, at] if slot == 0 else attn_y[d, at]
        else:
            value = jnp.where(swap, norm_o[slot, at, upper], norm_o[slot, at, mine])
        return jnp.where(owned, value, jnp.zeros_like(value))

    def span(unit):
        whole = unit[1] == "o" or unit[0] + "q" not in UNITS
        count = rows if whole else rows // 2
        return (rows // 2 if unit[1] == "q" else 0), count

    low = rows // line
    paired_up = set()

    def attn_ready(uc, unit):
        if unit[0] == "a" and unit[1] != "o" and ("q0", uc) not in paired_up:
            paired_up.add(("q0", uc))
            q0().wait_recv()

    def own_ready(uc, b):
        if b > 0 and (uc, b) not in paired_up:
            paired_up.add((uc, b))
            pc(b).wait_recv()

    def light(uc, name):
        def slab(unit):
            return slab_o[0 if unit[0] == "a" else 1].at[0 if unit[1] == "o" else 1]

        def half_of(unit, column):
            start, count = span(unit)
            tall = count // 2
            return slab(unit).at[pl.ds(pl.multiple_of(start + column * tall, tall), tall)]

        def quarter_of(unit, to):
            return slab(unit).at[to * low : (to + 1) * low]

        def place(source, column, b):
            spot = jnp.where(d == 0, source, near - 1 - source) * 2 + column
            slot, start, count = part(b)
            lanes = pl.ds(pl.multiple_of(spot * share, share), share)
            return rot_o.at[slot, pl.ds(start, count), lanes]

        def shared_from(uc, source, b):
            slot, start, count = part(b)
            return own_o.at[slot, pl.ds(start, count)] if uc == source else place(source, x, b)

        def gather(source, b, way, device):
            name = "g" + str(source) + str(b)
            where = place(source, x, b)
            return remote(shared_from(uc, source, b), where, name + way, name, device)

        if name == "q0":
            post(uc, q0)
        elif name == "A2":
            post(uc, a2)
        elif name == "B":
            post(uc, b2)
        elif name == "lift2s":

            @pl.when(s == 0)
            def _():
                res().wait_recv()
                lift(1, res_y).start()

        elif name[:2] == "pc":
            post(uc, lambda: pc(int(name[2])))
        elif name[:2] == "xs":
            i = int(name[2:])
            post(uc, lambda: remote(xs.at[i], xr.at[i], "x" + str(i), "x" + str(i), x_peer))
        elif name[0] in "IJ":
            i = int(name[1:])
            to = order[uc][i]
            own = name[0] == "I"
            store = zs if own else xs
            held = store.at[i]
            parts = [held]

            def across():
                return remote(xs.at[i], xr.at[i], "x" + str(i), "x" + str(i), x_peer)

            def along(way):
                key = ("L" if way == 0 else "R") + ("" if own else "x") + str(to)
                slots = (onto if own else onto_x) if way == 0 else (into if own else into_x)
                send = ("zs" if own else "xs") + str(i)
                return remote(store.at[i], slots.at[to], send, key, outward if way == 0 else inner)

            if own and (to == uc or to not in DEFERRED):
                across().wait_recv()
                parts.append(xr.at[i])
            if to >= uc and uc > 0:
                along(0).wait_recv()
                parts.append((onto if own else onto_x).at[to])
            if to <= uc and uc < line - 1:
                along(1).wait_recv()
                parts.append((into if own else into_x).at[to])
            if own and to == uc:
                combine(own_o.at[0], parts, rows, bf16)
            elif len(parts) > 1:
                combine(held, parts, rows)
            if to > uc:
                post(uc, lambda: along(0))
            elif to < uc:
                post(uc, lambda: along(1))
            elif not own:
                post(uc, across)
        elif name[:2] == "GX":
            source, b = int(name[2]), int(name[3])
            key = "gx" + name[2:]
            if (source, b) in CROSSED:
                own_ready(uc, b)
            post(uc, lambda: remote(shared_from(uc, source, b), place(source, x, b), key, key, x_peer))
        elif name[0] == "H":
            source, b = int(name[1]), int(name[2])
            where, key = place(source, 1 - x, b), "h" + name[1:]
            if uc == source:
                remote(where, where, "gx" + name[1:], "gx" + name[1:], x_peer).wait_recv()
            else:
                remote(where, where, key + "o", key, outward).wait_recv()

            def ahead(way, device):
                spot = place(source, 1 - x, b)
                return remote(spot, spot, key + way, key, device)

            if uc >= source and uc < line - 1:
                post(uc, lambda: ahead("o", outward))
            if uc <= source and uc > 0:
                post(uc, lambda: ahead("i", inner))
        elif name[0] == "G":
            source, b = int(name[1]), int(name[2])
            if uc == source:
                own_ready(uc, b)
            else:
                gather(source, b, "o", outward).wait_recv()
            if uc >= source and uc < line - 1:
                post(uc, lambda: gather(source, b, "o", outward))
            if uc <= source and uc > 0:
                post(uc, lambda: gather(source, b, "i", inner))
            if uc == source:
                combine(place(source, x, b), [shared_from(uc, source, b)], part(b)[2])
        else:
            slabs(uc, name, half_of, quarter_of)

    def slabs(uc, name, half_of, quarter_of):
        unit = next(k for k in UNITS if k in name)
        kind, rest = name.split(unit)
        k = UNITS.index(unit)
        tall = span(unit)[1] // 2
        used = slice(0, tall)

        def cross():
            return remote(sl_s.at[k, used], sl_x.at[k, used], "S" + unit, "S" + unit, x_peer)

        def flood(way):
            key = "fo" if way == 0 else "fi"
            device = outward if way == 0 else inner
            return remote(fl_s.at[k, way, used], fl_r.at[k, way, used], key + unit, key + unit, device)

        def back():
            return remote(half_of(unit, x), half_of(unit, x), "b" + unit, "b" + unit, x_peer)

        def reduce(to):
            key = "r" + unit + str(to)
            if to > uc:
                return remote(qt_s.at[k, to], qt_o.at[k, to], key, key + "o", outward)
            if to < uc:
                return remote(qt_s.at[k, to], qt_i.at[k, to], key, key + "i", inner)
            return remote(qt_s.at[k, to], qt_x.at[k], key, "rx" + unit, x_peer)

        def wave(source, way, device):
            key = "w" + unit + str(source)
            return remote(quarter_of(unit, source), quarter_of(unit, source), key + way, key, device)

        if unit in HALVED:
            if kind == "S":
                attn_ready(uc, unit)
                value = slab_source(unit)
                first, second = value[:tall], value[tall:]
                sl_k[k, used] = jnp.where(x == 0, first, second)
                sl_s[k, used] = jnp.where(x == 0, second, first)
                post(uc, cross)
            elif kind == "P":
                cross().wait_recv()
                combine(sl_p.at[k], [sl_k.at[k], sl_x.at[k]], tall)
            elif kind == "fo":
                parts = [sl_p.at[k]]
                if uc > 0:
                    flood(0).wait_recv()
                    parts.append(fl_r.at[k, 0])
                combine(fl_s.at[k, 0], parts, tall)
                post(uc, lambda: flood(0))
            elif kind == "fi":
                parts = [sl_p.at[k]]
                if uc < line - 1:
                    flood(1).wait_recv()
                    parts.append(fl_r.at[k, 1])
                combine(fl_s.at[k, 1], parts, tall)
                post(uc, lambda: flood(1))
            else:
                parts = [sl_p.at[k]]
                if uc > 0:
                    parts.append(fl_r.at[k, 0])
                    if uc == line - 1:
                        flood(0).wait_recv()
                if uc < line - 1:
                    parts.append(fl_r.at[k, 1])
                    if uc == 0:
                        flood(1).wait_recv()
                combine(half_of(unit, x), parts, tall)
                post(uc, back)
            return
        if kind == "S":
            attn_ready(uc, unit)
            qt_f[k] = slab_source(unit)
        elif kind == "r":
            to = int(rest)
            parts = [qt_f.at[k, to * low : (to + 1) * low]]
            if to >= uc and uc > 0:
                remote(qt_s.at[k, to], qt_o.at[k, to], "r" + unit + rest, "r" + unit + rest + "o", outward).wait_recv()
                parts.append(qt_o.at[k, to])
            if to <= uc and uc < line - 1:
                remote(qt_s.at[k, to], qt_i.at[k, to], "r" + unit + rest, "r" + unit + rest + "i", inner).wait_recv()
                parts.append(qt_i.at[k, to])
            combine(qt_s.at[k, to], parts, low)
            post(uc, lambda: reduce(to))
        else:
            source = int(rest)
            if source == uc:
                reduce(uc).wait_recv()
                combine(quarter_of(unit, uc), [qt_s.at[k, uc], qt_x.at[k]], low)
            else:
                wave(source, "o", outward).wait_recv()
            if source <= uc and uc < line - 1:
                post(uc, lambda: wave(source, "o", outward))
            if source >= uc and uc > 0:
                post(uc, lambda: wave(source, "i", inner))

    steps = step_names(line, near)
    shared = [steps[i] for i in SHARED]
    parts = [segments([steps[i] for i in o], shared) for o in ORDERS]
    started = [False]
    for k, name in enumerate(shared + [None]):
        for uc in range(line):
            if parts[uc][k]:

                @pl.when(u == uc)
                def _():
                    for each in parts[uc][k]:
                        light(uc, each)

        if name is None:
            break
        if name[0] in "XO" and not started[0]:
            started[0] = True
            loads[3].wait()
            loads[4].wait()
            setup()
            loads[2].wait()
        heavy(name)

    @pl.when(u >= near)
    def _():
        pc(1).wait_recv()
        pc(2).wait_recv()

    assert len(names) <= SEMAPHORES, len(names)

    combine(attn_o.at[0], [attn_v], rows)
    a2().wait_recv()
    b2().wait_recv()
    for k in range(4):
        here = slice(k * width, (k + 1) * width)
        attn_o[1, :, here] = jnp.where(swap, attn_y[(k + 2) % 4], attn_y[k])

    for unit in HALVED:
        m, b = 0 if unit[0] == "a" else 1, 0 if unit[1] == "o" else 1
        start, count = span(unit)
        tall = count // 2
        where = slab_o[m].at[b, pl.ds(pl.multiple_of(start + (1 - x) * tall, tall), tall)]
        remote(where, where, "b" + unit, "b" + unit, x_peer).wait_recv()
    for source in range(near):
        for b in range(3):
            if (source, b) in CROSSED:
                continue
            slot, start, count = part(b)
            spot = jnp.where(d == 0, source, near - 1 - source) * 2 + 1 - x
            lanes = pl.ds(pl.multiple_of(spot * share, share), share)
            where = rot_o.at[slot, pl.ds(start, count), lanes]
            key = "gx" + str(source) + str(b)
            remote(where, where, key, key, x_peer).wait_recv()

    for make in sent[None]:
        make().wait_send()
    for uc in range(line):

        @pl.when(u == uc)
        def _():
            for make in sent[uc]:
                make().wait_send()

    @pl.when(s == 0)
    def _():
        lift(0, res_h).wait_send()
        lift(1, res_y).wait_send()


SEMAPHORES = 192
ROOM = 64


def exchanged(*operands):
    attn, res, ffn, gain, mixing, blocks = operands
    n = lax.axis_size("tensor")
    rows, features = attn.shape
    share, width = BLK // n, HBLK // 2
    line = n // 2
    groups = ffn.shape[1] // (GROUP * KB)
    halved = len(UNITS)
    units = 1 if len(HALVED) == len(UNITS) else len(UNITS)
    f32, bf16 = jnp.float32, jnp.bfloat16
    vmem = pl.BlockSpec(memory_space=pltpu.VMEM)
    return pl.pallas_call(
        functools.partial(exchange_kernel, n, groups),
        out_shape=[
            jax.ShapeDtypeStruct((2, rows, features), bf16),
            jax.ShapeDtypeStruct((2, rows, features), bf16),
            jax.ShapeDtypeStruct((2, rows, width), bf16),
            jax.ShapeDtypeStruct((2, rows, width), bf16),
            jax.ShapeDtypeStruct((2, rows, BLK // 2), bf16),
            jax.ShapeDtypeStruct((2, rows, share), bf16),
        ],
        in_specs=[pl.BlockSpec(memory_space=pltpu.HBM)] * 6,
        out_specs=[vmem] * 6,
        scratch_shapes=[
            pltpu.VMEM((rows, features), bf16),
            pltpu.VMEM((rows, features), bf16),
            pltpu.VMEM(ffn.shape, bf16),
            pltpu.VMEM((4, rows, width), bf16),
            pltpu.VMEM((4, rows, width), bf16),
            pltpu.VMEM((rows, features), bf16),
            pltpu.VMEM((2, rows, features), bf16),
            pltpu.VMEM((line, rows, share), f32),
            pltpu.VMEM((line, rows, share), f32),
            pltpu.VMEM((line, rows, share), f32),
            pltpu.VMEM((line, rows, share), f32),
            pltpu.VMEM((line, rows, share), f32),
            pltpu.VMEM((line if DEFERRED else 1, rows, share), f32),
            pltpu.VMEM((line if DEFERRED else 1, rows, share), f32),
            pltpu.VMEM((rows, 128), f32),
            pltpu.VMEM((8, rows), f32),
            pltpu.VMEM((n, 8, rows), f32),
            pltpu.VMEM((8, rows), f32),
            pltpu.VMEM((8, rows), f32),
            pltpu.VMEM((2, rows, 128), f32),
            pltpu.VMEM((halved, rows // 2, width), bf16),
            pltpu.VMEM((halved, rows // 2, width), bf16),
            pltpu.VMEM((halved, rows // 2, width), bf16),
            pltpu.VMEM((halved, rows // 2, width), bf16),
            pltpu.VMEM((halved, 2, rows // 2, width), bf16),
            pltpu.VMEM((halved, 2, rows // 2, width), bf16),
            pltpu.VMEM(gain.shape, f32),
            pltpu.VMEM(mixing.shape, bf16),
            pltpu.SMEM(blocks.shape, jnp.int32),
            pltpu.VMEM((units, rows, width), bf16),
            pltpu.VMEM((units, line, rows // line, width), bf16),
            pltpu.VMEM((units, line, rows // line, width), bf16),
            pltpu.VMEM((units, line, rows // line, width), bf16),
            pltpu.VMEM((units, rows // line, width), bf16),
            pltpu.VMEM((ROOM, 128), bf16),
            pltpu.VMEM((4 * KB, 4 * ROOM), bf16),
            pltpu.VMEM((GROUP, share), f32),
            pltpu.VMEM((GROUP * KB, share), bf16),
            pltpu.SemaphoreType.DMA((6,)),
            pltpu.SemaphoreType.DMA((SEMAPHORES,)),
            pltpu.SemaphoreType.DMA((SEMAPHORES,)),
        ],
        compiler_params=pltpu.CompilerParams(
            collective_id=2, has_side_effects=True, vmem_limit_bytes=43 << 20
        ),
    )(*[pltpu.with_memory_space_constraint(v, pltpu.HBM) for v in operands])


def parity_sign(values):
    return (1 - 2 * (lax.population_count(values) & 1)).astype(jnp.float32)


def gram(left, right):
    return lax.dot_general(
        left, right, (((0,), (0,)), ((), ())), preferred_element_type=jnp.float32
    )


def general(residual_parts, attn_out, ffn_input, norm_gain, mixing, blocks):
    local_d = residual_parts.shape[2]
    local_f = ffn_input.shape[2]
    token_rows = residual_parts.shape[1]
    dp_count = lax.axis_size("dp")
    dp_member = lax.axis_index("dp")
    tensor_count = lax.axis_size("tensor")
    member = lax.axis_index("tensor")
    own_part = residual_parts[0]
    parts = gathered(own_part, "dp")
    attention = jnp.concatenate(gathered(attn_out[0], "dp"), axis=0)
    earlier = [passed_along(part, "section", 1) for part in parts]
    layers = [
        e.astype(jnp.float32) + p.astype(jnp.float32) for e, p in zip(earlier, parts)
    ]
    squares = jnp.sum(layers[0] * layers[0], axis=1).reshape(token_rows // 128, 128)

    a_local = local_f // KB
    order_a = a_local * tensor_count
    deep = GROUP * KB
    column = blocks[0, 1] * BLK + jnp.arange(BLK, dtype=jnp.int32)
    a_col, c_col = column // KB, column % KB
    pick = (jnp.arange(KB, dtype=jnp.int32)[:, None] == c_col[None, :]).astype(jnp.bfloat16)
    spread = jnp.dot(
        jnp.tile(mixing[0], (GROUP, 1)), pick, preferred_element_type=jnp.float32
    )
    row_a = jnp.arange(deep, dtype=jnp.int32) // KB
    base = (spread * parity_sign(row_a[:, None] & a_col[None, :])).astype(jnp.bfloat16)
    term = None
    for g in range(a_local // GROUP):
        sign = parity_sign((member * a_local + g * GROUP) & a_col) / math.sqrt(order_a)
        piece = jnp.dot(
            ffn_input[0, :, g * deep : (g + 1) * deep], base, preferred_element_type=jnp.float32
        )
        piece = piece * sign[None, :]
        term = piece if term is None else term + piece

    rotated, square_own = tensor_sum(term, squares, 0)

    square_total = gathered(square_own, "dp")
    rotated, square_total = lax.optimization_barrier((rotated, square_total))
    square_total = [s.reshape(token_rows) for s in square_total]
    share = BLK // tensor_count
    own_cols = lax.dynamic_slice_in_dim(rotated, member * share, share, 1)
    part_down = gram(own_cols, rotated)
    half = BLK // dp_count
    if dp_count == 2:
        kept = lax.dynamic_slice_in_dim(part_down, dp_member * half, half, 1)
        sent = lax.dynamic_slice_in_dim(part_down, (1 - dp_member) * half, half, 1)
        sum_down = kept + shifted(sent, "dp", 1)
    else:
        sum_down = lax.psum_scatter(part_down, "dp", scatter_dimension=1, tiled=True)

    normed = jnp.concatenate(
        [
            (x * lax.rsqrt(s / D + EPS)[:, None] * norm_gain[0][None, :]).astype(jnp.bfloat16)
            for x, s in zip(layers, square_total)
        ],
        axis=0,
    )
    first_col = blocks[0, 0] * HBLK
    width = HBLK // dp_count
    offset = first_col % local_d + dp_member * width
    owned = first_col // local_d == member
    slab = jnp.concatenate(
        [
            lax.dynamic_slice_in_dim(normed, offset, width, 1),
            lax.dynamic_slice_in_dim(attention, offset, width, 1),
        ],
        axis=0,
    )
    slab = jnp.where(owned, slab, 0).astype(jnp.bfloat16)
    (got,) = tensor_sum(slab, None, 1)
    tokens = token_rows * dp_count
    scale = 2.0 / tokens
    hess_in = (scale * gram(normed, got[:tokens]))[None]
    hess_o = (scale * gram(attention, got[tokens:]))[None]
    hess_down = (scale * sum_down)[None]
    return (hess_in, hess_o, hess_down)


STRIPS = 4


def gram_kernel(scale, attn, normed, slab_a, slab_n, rotated, own, *refs):
    out_in, out_o, out_down, held, held_down, done = refs

    def put(target, at, place):
        return pltpu.make_async_copy(held.at[place], target.at[at], done.at[place])

    held_down[...] = scale * gram(own[...], rotated[...])
    down = pltpu.make_async_copy(held_down, out_down, done.at[2 * STRIPS])
    down.start()
    tall = normed.shape[1] // STRIPS
    copies = []
    for k, (left, right, target) in enumerate([(attn, slab_a, out_o), (normed, slab_n, out_in)]):
        for strip in range(STRIPS):
            at = slice(strip * tall, (strip + 1) * tall)
            place = k * STRIPS + strip
            held[place] = scale * gram(left[:, at], right[...])
            copies.append(put(target, pl.ds(strip * tall, tall), place))
            copies[-1].start()
    for copy in copies + [down]:
        copy.wait()


def grams(scale, attn, normed, slab_a, slab_n, rotated, own):
    features, width = normed.shape[1], slab_n.shape[1]
    down = (own.shape[1], rotated.shape[1])
    f32 = jnp.float32
    return pl.pallas_call(
        functools.partial(gram_kernel, scale),
        out_shape=[
            jax.ShapeDtypeStruct((features, width), f32),
            jax.ShapeDtypeStruct((features, width), f32),
            jax.ShapeDtypeStruct(down, f32),
        ],
        in_specs=[pl.BlockSpec(memory_space=pltpu.VMEM)] * 6,
        out_specs=[pl.BlockSpec(memory_space=pl.ANY)] * 3,
        scratch_shapes=[
            pltpu.VMEM((2 * STRIPS, features // STRIPS, width), f32),
            pltpu.VMEM(down, f32),
            pltpu.SemaphoreType.DMA((2 * STRIPS + 1,)),
        ],
        compiler_params=pltpu.CompilerParams(vmem_limit_bytes=20 << 20),
    )(attn, normed, slab_a, slab_n, rotated, own)


def paired(residual_parts, attn_out, ffn_input, norm_gain, mixing, blocks):
    local_d = residual_parts.shape[2]
    token_rows = residual_parts.shape[1]
    share = BLK // lax.axis_size("tensor")
    attention, normed, slab_a, slab_n, rotated, own = exchanged(
        attn_out[0], residual_parts[0], ffn_input[0], norm_gain, mixing, blocks
    )
    tokens = token_rows * 2
    scale = 2.0 / tokens
    attention, normed = attention.reshape(tokens, local_d), normed.reshape(tokens, local_d)
    slab_a, slab_n = slab_a.reshape(tokens, HBLK // 2), slab_n.reshape(tokens, HBLK // 2)
    hess_in, hess_o, hess_down = grams(
        scale,
        attention,
        normed,
        slab_a,
        slab_n,
        rotated.reshape(tokens, BLK // 2),
        own.reshape(tokens, share),
    )
    return (hess_in[None], hess_o[None], hess_down[None])


def local(*arguments):
    n = lax.axis_size("tensor")
    by_pairs = lax.axis_size("dp") == 2 and lax.axis_size("section") == 2 and n == 2 * len(ORDERS)
    if by_pairs and arguments[0].shape[2] == 2 * HBLK:
        return paired(*arguments)
    return general(*arguments)


def solution(mesh):
    return jax.shard_map(
        local,
        mesh=mesh,
        in_specs=(
            P("section", "dp", "tensor"),
            P("section", "dp", "tensor"),
            P("section", "dp", "tensor"),
            P("section", "tensor"),
            P("section", None, None),
            P("section", None),
        ),
        out_specs=(
            P("section", "tensor", "dp"),
            P("section", "tensor", "dp"),
            P("section", "tensor", "dp"),
        ),
        check_vma=False,
    )
```

```python
import functools
import math

import jax
import jax.numpy as jnp
from jax import lax
from jax.experimental import pallas as pl
from jax.experimental.pallas import tpu as pltpu
from jax.sharding import PartitionSpec as P

D = 16384
KB = 52
HBLK = 1024
BLK = 2048
GROUP = 32


EPS = 1e-05

MESH = pl.DeviceIdType.MESH


def passed_along(x, axis, by):
    devices = lax.axis_size(axis)
    pairs = [(i, i + by) for i in range(devices) if 0 <= i + by < devices]
    return lax.ppermute(x, axis, pairs)


def shifted(x, axis, by):
    devices = lax.axis_size(axis)
    return lax.ppermute(x, axis, [(i, (i + by) % devices) for i in range(devices)])


def gathered(x, axis):
    return [x] + [shifted(x, axis, by) for by in range(1, lax.axis_size(axis))]


def reduce_kernel(n, extras, *refs):
    x_ref, refs = refs[0], refs[1:]
    e_ref, refs = (refs[0], refs[1:]) if extras else (None, refs)
    out_ref, refs = refs[0], refs[1:]
    eout_ref, refs = (refs[0], refs[1:]) if extras else (None, refs)
    recv, mine, send_a, recv_a, send_b, recv_b = refs[:6]
    me = lax.axis_index("tensor")

    barrier = pltpu.get_barrier_semaphore()
    for k in range(1, n):
        pl.semaphore_signal(
            barrier, inc=1, device_id={"tensor": lax.rem(me + k, n)}, device_id_type=MESH
        )
    pl.semaphore_wait(barrier, n - 1)

    def remote(src, dst, send, receive, k):
        return pltpu.make_async_remote_copy(
            src_ref=src,
            dst_ref=dst,
            send_sem=send.at[k],
            recv_sem=receive.at[k],
            device_id={"tensor": lax.rem(me + k, n)},
            device_id_type=MESH,
        )

    order = sorted(range(1, n), key=lambda k: -min(k, n - k))
    extra = []
    if extras:
        erecv, send_e, recv_e = refs[6:]
        extra = [remote(e_ref, erecv.at[k], send_e, recv_e, k) for k in order]
    first = [remote(x_ref.at[lax.rem(me + k, n)], recv.at[k], send_a, recv_a, k) for k in order]
    for copy in extra + first:
        copy.start()
    if extras:
        for copy in extra:
            copy.wait()
        eout_ref[...] = e_ref[...] + functools.reduce(
            lambda a, k: a + erecv[k], range(2, n), erecv[1]
        )
    for copy in first:
        copy.wait()
    total = x_ref[me].astype(jnp.float32)
    for k in range(1, n):
        total = total + recv[k].astype(jnp.float32)
    mine[...] = total.astype(mine.dtype)
    out_ref[me] = total.astype(mine.dtype)
    partner = me + 1 - 2 * lax.rem(me, 2)
    half = n // 2

    def placed(src, slot, index, target):
        return pltpu.make_async_remote_copy(
            src_ref=src,
            dst_ref=out_ref.at[slot],
            send_sem=send_b.at[index],
            recv_sem=recv_b.at[index],
            device_id={"tensor": target},
            device_id_type=MESH,
        )

    ring = sorted(range(1, half), key=lambda k: -min(k, half - k))
    along = {k: placed(mine, me, k, lax.rem(me + 2 * k, n)) for k in ring}
    across = [placed(mine, me, 0, partner)]
    for copy in list(along.values()) + across:
        copy.start()
    for k in sorted(range(1, half), key=lambda k: min(k, half - k)):
        along[k].wait_recv()
        source = lax.rem(me + n - 2 * k, n)
        copy = placed(out_ref.at[source], source, half - 1 + k, partner)
        copy.start()
        across.append(copy)
    for copy in along.values():
        copy.wait_send()
    for copy in across:
        copy.wait()


def tensor_sum(x, extra, ident):
    n = lax.axis_size("tensor")
    rows, columns = x.shape
    x = x.reshape(n, rows // n, columns)
    vmem = pl.BlockSpec(memory_space=pltpu.VMEM)
    operands = [x] + ([extra] if extra is not None else [])
    shapes = [jax.ShapeDtypeStruct(x.shape, jnp.bfloat16)]
    scratch = [
        pltpu.VMEM(x.shape, x.dtype),
        pltpu.VMEM(x.shape[1:], jnp.bfloat16),
    ] + [pltpu.SemaphoreType.DMA((n,))] * 4
    if extra is not None:
        shapes.append(jax.ShapeDtypeStruct(extra.shape, extra.dtype))
        scratch += [pltpu.VMEM((n,) + extra.shape, extra.dtype)]
        scratch += [pltpu.SemaphoreType.DMA((n,))] * 2
    out = pl.pallas_call(
        functools.partial(reduce_kernel, n, extra is not None),
        out_shape=shapes,
        in_specs=[vmem] * len(operands),
        out_specs=[vmem] * len(shapes),
        scratch_shapes=scratch,
        compiler_params=pltpu.CompilerParams(
            collective_id=ident, has_side_effects=True, vmem_limit_bytes=32 << 20
        ),
        cost_estimate=pl.CostEstimate(flops=0, bytes_accessed=100 << 20, transcendentals=0),
    )(*operands)
    return [out[0].reshape(rows, columns)] + list(out[1:])


UNITS = ("ao", "no", "ap", "np", "nq",)
HALVED = ("ao", "no", "ap", "np", "nq",)
DEFERRED = (3,)
CROSSED = ((0, 2),)
SHARED = (
    11, 12, 7, 13, 15, 14, 8, 9, 16, 17, 18, 10,
)
ORDERS = (
    (
        49, 11, 27, 12, 20, 7, 54, 13, 59, 15, 21, 14, 23, 8, 9, 16, 50, 17, 24, 18, 22, 55,
        60, 0, 69, 25, 4, 10, 52, 53, 51, 57, 62, 26, 31, 37, 5, 6, 58, 2, 63, 32, 38, 56, 34,
        61, 39, 40, 3, 33, 35, 41, 45, 36, 42, 70, 72, 71, 73,
    ),
    (
        49, 11, 12, 20, 7, 54, 13, 15, 21, 14, 27, 8, 9, 16, 50, 59, 17, 64, 18, 22, 23, 55, 0,
        69, 25, 4, 24, 60, 10, 52, 53, 51, 26, 34, 57, 40, 5, 6, 2, 58, 65, 62, 70, 35, 56, 36,
        31, 41, 3, 42, 63, 67, 37, 32, 61, 38, 72, 66, 33, 71, 45, 68, 73,
    ),
    (
        49, 11, 19, 12, 7, 54, 13, 15, 21, 14, 8, 64, 9, 16, 50, 17, 18, 22, 28, 23, 55, 59, 0,
        69, 25, 4, 24, 65, 10, 52, 53, 51, 57, 26, 5, 60, 70, 6, 2, 58, 34, 40, 56, 67, 62, 72,
        35, 3, 41, 36, 42, 66, 68, 31, 37, 63, 73, 32, 38, 61, 71, 33, 45,
    ),
    (
        49, 11, 19, 12, 7, 54, 64, 13, 15, 20, 14, 8, 9, 23, 16, 50, 17, 18, 24, 21, 55, 65, 0,
        30, 4, 25, 69, 10, 52, 51, 26, 5, 6, 2, 53, 57, 67, 56, 66, 70, 3, 58, 68, 34, 40, 72,
        35, 41, 36, 42, 31, 37, 73, 32, 38, 71, 33, 45,
    ),
)


def step_names(line, near):
    numbers = [str(i) for i in range(line)]
    pairs = [str(a) + str(b) for a in range(near) for b in range(3)]
    names = ["q0", "res", "A2", "B", "lift2s", "pc1", "pc2", "stat", "statr", "normo", "normp"]
    names += [k + i for k in ("X", "O", "xs", "I", "J") for i in numbers]
    names += [k + p for k in ("G", "GX", "H") for p in pairs]
    names += [k + unit for k in ("S", "P", "fo", "fi", "e") for unit in UNITS]
    return names + [k + unit + i for k in ("r", "v") for unit in UNITS for i in numbers]


def chosen(index, values):
    picked = values[0]
    for place, value in enumerate(values[1:], 1):
        picked = jnp.where(index == place, value, picked)
    return picked


def line_order(count):
    def edge(c):
        return min(c, count - 1 - c)

    return [
        sorted(range(count), key=lambda c: (-abs(c - z), edge(c))) for z in range(count)
    ]


def segments(order, shared):
    parts, rest = [], list(order)
    for heavy in shared:
        at = rest.index(heavy)
        parts.append(rest[:at])
        rest = rest[at + 1 :]
    return parts + [rest]


def exchange_kernel(n, groups, *refs):
    attn_h, res_h, ffn_h, gain_h, mixing_h, blocks_h = refs[:6]
    attn_o, norm_o, slab_a, slab_n, rot_o, own_o = refs[6:12]
    (
        attn_v, res_v, ffn_v, attn_s, attn_y, res_y, rc, xs, xr, zs, onto, into, onto_x, into_x,
        sq_col, sq_s, sq_r, tot_s, tot_r, inv, sl_k, sl_s, sl_x, sl_p, fl_s, fl_r,
        gain, mixing, blocks, qt_f, qt_s, qt_o, qt_i, qt_x, mix, pattern, flips, base,
        local_sem, send_sem, recv_sem,
    ) = refs[12:]
    rows, features = attn_v.shape
    deep = ffn_v.shape[1] // groups
    share = xs.shape[2]
    half = features // 2
    width = slab_a.shape[2]
    slab_o = (slab_a, slab_n)
    line = n // 2
    near = line // 2
    f32, bf16 = jnp.float32, jnp.bfloat16

    s = lax.axis_index("section")
    d = lax.axis_index("dp")
    t = lax.axis_index("tensor")
    z = t // 2
    x = t - 2 * z
    u = jnp.where(d == 0, z, line - 1 - z)
    toward = 2 - 4 * d
    outward = {"tensor": lax.rem(t + toward + n, n)}
    inner = {"tensor": lax.rem(t - toward + n, n)}
    x_peer = {"tensor": t + 1 - 2 * x}
    y_peer = {"dp": 1 - d}
    c_peer = {"section": 1 - s}
    order = line_order(line)
    names = {}

    def sem(name):
        return names.setdefault(name, len(names))

    def remote(source, target, send, receive, device):
        return pltpu.make_async_remote_copy(
            src_ref=source,
            dst_ref=target,
            send_sem=send_sem.at[sem(send)],
            recv_sem=recv_sem.at[sem(receive)],
            device_id=device,
            device_id_type=MESH,
        )

    sent = {}

    def post(uc, make):
        make().start()
        sent.setdefault(uc, []).append(make)

    def combine(target, parts, count, kind=None, strip=48):
        def step(b, carry):
            at = pl.ds(pl.multiple_of(b * strip, strip), strip)
            total = parts[0][at, :]
            for part in parts[1:]:
                total = total + part[at, :]
            target[at, :] = total if kind is None else total.astype(kind)
            return carry

        lax.fori_loop(0, count // strip, step, 0)

    pairs = [(attn_h, attn_v), (res_h, res_v), (ffn_h, ffn_v)]
    pairs += [(gain_h, gain), (mixing_h, mixing), (blocks_h, blocks)]
    loads = [pltpu.make_async_copy(a, b, local_sem.at[i]) for i, (a, b) in enumerate(pairs)]
    for i in (5, 0, 1, 2, 3, 4):
        loads[i].start()

    barrier = pltpu.get_barrier_semaphore()
    others = [{"tensor": lax.rem(t + k, n)} for k in range(1, n)] + [y_peer, c_peer]
    for device in others:
        pl.semaphore_signal(barrier, inc=1, device_id=device, device_id_type=MESH)
    pl.semaphore_wait(barrier, n + 1)

    loads[5].wait()
    per = features // HBLK
    swap = lax.rem(blocks[0, 0], per) > 0
    owned = lax.div(blocks[0, 0], per) == t

    def q0():
        return remote(attn_s.at[1 - d], attn_y.at[1 - d], "q0", "q0", y_peer)

    def a2():
        return remote(attn_s.at[d], attn_y.at[d], "A2", "A2", y_peer)

    def b2():
        return remote(attn_s.at[2:4], attn_y.at[2:4], "B", "B", y_peer)

    def res():
        return remote(res_h, res_y, "res", "res", y_peer)

    def tot():
        return remote(tot_s, tot_r, "tot", "tot", y_peer)

    def part(b):
        return (0, 0, rows) if b == 0 else (1, (b - 1) * (rows // 2), rows // 2)

    def pc(b):
        slot, start, count = part(b)
        at = pl.ds(start, count)
        return remote(own_o.at[0, at], own_o.at[1, at], "pc" + str(b), "pc" + str(b), y_peer)

    def lift(slot, source):
        return remote(source, rc.at[slot], "lift" + str(slot), "lift" + str(slot), c_peer)

    post(None, res)

    @pl.when(s == 0)
    def _():
        lift(0, res_h).start()

    loads[0].wait()
    for k in range(4):
        here = slice(k * width, (k + 1) * width)
        there = slice((k + 2) % 4 * width, ((k + 2) % 4 + 1) * width)
        attn_s[k] = jnp.where(swap, attn_v[:, there], attn_v[:, here])

    def destination(i):
        flat = [order[a][i] for a in range(line)]
        to = chosen(u, flat)
        return jnp.where(d == 0, to, line - 1 - to)

    def setup():
        mix[...] = jnp.zeros_like(mix)
        mix[:KB, :KB] = mixing[0]
        row = lax.broadcasted_iota(jnp.int32, pattern.shape, 0)
        lane = lax.broadcasted_iota(jnp.int32, pattern.shape, 1)
        inside = jnp.bitwise_and(lane, ROOM - 1)
        hit = (row == (lane // ROOM) * KB + inside) & (inside < KB)
        pattern[...] = jnp.where(hit, 1.0, 0.0).astype(bf16)

    def odd(values):
        for shift in (8, 4, 2, 1):
            values = jnp.bitwise_xor(values, jnp.right_shift(values, shift))
        return (1 - 2 * jnp.bitwise_and(values, 1)).astype(f32)

    def rotate(target, j):
        lane = lax.broadcasted_iota(jnp.int32, (8, share), 1)
        column = blocks[0, 1] * BLK + j * share + lane
        a_col = ((column.astype(f32) + 0.5) / KB).astype(jnp.int32)
        c_col = column - a_col * KB
        depth = mix.shape[1]
        row = lax.broadcasted_iota(jnp.int32, (depth, share), 0)
        pick = jnp.where(row == c_col[:1, :], 1.0, 0.0).astype(bf16)
        mixed = jnp.dot(mix[...], pick, preferred_element_type=f32)
        for start in range(0, GROUP, 8):
            rank = start + lax.broadcasted_iota(jnp.int32, (8, share), 0)
            flips[start : start + 8, :] = odd(jnp.bitwise_and(rank, a_col))
        quad = pattern.shape[0] // KB

        for q in range(GROUP // quad):
            wide = [(mixed * flips[r : r + 1, :]).astype(bf16) for r in range(q * quad, (q + 1) * quad)]
            base[q * quad * KB : (q + 1) * quad * KB, :] = jnp.dot(
                pattern[...], jnp.concatenate(wide, axis=0), preferred_element_type=f32
            ).astype(bf16)
        a_local = groups * GROUP
        total = None
        for g in range(groups):
            part = jnp.dot(
                ffn_v[:, g * deep : (g + 1) * deep], base[...], preferred_element_type=f32
            )
            sign = odd(jnp.bitwise_and(t * a_local + g * GROUP, a_col)) / math.sqrt(a_local * n)
            part = part * sign[:1, :]
            total = part if total is None else total + part
        target[...] = total

    strip = 64

    def stat():
        loads[1].wait()

        @pl.when(s == 0)
        def _():
            rc[...] = jnp.zeros_like(rc)

        @pl.when(s > 0)
        def _():
            lift(0, res_h).wait_recv()

        def squares(b, carry):
            at = pl.ds(pl.multiple_of(b * strip, strip), strip)
            acc = jnp.zeros((strip, 128), f32)
            for c in range(features // 128):
                lanes = slice(c * 128, (c + 1) * 128)
                v = res_v[at, lanes].astype(f32) + rc[0, at, lanes].astype(f32)
                acc = acc + v * v
            sq_col[at, :] = jnp.broadcast_to(jnp.sum(acc, axis=1, keepdims=True), (strip, 128))
            return carry

        lax.fori_loop(0, rows // strip, squares, 0)
        sq_s[...] = jnp.transpose(sq_col[...])[:8, :]
        for i in range(1, n):
            post(None, functools.partial(stat_copy, i))

    def stat_copy(i):
        name = "stat" + str(i)
        return remote(sq_s, sq_r.at[i], name, name, {"tensor": lax.rem(t + i, n)})

    def inverse(slot, sums):
        spread = jnp.broadcast_to(sums[:1, :], (128, rows))
        inv[slot] = lax.rsqrt(jnp.transpose(spread) / (n * features) + EPS)

    def stats_in():
        total = sq_s[...]
        for i in range(1, n):
            stat_copy(i).wait_recv()
            total = total + sq_r[i]
        tot_s[...] = total
        post(None, tot)
        inverse(0, total)

    def normalize(slot, part):
        def step(b, carry):
            at = pl.ds(pl.multiple_of(b * strip, strip), strip)
            by = inv[slot, at, :]
            for c in range(features // 128):
                lanes = slice(c * 128, (c + 1) * 128)
                v = part[at, lanes].astype(f32) + rc[slot, at, lanes].astype(f32)
                norm_o[slot, at, lanes] = (v * by * gain[:, lanes]).astype(bf16)
            return carry

        lax.fori_loop(0, rows // strip, step, 0)

    def normalize_peer():
        tot().wait_recv()
        inverse(1, tot_r[...])

        @pl.when(s > 0)
        def _():
            res().wait_recv()
            lift(1, res_y).wait_recv()

        normalize(1, res_y)

    def heavy(name):
        if name[0] in "XO":
            i = int(name[1:])
            column = 1 - x if name[0] == "X" else x
            rotate((xs if name[0] == "X" else zs).at[i], 2 * destination(i) + column)
        elif name == "stat":
            stat()
        elif name == "statr":
            stats_in()
        elif name == "normo":
            normalize(0, res_v)
        else:
            normalize_peer()

    mine = pl.ds(pl.multiple_of(d * width, width), width)
    upper = pl.ds(pl.multiple_of(half + d * width, width), width)

    def slab_source(name):
        slot = 0 if name[1] == "o" else 1
        start, count = span(name)
        at = slice(start, start + count)
        if name[0] == "a":
            value = attn_s[d, at] if slot == 0 else attn_y[d, at]
        else:
            value = jnp.where(swap, norm_o[slot, at, upper], norm_o[slot, at, mine])
        return jnp.where(owned, value, jnp.zeros_like(value))

    def span(unit):
        whole = unit[1] == "o" or unit[0] + "q" not in UNITS
        count = rows if whole else rows // 2
        return (rows // 2 if unit[1] == "q" else 0), count

    low = rows // line
    paired_up = set()

    def attn_ready(uc, unit):
        if unit[0] == "a" and unit[1] != "o" and ("q0", uc) not in paired_up:
            paired_up.add(("q0", uc))
            q0().wait_recv()

    def own_ready(uc, b):
        if b > 0 and (uc, b) not in paired_up:
            paired_up.add((uc, b))
            pc(b).wait_recv()

    def light(uc, name):
        def slab(unit):
            return slab_o[0 if unit[0] == "a" else 1].at[0 if unit[1] == "o" else 1]

        def half_of(unit, column):
            start, count = span(unit)
            tall = count // 2
            return slab(unit).at[pl.ds(pl.multiple_of(start + column * tall, tall), tall)]

        def quarter_of(unit, to):
            return slab(unit).at[to * low : (to + 1) * low]

        def place(source, column, b):
            spot = jnp.where(d == 0, source, near - 1 - source) * 2 + column
            slot, start, count = part(b)
            lanes = pl.ds(pl.multiple_of(spot * share, share), share)
            return rot_o.at[slot, pl.ds(start, count), lanes]

        def shared_from(uc, source, b):
            slot, start, count = part(b)
            return own_o.at[slot, pl.ds(start, count)] if uc == source else place(source, x, b)

        def gather(source, b, way, device):
            name = "g" + str(source) + str(b)
            where = place(source, x, b)
            return remote(shared_from(uc, source, b), where, name + way, name, device)

        if name == "q0":
            post(uc, q0)
        elif name == "A2":
            post(uc, a2)
        elif name == "B":
            post(uc, b2)
        elif name == "lift2s":

            @pl.when(s == 0)
            def _():
                res().wait_recv()
                lift(1, res_y).start()

        elif name[:2] == "pc":
            post(uc, lambda: pc(int(name[2])))
        elif name[:2] == "xs":
            i = int(name[2:])
            post(uc, lambda: remote(xs.at[i], xr.at[i], "x" + str(i), "x" + str(i), x_peer))
        elif name[0] in "IJ":
            i = int(name[1:])
            to = order[uc][i]
            own = name[0] == "I"
            store = zs if own else xs
            held = store.at[i]
            parts = [held]

            def across():
                return remote(xs.at[i], xr.at[i], "x" + str(i), "x" + str(i), x_peer)

            def along(way):
                key = ("L" if way == 0 else "R") + ("" if own else "x") + str(to)
                slots = (onto if own else onto_x) if way == 0 else (into if own else into_x)
                send = ("zs" if own else "xs") + str(i)
                return remote(store.at[i], slots.at[to], send, key, outward if way == 0 else inner)

            if own and (to == uc or to not in DEFERRED):
                across().wait_recv()
                parts.append(xr.at[i])
            if to >= uc and uc > 0:
                along(0).wait_recv()
                parts.append((onto if own else onto_x).at[to])
            if to <= uc and uc < line - 1:
                along(1).wait_recv()
                parts.append((into if own else into_x).at[to])
            if own and to == uc:
                combine(own_o.at[0], parts, rows, bf16)
            elif len(parts) > 1:
                combine(held, parts, rows)
            if to > uc:
                post(uc, lambda: along(0))
            elif to < uc:
                post(uc, lambda: along(1))
            elif not own:
                post(uc, across)
        elif name[:2] == "GX":
            source, b = int(name[2]), int(name[3])
            key = "gx" + name[2:]
            if (source, b) in CROSSED:
                own_ready(uc, b)
            post(uc, lambda: remote(shared_from(uc, source, b), place(source, x, b), key, key, x_peer))
        elif name[0] == "H":
            source, b = int(name[1]), int(name[2])
            where, key = place(source, 1 - x, b), "h" + name[1:]
            if uc == source:
                remote(where, where, "gx" + name[1:], "gx" + name[1:], x_peer).wait_recv()
            else:
                remote(where, where, key + "o", key, outward).wait_recv()

            def ahead(way, device):
                spot = place(source, 1 - x, b)
                return remote(spot, spot, key + way, key, device)

            if uc >= source and uc < line - 1:
                post(uc, lambda: ahead("o", outward))
            if uc <= source and uc > 0:
                post(uc, lambda: ahead("i", inner))
        elif name[0] == "G":
            source, b = int(name[1]), int(name[2])
            if uc == source:
                own_ready(uc, b)
            else:
                gather(source, b, "o", outward).wait_recv()
            if uc >= source and uc < line - 1:
                post(uc, lambda: gather(source, b, "o", outward))
            if uc <= source and uc > 0:
                post(uc, lambda: gather(source, b, "i", inner))
            if uc == source:
                combine(place(source, x, b), [shared_from(uc, source, b)], part(b)[2])
        else:
            slabs(uc, name, half_of, quarter_of)

    def slabs(uc, name, half_of, quarter_of):
        unit = next(k for k in UNITS if k in name)
        kind, rest = name.split(unit)
        k = UNITS.index(unit)
        tall = span(unit)[1] // 2
        used = slice(0, tall)

        def cross():
            return remote(sl_s.at[k, used], sl_x.at[k, used], "S" + unit, "S" + unit, x_peer)

        def flood(way):
            key = "fo" if way == 0 else "fi"
            device = outward if way == 0 else inner
            return remote(fl_s.at[k, way, used], fl_r.at[k, way, used], key + unit, key + unit, device)

        def back():
            return remote(half_of(unit, x), half_of(unit, x), "b" + unit, "b" + unit, x_peer)

        def reduce(to):
            key = "r" + unit + str(to)
            if to > uc:
                return remote(qt_s.at[k, to], qt_o.at[k, to], key, key + "o", outward)
            if to < uc:
                return remote(qt_s.at[k, to], qt_i.at[k, to], key, key + "i", inner)
            return remote(qt_s.at[k, to], qt_x.at[k], key, "rx" + unit, x_peer)

        def wave(source, way, device):
            key = "w" + unit + str(source)
            return remote(quarter_of(unit, source), quarter_of(unit, source), key + way, key, device)

        if unit in HALVED:
            if kind == "S":
                attn_ready(uc, unit)
                value = slab_source(unit)
                first, second = value[:tall], value[tall:]
                sl_k[k, used] = jnp.where(x == 0, first, second)
                sl_s[k, used] = jnp.where(x == 0, second, first)
                post(uc, cross)
            elif kind == "P":
                cross().wait_recv()
                combine(sl_p.at[k], [sl_k.at[k], sl_x.at[k]], tall)
            elif kind == "fo":
                parts = [sl_p.at[k]]
                if uc > 0:
                    flood(0).wait_recv()
                    parts.append(fl_r.at[k, 0])
                combine(fl_s.at[k, 0], parts, tall)
                post(uc, lambda: flood(0))
            elif kind == "fi":
                parts = [sl_p.at[k]]
                if uc < line - 1:
                    flood(1).wait_recv()
                    parts.append(fl_r.at[k, 1])
                combine(fl_s.at[k, 1], parts, tall)
                post(uc, lambda: flood(1))
            else:
                parts = [sl_p.at[k]]
                if uc > 0:
                    parts.append(fl_r.at[k, 0])
                    if uc == line - 1:
                        flood(0).wait_recv()
                if uc < line - 1:
                    parts.append(fl_r.at[k, 1])
                    if uc == 0:
                        flood(1).wait_recv()
                combine(half_of(unit, x), parts, tall)
                post(uc, back)
            return
        if kind == "S":
            attn_ready(uc, unit)
            qt_f[k] = slab_source(unit)
        elif kind == "r":
            to = int(rest)
            parts = [qt_f.at[k, to * low : (to + 1) * low]]
            if to >= uc and uc > 0:
                remote(qt_s.at[k, to], qt_o.at[k, to], "r" + unit + rest, "r" + unit + rest + "o", outward).wait_recv()
                parts.append(qt_o.at[k, to])
            if to <= uc and uc < line - 1:
                remote(qt_s.at[k, to], qt_i.at[k, to], "r" + unit + rest, "r" + unit + rest + "i", inner).wait_recv()
                parts.append(qt_i.at[k, to])
            combine(qt_s.at[k, to], parts, low)
            post(uc, lambda: reduce(to))
        else:
            source = int(rest)
            if source == uc:
                reduce(uc).wait_recv()
                combine(quarter_of(unit, uc), [qt_s.at[k, uc], qt_x.at[k]], low)
            else:
                wave(source, "o", outward).wait_recv()
            if source <= uc and uc < line - 1:
                post(uc, lambda: wave(source, "o", outward))
            if source >= uc and uc > 0:
                post(uc, lambda: wave(source, "i", inner))

    steps = step_names(line, near)
    shared = [steps[i] for i in SHARED]
    parts = [segments([steps[i] for i in o], shared) for o in ORDERS]
    started = [False]
    for k, name in enumerate(shared + [None]):
        for uc in range(line):
            if parts[uc][k]:

                @pl.when(u == uc)
                def _():
                    for each in parts[uc][k]:
                        light(uc, each)

        if name is None:
            break
        if name[0] in "XO" and not started[0]:
            started[0] = True
            loads[3].wait()
            loads[4].wait()
            setup()
            loads[2].wait()
        heavy(name)

    @pl.when(u >= near)
    def _():
        pc(1).wait_recv()
        pc(2).wait_recv()

    assert len(names) <= SEMAPHORES, len(names)

    combine(attn_o.at[0], [attn_v], rows)
    a2().wait_recv()
    b2().wait_recv()
    for k in range(4):
        here = slice(k * width, (k + 1) * width)
        attn_o[1, :, here] = jnp.where(swap, attn_y[(k + 2) % 4], attn_y[k])

    for unit in HALVED:
        m, b = 0 if unit[0] == "a" else 1, 0 if unit[1] == "o" else 1
        start, count = span(unit)
        tall = count // 2
        where = slab_o[m].at[b, pl.ds(pl.multiple_of(start + (1 - x) * tall, tall), tall)]
        remote(where, where, "b" + unit, "b" + unit, x_peer).wait_recv()
    for source in range(near):
        for b in range(3):
            if (source, b) in CROSSED:
                continue
            slot, start, count = part(b)
            spot = jnp.where(d == 0, source, near - 1 - source) * 2 + 1 - x
            lanes = pl.ds(pl.multiple_of(spot * share, share), share)
            where = rot_o.at[slot, pl.ds(start, count), lanes]
            key = "gx" + str(source) + str(b)
            remote(where, where, key, key, x_peer).wait_recv()

    for make in sent[None]:
        make().wait_send()
    for uc in range(line):

        @pl.when(u == uc)
        def _():
            for make in sent[uc]:
                make().wait_send()

    @pl.when(s == 0)
    def _():
        lift(0, res_h).wait_send()
        lift(1, res_y).wait_send()


SEMAPHORES = 192
ROOM = 64


def exchanged(*operands):
    attn, res, ffn, gain, mixing, blocks = operands
    n = lax.axis_size("tensor")
    rows, features = attn.shape
    share, width = BLK // n, HBLK // 2
    line = n // 2
    groups = ffn.shape[1] // (GROUP * KB)
    halved = len(UNITS)
    units = 1 if len(HALVED) == len(UNITS) else len(UNITS)
    f32, bf16 = jnp.float32, jnp.bfloat16
    vmem = pl.BlockSpec(memory_space=pltpu.VMEM)
    return pl.pallas_call(
        functools.partial(exchange_kernel, n, groups),
        out_shape=[
            jax.ShapeDtypeStruct((2, rows, features), bf16),
            jax.ShapeDtypeStruct((2, rows, features), bf16),
            jax.ShapeDtypeStruct((2, rows, width), bf16),
            jax.ShapeDtypeStruct((2, rows, width), bf16),
            jax.ShapeDtypeStruct((2, rows, BLK // 2), bf16),
            jax.ShapeDtypeStruct((2, rows, share), bf16),
        ],
        in_specs=[pl.BlockSpec(memory_space=pltpu.HBM)] * 6,
        out_specs=[vmem] * 6,
        scratch_shapes=[
            pltpu.VMEM((rows, features), bf16),
            pltpu.VMEM((rows, features), bf16),
            pltpu.VMEM(ffn.shape, bf16),
            pltpu.VMEM((4, rows, width), bf16),
            pltpu.VMEM((4, rows, width), bf16),
            pltpu.VMEM((rows, features), bf16),
            pltpu.VMEM((2, rows, features), bf16),
            pltpu.VMEM((line, rows, share), f32),
            pltpu.VMEM((line, rows, share), f32),
            pltpu.VMEM((line, rows, share), f32),
            pltpu.VMEM((line, rows, share), f32),
            pltpu.VMEM((line, rows, share), f32),
            pltpu.VMEM((line if DEFERRED else 1, rows, share), f32),
            pltpu.VMEM((line if DEFERRED else 1, rows, share), f32),
            pltpu.VMEM((rows, 128), f32),
            pltpu.VMEM((8, rows), f32),
            pltpu.VMEM((n, 8, rows), f32),
            pltpu.VMEM((8, rows), f32),
            pltpu.VMEM((8, rows), f32),
            pltpu.VMEM((2, rows, 128), f32),
            pltpu.VMEM((halved, rows // 2, width), bf16),
            pltpu.VMEM((halved, rows // 2, width), bf16),
            pltpu.VMEM((halved, rows // 2, width), bf16),
            pltpu.VMEM((halved, rows // 2, width), bf16),
            pltpu.VMEM((halved, 2, rows // 2, width), bf16),
            pltpu.VMEM((halved, 2, rows // 2, width), bf16),
            pltpu.VMEM(gain.shape, f32),
            pltpu.VMEM(mixing.shape, bf16),
            pltpu.SMEM(blocks.shape, jnp.int32),
            pltpu.VMEM((units, rows, width), bf16),
            pltpu.VMEM((units, line, rows // line, width), bf16),
            pltpu.VMEM((units, line, rows // line, width), bf16),
            pltpu.VMEM((units, line, rows // line, width), bf16),
            pltpu.VMEM((units, rows // line, width), bf16),
            pltpu.VMEM((ROOM, 128), bf16),
            pltpu.VMEM((4 * KB, 4 * ROOM), bf16),
            pltpu.VMEM((GROUP, share), f32),
            pltpu.VMEM((GROUP * KB, share), bf16),
            pltpu.SemaphoreType.DMA((6,)),
            pltpu.SemaphoreType.DMA((SEMAPHORES,)),
            pltpu.SemaphoreType.DMA((SEMAPHORES,)),
        ],
        compiler_params=pltpu.CompilerParams(
            collective_id=2, has_side_effects=True, vmem_limit_bytes=43 << 20
        ),
    )(*[pltpu.with_memory_space_constraint(v, pltpu.HBM) for v in operands])


def parity_sign(values):
    return (1 - 2 * (lax.population_count(values) & 1)).astype(jnp.float32)


def gram(left, right):
    return lax.dot_general(
        left, right, (((0,), (0,)), ((), ())), preferred_element_type=jnp.float32
    )


def general(residual_parts, attn_out, ffn_input, norm_gain, mixing, blocks):
    local_d = residual_parts.shape[2]
    local_f = ffn_input.shape[2]
    token_rows = residual_parts.shape[1]
    dp_count = lax.axis_size("dp")
    dp_member = lax.axis_index("dp")
    tensor_count = lax.axis_size("tensor")
    member = lax.axis_index("tensor")
    own_part = residual_parts[0]
    parts = gathered(own_part, "dp")
    attention = jnp.concatenate(gathered(attn_out[0], "dp"), axis=0)
    earlier = [passed_along(part, "section", 1) for part in parts]
    layers = [
        e.astype(jnp.float32) + p.astype(jnp.float32) for e, p in zip(earlier, parts)
    ]
    squares = jnp.sum(layers[0] * layers[0], axis=1).reshape(token_rows // 128, 128)

    a_local = local_f // KB
    order_a = a_local * tensor_count
    deep = GROUP * KB
    column = blocks[0, 1] * BLK + jnp.arange(BLK, dtype=jnp.int32)
    a_col, c_col = column // KB, column % KB
    pick = (jnp.arange(KB, dtype=jnp.int32)[:, None] == c_col[None, :]).astype(jnp.bfloat16)
    spread = jnp.dot(
        jnp.tile(mixing[0], (GROUP, 1)), pick, preferred_element_type=jnp.float32
    )
    row_a = jnp.arange(deep, dtype=jnp.int32) // KB
    base = (spread * parity_sign(row_a[:, None] & a_col[None, :])).astype(jnp.bfloat16)
    term = None
    for g in range(a_local // GROUP):
        sign = parity_sign((member * a_local + g * GROUP) & a_col) / math.sqrt(order_a)
        piece = jnp.dot(
            ffn_input[0, :, g * deep : (g + 1) * deep], base, preferred_element_type=jnp.float32
        )
        piece = piece * sign[None, :]
        term = piece if term is None else term + piece

    rotated, square_own = tensor_sum(term, squares, 0)

    square_total = gathered(square_own, "dp")
    rotated, square_total = lax.optimization_barrier((rotated, square_total))
    square_total = [s.reshape(token_rows) for s in square_total]
    share = BLK // tensor_count
    own_cols = lax.dynamic_slice_in_dim(rotated, member * share, share, 1)
    part_down = gram(own_cols, rotated)
    half = BLK // dp_count
    if dp_count == 2:
        kept = lax.dynamic_slice_in_dim(part_down, dp_member * half, half, 1)
        sent = lax.dynamic_slice_in_dim(part_down, (1 - dp_member) * half, half, 1)
        sum_down = kept + shifted(sent, "dp", 1)
    else:
        sum_down = lax.psum_scatter(part_down, "dp", scatter_dimension=1, tiled=True)

    normed = jnp.concatenate(
        [
            (x * lax.rsqrt(s / D + EPS)[:, None] * norm_gain[0][None, :]).astype(jnp.bfloat16)
            for x, s in zip(layers, square_total)
        ],
        axis=0,
    )
    first_col = blocks[0, 0] * HBLK
    width = HBLK // dp_count
    offset = first_col % local_d + dp_member * width
    owned = first_col // local_d == member
    slab = jnp.concatenate(
        [
            lax.dynamic_slice_in_dim(normed, offset, width, 1),
            lax.dynamic_slice_in_dim(attention, offset, width, 1),
        ],
        axis=0,
    )
    slab = jnp.where(owned, slab, 0).astype(jnp.bfloat16)
    (got,) = tensor_sum(slab, None, 1)
    tokens = token_rows * dp_count
    scale = 2.0 / tokens
    hess_in = (scale * gram(normed, got[:tokens]))[None]
    hess_o = (scale * gram(attention, got[tokens:]))[None]
    hess_down = (scale * sum_down)[None]
    return (hess_in, hess_o, hess_down)


STRIPS = 4


def gram_kernel(scale, attn, normed, slab_a, slab_n, rotated, own, *refs):
    out_in, out_o, out_down, held, held_down, done = refs

    def put(target, at, place):
        return pltpu.make_async_copy(held.at[place], target.at[at], done.at[place])

    held_down[...] = scale * gram(own[...], rotated[...])
    down = pltpu.make_async_copy(held_down, out_down, done.at[2 * STRIPS])
    down.start()
    tall = normed.shape[1] // STRIPS
    copies = []
    for k, (left, right, target) in enumerate([(attn, slab_a, out_o), (normed, slab_n, out_in)]):
        for strip in range(STRIPS):
            at = slice(strip * tall, (strip + 1) * tall)
            place = k * STRIPS + strip
            held[place] = scale * gram(left[:, at], right[...])
            copies.append(put(target, pl.ds(strip * tall, tall), place))
            copies[-1].start()
    for copy in copies + [down]:
        copy.wait()


def grams(scale, attn, normed, slab_a, slab_n, rotated, own):
    features, width = normed.shape[1], slab_n.shape[1]
    down = (own.shape[1], rotated.shape[1])
    f32 = jnp.float32
    return pl.pallas_call(
        functools.partial(gram_kernel, scale),
        out_shape=[
            jax.ShapeDtypeStruct((features, width), f32),
            jax.ShapeDtypeStruct((features, width), f32),
            jax.ShapeDtypeStruct(down, f32),
        ],
        in_specs=[pl.BlockSpec(memory_space=pltpu.VMEM)] * 6,
        out_specs=[pl.BlockSpec(memory_space=pl.ANY)] * 3,
        scratch_shapes=[
            pltpu.VMEM((2 * STRIPS, features // STRIPS, width), f32),
            pltpu.VMEM(down, f32),
            pltpu.SemaphoreType.DMA((2 * STRIPS + 1,)),
        ],
        compiler_params=pltpu.CompilerParams(vmem_limit_bytes=20 << 20),
    )(attn, normed, slab_a, slab_n, rotated, own)


def paired(residual_parts, attn_out, ffn_input, norm_gain, mixing, blocks):
    local_d = residual_parts.shape[2]
    token_rows = residual_parts.shape[1]
    share = BLK // lax.axis_size("tensor")
    attention, normed, slab_a, slab_n, rotated, own = exchanged(
        attn_out[0], residual_parts[0], ffn_input[0], norm_gain, mixing, blocks
    )
    tokens = token_rows * 2
    scale = 2.0 / tokens
    attention, normed = attention.reshape(tokens, local_d), normed.reshape(tokens, local_d)
    slab_a, slab_n = slab_a.reshape(tokens, HBLK // 2), slab_n.reshape(tokens, HBLK // 2)
    hess_in, hess_o, hess_down = grams(
        scale,
        attention,
        normed,
        slab_a,
        slab_n,
        rotated.reshape(tokens, BLK // 2),
        own.reshape(tokens, share),
    )
    return (hess_in[None], hess_o[None], hess_down[None])


def local(*arguments):
    n = lax.axis_size("tensor")
    by_pairs = lax.axis_size("dp") == 2 and lax.axis_size("section") == 2 and n == 2 * len(ORDERS)
    if by_pairs and arguments[0].shape[2] == 2 * HBLK:
        return paired(*arguments)
    return general(*arguments)


def solution(mesh):
    return jax.shard_map(
        local,
        mesh=mesh,
        in_specs=(
            P("section", "dp", "tensor"),
            P("section", "dp", "tensor"),
            P("section", "dp", "tensor"),
            P("section", "tensor"),
            P("section", None, None),
            P("section", None),
        ),
        out_specs=(
            P("section", "tensor", "dp"),
            P("section", "tensor", "dp"),
            P("section", "tensor", "dp"),
        ),
        check_vma=False,
    )
```
